32 devices in a mesh: gx: 2 (over core), gy: 4 (over y, x), gz: 4 (over z).
Axes of the slice: x: 2, y: 2, z: 4, core: 2. Of those that a mesh axis runs over, the one named last changes fastest.
Arguments:
- pressure_rhs: float32 [32, 128, 2048], P('gx', 'gy', 'gz'), may hold values from -6 to 6
- shift_diag: float32 [32, 128, 2048], P('gx', 'gy', 'gz'), may hold values from 0.02 to 0.3
- positions: float32 [3, 262144], P(None, ('gx', 'gy', 'gz')), may hold values from -6 to 6
- normals: float32 [3, 262144], P(None, ('gx', 'gy', 'gz')), may hold values from -6 to 6
- tension: float32 [262144], P(('gx', 'gy', 'gz')), may hold values from 0.3 to 3
- edge_weight: float32 [6, 262144], P(None, ('gx', 'gy', 'gz')), may hold values from 0.5 to 2
- owner_map: int32 [262144, 1], P(('gx', 'gy', 'gz')), may hold values from 0 to 31; in each aligned block of 8192 rows (0 to 8191, 8192 to 16383, ...) at most 1024 rows name the same one
- cell_map: int32 [262144], P(('gx', 'gy', 'gz')), may hold values from 0 to 262143
- connectivity: int32 [6, 262144], P(None, ('gx', 'gy', 'gz')), may hold values from 0 to 262143, as said below
Outputs:
- pressure: float32 [32, 128, 2048], P('gx', 'gy', 'gz')
- surface_force: float32 [3, 262144], P(None, ('gx', 'gy', 'gz'))
The draws below stay inside these ranges and needn't reach their ends.
Inputs may be any that keep to these rules, and one draw needn't show every extreme that they name: `connectivity`: each neighbour index differs from the point's own index by 1 to 64, counted cyclically over 262144; the distance 64 occurs. `owner_map`: among the points of one device no owner is named more than 1024 times, a bound that some block reaches.
All inputs are finite; a program needn't handle non-finite values.
Results may differ from the reference program's by a relative error of at most 0.0003.
Values sent between devices are 32-bit elements; how exact they have to be, the bound alone decides.
A program may use at most 192 MiB of HBM per device.

```python
import math
import jax
import jax.numpy as jnp
import numpy as np

CX = 16
CY = 32
CZ = 512
PTS_DEV = 8192
NEIGH = 6
HALO = 64
SMOOTH = 3
COARSE_SMOOTH = 4
POINTS = 262144
CAP = 1024
NX = 32
NY = 128
NZ = 2048
N_GY = 4
N_GZ = 4
DEVICES = 32


def draw_connectivity(key, part):
    first = jax.random.fold_in(key, 11)
    second = jax.random.fold_in(key, 12)
    reach = jax.random.randint(first, (NEIGH, POINTS), 1, HALO + 1)
    reach = reach.at[0, 0].set(HALO)
    sign = jax.random.randint(second, (NEIGH, POINTS), 0, 2) * 2 - 1
    base = jnp.arange(POINTS, dtype=jnp.int32)[None, :]
    return ((base + sign * reach) % POINTS).astype(jnp.int32)


def plant(entries, stream_key, smallest, high):
    dims = entries.shape
    place = [jax.random.randint(jax.random.fold_in(stream_key, axis), (), 0, dims[axis]) for axis in range(len(dims))]
    entries = entries.at[tuple(place)].set(smallest)
    longest = dims.index(max(dims))
    place[longest] = (place[longest] + 1) % dims[longest]
    return entries.at[tuple(place)].set(high)


def block_levels(own_key, extent, pieces, least, top_value):
    factor_of, own = 1.0, jax.random.fold_in(own_key, 6)
    for axis_at, shards_of in pieces:
        heights = jnp.exp(jax.random.uniform(jax.random.fold_in(own, axis_at), (shards_of,), jnp.float32, least / len(pieces), top_value / len(pieces)))
        factor_of = factor_of * jnp.repeat(heights, extent[axis_at] // shards_of).reshape([-1 if axis == axis_at else 1 for axis in range(len(extent))])
    return factor_of


def deal_out(key, own, number, rows, amount, top, most, slope):
    sequence = jax.random.permutation(key, amount)
    heavy_load, common = shares(amount, rows * top, most, slope, True), shares(amount, rows * top, most, slope, False)
    places = jnp.arange(amount)

    def named(tallies, rotation):
        used = int((tallies > 0).sum())
        fixed = max(1, used // 4)
        shifted = fixed + (places - fixed + rotation * (used - fixed)) % max(1, amount - fixed)
        return jnp.zeros((amount,), jnp.int32).at[sequence[jnp.where(places < fixed, places, shifted)]].set(jnp.asarray(tallies, jnp.int32))

    tallies = jnp.where(number % 4 == 0, named(heavy_load, number // 4), named(common, number - number // 4 - 1))
    mixed = jax.random.permutation(jax.random.fold_in(own, 3), amount)
    giver, taker = mixed[0:amount // 2 * 2:2], mixed[1:amount // 2 * 2:2]
    room = jnp.minimum(tallies[giver] - 1, most - tallies[taker]) // 2
    room = jnp.where((giver == sequence[0]) | (taker == sequence[0]) | (tallies[taker] == 0), 0, jnp.maximum(room, 0))
    shifted = jax.random.randint(jax.random.fold_in(own, 4), (amount // 2,), 0, 1 << 20) % (room + 1)
    tallies = tallies.at[giver].add(-shifted).at[taker].add(shifted)
    members = jnp.searchsorted(jnp.cumsum(tallies), jnp.arange(rows * top), side="right").astype(jnp.int32)
    listing = members.reshape(top, rows).T
    listing = listing[jax.random.permutation(jax.random.fold_in(own, 1), rows)]
    rotation = jax.random.randint(jax.random.fold_in(own, 2), (rows, 1), 0, top)
    return jnp.take_along_axis(listing, (jnp.arange(top)[None, :] + rotation) % top, axis=1)


def shares(count, total, bound, slope, full):
    weights = [(1 << 20) // math.isqrt(grade ** slope) + 1 for grade in range(1, count + 1)]
    largest = bound if full else min(bound, max(-(-total // count), total * weights[0] // sum(weights)))
    least = 1 if total - largest >= count - 1 else 0
    given, surplus = [largest] + [least] * (count - 1), total - largest - least * (count - 1)
    while surplus > 0:
        free = [i for i in range(1, count) if given[i] < largest] or [i for i in range(1, count) if given[i] < bound]
        whole, budget = sum([weights[i] for i in free]), surplus
        for i in free:
            more = min(bound - given[i], max(1, budget * weights[i] // whole), surplus)
            given[i] = given[i] + more
            surplus = surplus - more
    return np.array(given)


def scatter_about(stream_key, extent, scale, most, split=(), kind=jnp.bfloat16):
    gain = block_levels(stream_key, extent, split, -0.22, 0.18) if split else 1.0
    array = jax.random.normal(stream_key, extent, jnp.float32) * scale * gain
    return jnp.minimum(jnp.maximum(array, -most), most).astype(kind)


def setup_inputs(seed: int = 0) -> dict:
    keys = jax.random.split(jax.random.key(seed), 10)
    pressure_rhs = scatter_about(keys[0], (NX, NY, NZ), 1.0, 6.0, ((0, 2), (1, 4), (2, 4)), jnp.float32)
    shift_diag = jnp.clip(jnp.exp(math.log(0.3) - 2.7080503 * jax.random.uniform(keys[1], (NX, NY, NZ), jnp.float32) ** block_levels(keys[1], (NX, NY, NZ), ((0, 2), (1, 4), (2, 4)), -0.2, 0.2)), 0.02, 0.3)
    positions = scatter_about(keys[2], (3, POINTS), 1.0, 6.0, ((1, 32),), jnp.float32)
    normals = scatter_about(keys[3], (3, POINTS), 1.0, 6.0, ((1, 32),), jnp.float32)
    tension = jnp.clip(jnp.exp(math.log(3.0) - 2.3025851 * jax.random.uniform(keys[4], (POINTS,), jnp.float32) ** block_levels(keys[4], (POINTS,), ((0, 32),), -0.2, 0.2)), 0.3, 3.0)
    edge_weight = jnp.clip(jnp.exp(math.log(2.0) - 1.3862944 * jax.random.uniform(keys[5], (NEIGH, POINTS), jnp.float32) ** block_levels(keys[5], (NEIGH, POINTS), ((1, 32),), -0.2, 0.2)), 0.5, 2.0)
    owner_map_keys = jax.random.split(jax.random.fold_in(keys[6], 1), POINTS // PTS_DEV)
    owner_map_turns = jax.random.permutation(jax.random.fold_in(keys[6], 3), POINTS // PTS_DEV)
    owner_map = jax.vmap(lambda own, number: deal_out(jax.random.fold_in(keys[6], 2), own, number, PTS_DEV, DEVICES, 1, CAP, 2))(owner_map_keys, owner_map_turns).reshape((POINTS, 1))
    cell_map = plant(jax.random.randint(keys[7], (POINTS,), 0, CX * CY * CZ), jax.random.fold_in(keys[7], 1), 0, (CX * CY * CZ) - 1).astype(jnp.int32)
    connectivity = draw_connectivity(jax.random.fold_in(keys[9], 71), 0)
    return dict(pressure_rhs=pressure_rhs, shift_diag=shift_diag, positions=positions, normals=normals, tension=tension, edge_weight=edge_weight, owner_map=owner_map, cell_map=cell_map, connectivity=connectivity)


centre = 1.125
spread = 0.875


def operate(field, shift):
    padded = jnp.pad(field, 1)
    beside = padded[2:, 1:-1, 1:-1] + padded[:-2, 1:-1, 1:-1]
    beside = beside + padded[1:-1, 2:, 1:-1] + padded[1:-1, :-2, 1:-1]
    beside = beside + padded[1:-1, 1:-1, 2:] + padded[1:-1, 1:-1, :-2]
    return (6.0 + shift) * field - beside


def chebyshev(target, shift, start, sweeps):
    inverse = 1.0 / (6.0 + shift)
    ratio = centre / spread
    factor = 1.0 / ratio
    if start is None:
        update = inverse * target / centre
        answer = update
    else:
        update = inverse * (target - operate(start, shift)) / centre
        answer = start + update
    for sweep in range(1, sweeps):
        remain = inverse * (target - operate(answer, shift))
        factor_new = 1.0 / (2.0 * ratio - factor)
        update = factor_new * factor * update + (2.0 * factor_new / spread) * remain
        answer = answer + update
        factor = factor_new
    return answer


def blocks(field):
    nxh, nyh, nzh = field.shape[0] // 2, field.shape[1] // 2, field.shape[2] // 2
    return field.reshape(nxh, 2, nyh, 2, nzh, 2)


def reference(pressure_rhs, shift_diag, positions, normals, tension, edge_weight, owner_map, cell_map, connectivity):
    neighbours = positions[:, connectivity]
    surface_force = tension[None, :] * jnp.sum(edge_weight[None, :, :] * (neighbours - positions[:, None, :]), axis=1)
    jump = jnp.sum(surface_force * normals, axis=0)
    owner = owner_map[:, 0]
    ox = owner // (N_GY * N_GZ)
    oy = (owner // N_GZ) % N_GY
    oz = owner % N_GZ
    cx = cell_map // (CY * CZ)
    cy = (cell_map // CZ) % CY
    cz = cell_map % CZ
    forcing = pressure_rhs.at[ox * CX + cx, oy * CY + cy, oz * CZ + cz].add(jump)
    smooth = chebyshev(forcing, shift_diag, None, SMOOTH)
    remain = forcing - operate(smooth, shift_diag)
    coarse_rhs = 0.5 * jnp.sum(blocks(remain), axis=(1, 3, 5))
    coarse_shift = 4.0 * jnp.mean(blocks(shift_diag), axis=(1, 3, 5))
    coarse_fix = chebyshev(coarse_rhs, coarse_shift, None, COARSE_SMOOTH)
    spreadout = jnp.repeat(jnp.repeat(jnp.repeat(coarse_fix, 2, axis=0), 2, axis=1), 2, axis=2)
    pressure = chebyshev(forcing, shift_diag, smooth + spreadout, SMOOTH)
    return pressure, surface_force
```

```python
import functools

import jax
import jax.numpy as jnp
from jax import lax
from jax.experimental import pallas as pl
from jax.experimental.pallas import tpu as pltpu
from jax.sharding import PartitionSpec as P

HALO = 64
SMOOTH = 3
COARSE_SMOOTH = 4


centre = 1.125
spread = 0.875


def padded_2(cells, sides, closed):
    for axis, dim, width in sides:
        count = lax.axis_size(axis)
        ends = count if closed else count - 1
        head = lax.slice_in_dim(cells, 0, width, axis=dim)
        tail = lax.slice_in_dim(cells, cells.shape[dim] - width, cells.shape[dim], axis=dim)
        cells = jnp.concatenate(
            [
                lax.ppermute(tail, axis, [(i, (i + 1) % count) for i in range(ends)]),
                cells,
                lax.ppermute(head, axis, [((i + 1) % count, i) for i in range(ends)]),
            ],
            axis=dim,
        )
    return cells


def factors(sweeps):
    ratio = centre / spread
    fac = 1.0 / ratio
    pairs = [(0.0, 1.0 / centre)]
    for _ in range(1, sweeps):
        fac_new = 1.0 / (2.0 * ratio - fac)
        pairs.append((fac_new * fac, 2.0 * fac_new / spread))
        fac = fac_new
    return pairs


def beside(ref, x, cells):
    ny, nz = cells.shape
    total = ref[x - 1] + ref[x + 1]
    total = total + pltpu.roll(cells, 1, 0) + pltpu.roll(cells, ny - 1, 0)
    return total + pltpu.roll(cells, 1, 1) + pltpu.roll(cells, nz - 1, 1)


LANES = 2 * HALO


def split3(x):
    a = x.astype(jnp.bfloat16)
    rest = x - a.astype(jnp.float32)
    b = rest.astype(jnp.bfloat16)
    c = (rest - b.astype(jnp.float32)).astype(jnp.bfloat16)
    return a, b, c


MESH = pl.DeviceIdType.MESH
FINE = SMOOTH
COARSE = COARSE_SMOOTH - 1 + (SMOOTH + 1) // 2


def sweep(rhs, inverse, src, dst, update, first, last, pair, keep=None):
    old, new = pair

    def slab(x, carry):
        cells = src[x]
        change = new * (inverse[x] * (rhs[x] + beside(src, x, cells)) - cells)
        if old:
            change = change + old * update[x]
        if keep is None:
            update[x] = change
            dst[x] = cells + change
        else:
            keep(x, cells + change)
        return carry

    lax.fori_loop(first, last, slab, 0)


def begin(rhs, inverse, dst, update, slabs):
    def slab(x, carry):
        change = inverse[x] * rhs[x] * (1.0 / centre)
        update[x] = change
        dst[x] = change
        return carry

    lax.fori_loop(0, slabs, slab, 0)


def near(axes):
    ok = None
    where = {}
    for axis, step in axes:
        place = lax.axis_index(axis) + step
        fits = (place >= 0) & (place < lax.axis_size(axis))
        ok = fits if ok is None else ok & fits
        where[axis] = place
    return ok, where


SIDES = (-1, 1)
LINKS = (
    [(("gy", a),) for a in SIDES]
    + [(("gz", b),) for b in SIDES]
    + [(("gy", a), ("gz", b)) for b in SIDES for a in SIDES]
    + [(("gx", a),) for a in SIDES]
)
MIRROR = [1, 0, 3, 2, 7, 6, 5, 4, 9, 8]


def greet(links):
    barrier = pltpu.get_barrier_semaphore()
    peers = 0
    for link in links:
        ok, where = near(link)
        peers = peers + ok.astype(jnp.int32)

        @pl.when(ok)
        def _():
            pl.semaphore_signal(barrier, inc=1, device_id=where, device_id_type=MESH)

    pl.semaphore_wait(barrier, peers)


class Field:
    def __init__(self, ext, depth, wide, send, recv, send_sem, recv_sem, land=None):
        self.ext, self.depth, self.wide = ext, depth, wide
        self.send, self.recv = send, recv
        self.send_sem, self.recv_sem = send_sem, recv_sem
        self.land = land
        self.nx = ext.shape[0] - 2 * depth
        self.ny = ext.shape[1] - 2 * wide
        self.nz = ext.shape[2] - 128

    def message(self, m):
        d, nx, ny, nz, h = self.depth, self.nx, self.ny, self.nz, self.wide
        ext = self.ext
        if m < 2:
            if h == 8:
                rows = (0, ny - h)[m]
                src = ext.at[pl.ds(d, nx), pl.ds(rows, h), pl.ds(0, nz)]
                place = (ny + h, ny)[m]
                got = ext.at[pl.ds(d, nx), pl.ds(place, h), pl.ds(0, nz)]
                other = ext.at[pl.ds(d, nx), pl.ds((ny, ny + h)[m], h), pl.ds(0, nz)]
            else:
                src = self.send[0].at[m]
                got = self.recv[0].at[m]
                other = self.recv[0].at[1 - m]
        elif m < 4:
            src = self.send[1].at[m - 2]
            got = self.recv[1].at[m - 2]
            other = self.recv[1].at[3 - m]
        elif m < 8:
            b, a = divmod(m - 4, 2)
            src = self.send[1].at[b, pl.ds((0, ny - 8)[a], 8)]
            got = self.recv[2].at[b, a]
            other = self.recv[2].at[1 - b, 1 - a]
        else:
            a = m - 8
            src = ext.at[pl.ds((d, nx)[a], d)]
            if self.land is None:
                got = ext.at[pl.ds((0, d + nx)[a], d)]
                other = ext.at[pl.ds((d + nx, 0)[a], d)]
            else:
                got = self.land.at[a]
                other = self.land.at[1 - a]
        return src, other, got

    def copy(self, m, incoming):
        src, other, got = self.message(m)
        k = m if incoming else MIRROR[m]
        return pltpu.make_async_remote_copy(
            src_ref=got if incoming else src,
            dst_ref=got if incoming else other,
            send_sem=self.send_sem.at[m],
            recv_sem=self.recv_sem.at[k],
            device_id=near(LINKS[m])[1],
            device_id_type=MESH,
        )

    def start(self, which):
        for m in which:
            @pl.when(near(LINKS[m])[0])
            def _():
                self.copy(m, False).start()

    def finish(self, which):
        for m in which:
            ok = near(LINKS[m])[0]

            @pl.when(ok)
            def _():
                self.copy(m, False).wait_send()
                self.copy(m, True).wait_recv()

            @pl.when(jnp.logical_not(ok))
            def _():
                got = self.message(m)[2]
                got[...] = jnp.zeros(got.shape, jnp.float32)

    def pack(self):
        d, nx, ny, nz, h = self.depth, self.nx, self.ny, self.nz, self.wide
        ext = self.ext
        if h != 8:
            sub = lax.broadcasted_iota(jnp.int32, (8, nz), 0)

            def pair(t, carry):
                one, two = d + 2 * t, d + 2 * t + 1
                low = jnp.where(sub < h, ext[one, :8, :nz], pltpu.roll(ext[two, :8, :nz], h, 0))
                high = jnp.where(
                    sub < h, pltpu.roll(ext[one, ny - 8 : ny, :nz], h, 0), ext[two, ny - 8 : ny, :nz]
                )
                self.send[0][0, t] = low
                self.send[0][1, t] = high
                return carry

            lax.fori_loop(0, nx // 2, pair, 0)
        group = lax.broadcasted_iota(jnp.int32, (ny, 128), 1) // (2 * h)

        def slab(x, carry):
            low, high = carry
            mine = group == x
            shift = 2 * h * x + h
            low = jnp.where(mine, pltpu.roll(ext[d + x, :ny, :128], shift, 1), low)
            high = jnp.where(mine, pltpu.roll(ext[d + x, :ny, nz - 128 : nz], shift, 1), high)
            return low, high

        zero = jnp.zeros((ny, 128), jnp.float32)
        low, high = lax.fori_loop(0, nx, slab, (zero, zero))
        self.send[1][0] = low
        self.send[1][1] = high

    def unpack(self):
        d, nx, ny, nz, h = self.depth, self.nx, self.ny, self.nz, self.wide
        ext = self.ext
        if h != 8:
            sub = lax.broadcasted_iota(jnp.int32, (8, nz), 0)

            def pair(t, carry):
                minus, plus = self.recv[0][0, t], self.recv[0][1, t]
                ext[d + 2 * t, ny : ny + 8, :nz] = jnp.where(sub < h, plus, pltpu.roll(minus, h, 0))
                ext[d + 2 * t + 1, ny : ny + 8, :nz] = jnp.where(
                    sub < h, pltpu.roll(plus, h, 0), minus
                )
                return carry

            lax.fori_loop(0, nx // 2, pair, 0)
        ends = []
        for b in range(2):
            corner = (self.recv[2][b, 1], self.recv[2][b, 0])
            if h == 8:
                ends.append(jnp.concatenate([self.recv[1][b], *corner], axis=0))
            else:
                sub = lax.broadcasted_iota(jnp.int32, (8, 128), 0)
                ends.append(
                    jnp.concatenate([self.recv[1][b], jnp.where(sub < h, *corner)], axis=0)
                )
        lane = lax.broadcasted_iota(jnp.int32, ends[0].shape, 1)
        both = jnp.where(lane % (2 * h) < h, ends[0], ends[1])
        edge = (lane < h) | (lane >= 128 - h)

        def slab(x, carry):
            moved = pltpu.roll(both, 128 - h - 2 * h * x, 1)
            ext[d + x, :, nz : nz + 128] = jnp.where(edge, moved, 0.0)
            return carry

        lax.fori_loop(0, nx, slab, 0)


def exchange(fields, between=None):
    for field in fields:
        field.pack()
        field.start(range(8))
    if between is not None:
        between()
    for field in fields:
        field.finish(range(8))
        field.unpack()
        field.start((8, 9))
    for field in fields:
        field.finish((8, 9))


def pooled(src, pairs, into, after):
    nx, ny, nz = src.shape
    depth = COARSE

    def add(j, carry):
        pairs[j] = src[2 * j] + src[2 * j + 1]
        return carry

    lax.fori_loop(0, nx // 2, add, 0)
    flat = pairs[...].reshape(nx // 2 * ny, nz)

    def halves(rows, cols, dim):
        r = lax.broadcasted_iota(jnp.int32, (rows, cols), dim)
        c = lax.broadcasted_iota(jnp.int32, (rows, cols), 1 - dim)
        return (r == jnp.right_shift(c, 1)).astype(jnp.float32).astype(jnp.bfloat16)

    along_z = halves(nz, nz // 2, 1)
    along_y = halves(nx // 2 * ny // 2, nx // 2 * ny, 0)
    flat = sum(jnp.dot(p, along_z, preferred_element_type=jnp.float32) for p in split3(flat))
    flat = sum(jnp.dot(along_y, p, preferred_element_type=jnp.float32) for p in split3(flat))
    out = after(0.5 * flat).reshape(nx // 2, ny // 2, nz // 2)
    into[depth : depth + nx // 2, : ny // 2, : nz // 2] = out


def cycle_kernel(
    forcing, shift, pressure,
    rhs, inverse, one, two, update, land, crhs, cinverse, cone, ctwo, cupdate, remain, pairs,
    ysend, yrecv, zsend, zrecv, yzrecv, czsend, czrecv, cyzrecv, send_sem, recv_sem,
):
    greet(LINKS)
    nx, ny, nz = forcing.shape

    def fine(k, ext, landing=None):
        return Field(
            ext, FINE, 4, (ysend.at[k], zsend.at[k]), (yrecv.at[k], zrecv.at[k], yzrecv.at[k]),
            send_sem.at[k], recv_sem.at[k], landing,
        )

    def coarse(k, ext):
        return Field(
            ext, COARSE, 8, (None, czsend.at[k]), (None, czrecv.at[k], cyzrecv.at[k]),
            send_sem.at[3 + k], recv_sem.at[3 + k],
        )

    def load(x, carry):
        rhs[FINE + x, :ny, :nz] = forcing[x]
        inverse[FINE + x, :ny, :nz] = 1.0 / (6.0 + shift[x])
        return carry

    lax.fori_loop(0, nx, load, 0)
    pooled(shift, pairs, cinverse, lambda total: 1.0 / (6.0 + total))
    exchange([fine(0, rhs), fine(1, inverse), coarse(0, cinverse)])

    slabs = nx + 2 * FINE
    pairs_of = factors(SMOOTH)
    bufs = (one, two)
    begin(rhs, inverse, one, update, slabs)
    for k in range(1, SMOOTH):
        sweep(rhs, inverse, bufs[(k - 1) % 2], bufs[k % 2], update, k, slabs - k, pairs_of[k])
    smooth = bufs[(SMOOTH - 1) % 2]
    other = bufs[SMOOTH % 2]

    def residual(x, carry):
        cells = smooth[x]
        total = rhs[x] + beside(smooth, x, cells)
        remain[x - FINE] = total[:ny, :nz] - (6.0 + shift[x - FINE]) * cells[:ny, :nz]
        return carry

    lax.fori_loop(FINE, FINE + nx, residual, 0)
    pooled(remain, pairs, crhs, lambda total: total)
    exchange([fine(2, smooth, land), coarse(1, crhs)])

    cslabs = crhs.shape[0]
    pairs_of = factors(COARSE_SMOOTH)
    cbufs = (cone, ctwo)
    begin(crhs, cinverse, cone, cupdate, cslabs)
    for k in range(1, COARSE_SMOOTH):
        sweep(
            crhs, cinverse, cbufs[(k - 1) % 2], cbufs[k % 2], cupdate, k, cslabs - k, pairs_of[k]
        )
    fix = cbufs[(COARSE_SMOOTH - 1) % 2]

    low = COARSE - (FINE + 1) // 2
    count = cslabs - 2 * low
    cny, cnz = fix.shape[1:]
    fny, fnz = smooth.shape[1:]
    flat = fix[low : low + count].reshape(count * cny, cnz)

    def fan(shape, fine_dim, per_f, per_c, core, jump):
        f = lax.broadcasted_iota(jnp.int32, shape, fine_dim)
        c = lax.broadcasted_iota(jnp.int32, shape, 1 - fine_dim)
        block = 0
        for g in range(1, shape[fine_dim] // per_f):
            block = block + (f >= g * per_f).astype(jnp.int32)
        inner = f - block * per_f
        target = jnp.right_shift(inner, 1) + jnp.where(inner >= core, jump, 0) + block * per_c
        return (c == target).astype(jnp.float32).astype(jnp.bfloat16)

    fan_y = fan((count * fny, count * cny), 0, fny, cny, ny + 4, cny - fny // 2)
    fan_z = fan((cnz, fnz), 1, fnz, cnz, nz + 64, cnz - fnz // 2)
    tall = sum(jnp.dot(fan_y, p, preferred_element_type=jnp.float32) for p in split3(flat))
    full = sum(jnp.dot(p, fan_z, preferred_element_type=jnp.float32) for p in split3(tall))
    for j in range(count):
        part = full[j * fny : (j + 1) * fny]
        for half in range(2):
            x = FINE + 2 * (low + j - COARSE) + half
            if 0 <= x < FINE:
                smooth[x] = land[0, x] + part
            elif FINE <= x < FINE + nx:
                smooth[x] = smooth[x] + part
            elif FINE + nx <= x < slabs:
                smooth[x] = land[1, x - FINE - nx] + part

    pairs_of = factors(SMOOTH)
    bufs = (smooth, other)

    def keep(x, cells):
        pressure[x - FINE] = cells[:ny, :nz]

    for k in range(SMOOTH):
        sweep(
            rhs, inverse, bufs[k % 2], bufs[(k + 1) % 2], update,
            k + 1, slabs - k - 1, pairs_of[k], keep if k == SMOOTH - 1 else None,
        )


def cycle(forcing, shift):
    nx, ny, nz = forcing.shape
    cx, cy, cz = nx // 2, ny // 2, nz // 2

    def buf(*shape):
        return pltpu.VMEM(shape, jnp.float32)

    wide = buf(nx + 2 * FINE, ny + 8, nz + 128)
    cwide = buf(cx + 2 * COARSE, cy + 16, cz + 128)
    vmem = pl.BlockSpec(memory_space=pltpu.VMEM)
    return pl.pallas_call(
        cycle_kernel,
        in_specs=[vmem] * 2,
        out_specs=vmem,
        out_shape=jax.ShapeDtypeStruct(forcing.shape, jnp.float32),
        scratch_shapes=[wide] * 5
        + [buf(2, FINE, ny + 8, nz + 128)]
        + [cwide] * 5
        + [buf(nx, ny, nz), buf(cx, ny, nz)]
        + [buf(3, 2, nx // 2, 8, nz)] * 2
        + [buf(3, 2, ny, 128)] * 2
        + [buf(3, 2, 2, 8, 128)]
        + [buf(2, 2, cy, 128)] * 2
        + [buf(2, 2, 2, 8, 128)]
        + [pltpu.SemaphoreType.DMA((5, 10))] * 2,
        compiler_params=pltpu.CompilerParams(
            collective_id=1, has_side_effects=True, vmem_limit_bytes=60 * 2**20
        ),
    )(forcing, shift)


def points_kernel(
    ndevice, capacity, pos_ref, nrm_ref, ten_ref, wgt_ref, con_ref, own_ref, cel_ref,
    force_ref, packed_ref, carry_ref,
):
    step = pl.program_id(0)
    chunk = ten_ref.shape[1]

    @pl.when(step == 0)
    def _():
        packed_ref[...] = jnp.zeros_like(packed_ref)
        carry_ref[...] = jnp.zeros_like(carry_ref)

    jumps = []
    for sub in range(chunk // LANES):
        here = pl.ds(sub * LANES, LANES)
        base = pl.multiple_of(step * chunk + sub * LANES, LANES)
        lower = pos_ref[:, pl.ds(base, LANES)]
        upper = pos_ref[:, pl.ds(base + LANES, LANES)]
        centre_pos = jnp.concatenate([lower[:, HALO:], upper[:, :HALO]], axis=1)
        total = jnp.zeros_like(lower)
        for which in range(con_ref.shape[0]):
            index = con_ref[which : which + 1, here] - base
            wide = jnp.broadcast_to(index, lower.shape)
            low = jnp.bitwise_and(wide, LANES - 1)
            near = jnp.take_along_axis(lower, low, axis=1, mode="promise_in_bounds")
            far = jnp.take_along_axis(upper, low, axis=1, mode="promise_in_bounds")
            picked = jnp.where(wide < LANES, near, far)
            total = total + wgt_ref[which : which + 1, here] * (picked - centre_pos)
        force = ten_ref[:, here] * total[:3]
        force_ref[:, here] = force
        jumps.append(jnp.sum(force * nrm_ref[:, here], axis=0, keepdims=True))
    jump = jnp.concatenate(jumps, axis=1)

    hot = (lax.broadcasted_iota(jnp.int32, (ndevice, chunk), 0) == own_ref[...]).astype(jnp.float32)
    hot_half = hot.astype(jnp.bfloat16)
    before = (
        lax.broadcasted_iota(jnp.int32, (chunk, chunk), 0)
        < lax.broadcasted_iota(jnp.int32, (chunk, chunk), 1)
    ).astype(jnp.bfloat16)
    earlier = jnp.dot(hot_half, before, preferred_element_type=jnp.float32) + carry_ref[...]
    rank = jnp.sum(hot * earlier, axis=0, keepdims=True).astype(jnp.int32)
    carry_ref[...] = carry_ref[...] + jnp.sum(hot, axis=1, keepdims=True)
    slots = (
        lax.broadcasted_iota(jnp.int32, (capacity, chunk), 0) == rank
    ).astype(jnp.float32).astype(jnp.bfloat16)
    cell = cel_ref[...]
    parts = [piece.astype(jnp.float32) for piece in split3(jump)]
    for bits in (0, 8, 16):
        piece = jnp.bitwise_and(jnp.right_shift(cell, bits), 255).astype(jnp.float32)
        parts.append(piece)
    left = jnp.concatenate([(hot * part).astype(jnp.bfloat16) for part in parts], axis=0)
    packed = lax.dot_general(
        left, slots, (((1,), (1,)), ((), ())), preferred_element_type=jnp.float32
    )
    n = ndevice
    values = packed[0:n] + packed[n : 2 * n] + packed[2 * n : 3 * n]
    cells = packed[3 * n : 4 * n] + 256.0 * packed[4 * n : 5 * n] + 65536.0 * packed[5 * n :]
    packed_ref[:, :capacity] += values
    packed_ref[:, capacity:] += cells


def points(padded, normals, tension, edge_weight, relative, owner_ids, cell_map, ndevice, capacity):
    npoint = tension.shape[0]
    chunk = 4 * LANES if npoint % (4 * LANES) == 0 else LANES
    padded = jnp.concatenate([padded, jnp.zeros((5, padded.shape[1]), jnp.float32)], axis=0)
    neigh = relative.shape[0]

    def rows(count):
        return pl.BlockSpec((count, chunk), lambda i: (0, i))

    return pl.pallas_call(
        functools.partial(points_kernel, ndevice, capacity),
        grid=(npoint // chunk,),
        in_specs=[
            pl.BlockSpec(padded.shape, lambda i: (0, 0)),
            rows(3), rows(1), rows(neigh), rows(neigh), rows(1), rows(1),
        ],
        out_specs=[rows(3), pl.BlockSpec((ndevice, 2 * capacity), lambda i: (0, 0))],
        out_shape=[
            jax.ShapeDtypeStruct((3, npoint), jnp.float32),
            jax.ShapeDtypeStruct((ndevice, 2 * capacity), jnp.float32),
        ],
        scratch_shapes=[pltpu.VMEM((ndevice, 1), jnp.float32)],
        cost_estimate=pl.CostEstimate(
            flops=2 * npoint * capacity * 6 * ndevice, bytes_accessed=40000000, transcendentals=0
        ),
    )(
        padded, normals, tension[None], edge_weight, relative, owner_ids[None], cell_map[None]
    )


def scatter_kernel(rhs_ref, val_ref, row_ref, col_ref, out_ref):
    @pl.when(pl.program_id(0) == 0)
    def _():
        out_ref[...] = rhs_ref[...]

    nrow, ncol = out_ref.shape
    count = val_ref.shape[2]
    value = val_ref[0]
    first = value.astype(jnp.bfloat16)
    second = (value - first.astype(jnp.float32)).astype(jnp.bfloat16)
    by_row = (
        (lax.broadcasted_iota(jnp.int32, (nrow, count), 0) == row_ref[0])
        .astype(jnp.float32)
        .astype(jnp.bfloat16)
    )
    same = lax.broadcasted_iota(jnp.int32, (ncol, count), 0) == col_ref[0]
    total = out_ref[...]
    for piece in (first, second):
        by_col = jnp.where(same, piece.astype(jnp.float32), 0.0).astype(jnp.bfloat16)
        total = total + lax.dot_general(
            by_row, by_col, (((1,), (1,)), ((), ())), preferred_element_type=jnp.float32
        )
    out_ref[...] = total


def scatter(rhs, values, cells):
    nx, ny, nz = rhs.shape
    nrow = nx * ny
    sources, count = values.shape
    rows = cells // nz
    cols = cells - rows * nz
    one = pl.BlockSpec((1, 1, count), lambda i: (i, 0, 0))
    whole = pl.BlockSpec((nrow, nz), lambda i: (0, 0))
    out = pl.pallas_call(
        scatter_kernel,
        grid=(sources,),
        in_specs=[whole, one, one, one],
        out_specs=whole,
        out_shape=jax.ShapeDtypeStruct((nrow, nz), jnp.float32),
        cost_estimate=pl.CostEstimate(
            flops=4 * nrow * nz * sources * count, bytes_accessed=4000000, transcendentals=0
        ),
    )(rhs.reshape(nrow, nz), values[:, None], rows[:, None], cols[:, None])
    return out.reshape(nx, ny, nz)


def body(
    pressure_rhs,
    shift_diag,
    positions,
    normals,
    tension,
    edge_weight,
    owner_map,
    cell_map,
    connectivity,
):
    npoint = positions.shape[1]
    ndevice = lax.axis_size(("gx", "gy", "gz"))
    total = npoint * ndevice
    begin = lax.axis_index(("gx", "gy", "gz")) * npoint
    padded = padded_2(positions, ((("gx", "gy", "gz"), 1, HALO),), True)
    relative = (connectivity - begin + HALO + total) % total
    capacity = 4 * npoint // ndevice
    surface_force, packed = points(
        padded, normals, tension, edge_weight, relative, owner_map[:, 0], cell_map,
        ndevice, capacity,
    )
    got = lax.all_to_all(packed, ("gx", "gy", "gz"), split_axis=0, concat_axis=0, tiled=True)
    forcing = scatter(pressure_rhs, got[:, :capacity], got[:, capacity:].astype(jnp.int32))

    pressure = cycle(forcing, shift_diag)
    return (pressure, surface_force)


def solution(mesh):
    return jax.shard_map(
        body,
        mesh=mesh,
        in_specs=(
            P("gx", "gy", "gz"),
            P("gx", "gy", "gz"),
            P(None, ("gx", "gy", "gz")),
            P(None, ("gx", "gy", "gz")),
            P(("gx", "gy", "gz")),
            P(None, ("gx", "gy", "gz")),
            P(("gx", "gy", "gz"), None),
            P(("gx", "gy", "gz")),
            P(None, ("gx", "gy", "gz")),
        ),
        out_specs=(P("gx", "gy", "gz"), P(None, ("gx", "gy", "gz"))),
        check_vma=False,
    )
```

```python
import functools

import jax
import jax.numpy as jnp
from jax import lax
from jax.experimental import pallas as pl
from jax.experimental.pallas import tpu as pltpu
from jax.sharding import PartitionSpec as P

HALO = 64
SMOOTH = 3
COARSE_SMOOTH = 4


centre = 1.125
spread = 0.875


def padded_2(cells, sides, closed):
    for axis, dim, width in sides:
        count = lax.axis_size(axis)
        ends = count if closed else count - 1
        head = lax.slice_in_dim(cells, 0, width, axis=dim)
        tail = lax.slice_in_dim(cells, cells.shape[dim] - width, cells.shape[dim], axis=dim)
        cells = jnp.concatenate(
            [
                lax.ppermute(tail, axis, [(i, (i + 1) % count) for i in range(ends)]),
                cells,
                lax.ppermute(head, axis, [((i + 1) % count, i) for i in range(ends)]),
            ],
            axis=dim,
        )
    return cells


def factors(sweeps):
    ratio = centre / spread
    fac = 1.0 / ratio
    pairs = [(0.0, 1.0 / centre)]
    for _ in range(1, sweeps):
        fac_new = 1.0 / (2.0 * ratio - fac)
        pairs.append((fac_new * fac, 2.0 * fac_new / spread))
        fac = fac_new
    return pairs


def beside(ref, x, cells):
    ny, nz = cells.shape
    total = ref[x - 1] + ref[x + 1]
    total = total + pltpu.roll(cells, 1, 0) + pltpu.roll(cells, ny - 1, 0)
    return total + pltpu.roll(cells, 1, 1) + pltpu.roll(cells, nz - 1, 1)


LANES = 2 * HALO


def split3(x):
    a = x.astype(jnp.bfloat16)
    rest = x - a.astype(jnp.float32)
    b = rest.astype(jnp.bfloat16)
    c = (rest - b.astype(jnp.float32)).astype(jnp.bfloat16)
    return a, b, c


MESH = pl.DeviceIdType.MESH
FINE = SMOOTH
COARSE = COARSE_SMOOTH - 1 + (SMOOTH + 1) // 2


def sweep(rhs, inverse, src, dst, update, first, last, pair, keep=None):
    old, new = pair

    def slab(x, carry):
        cells = src[x]
        change = new * (inverse[x] * (rhs[x] + beside(src, x, cells)) - cells)
        if old:
            change = change + old * update[x]
        if keep is None:
            update[x] = change
            dst[x] = cells + change
        else:
            keep(x, cells + change)
        return carry

    lax.fori_loop(first, last, slab, 0)


def begin(rhs, inverse, dst, update, slabs):
    def slab(x, carry):
        change = inverse[x] * rhs[x] * (1.0 / centre)
        update[x] = change
        dst[x] = change
        return carry

    lax.fori_loop(0, slabs, slab, 0)


def near(axes):
    ok = None
    where = {}
    for axis, step in axes:
        place = lax.axis_index(axis) + step
        fits = (place >= 0) & (place < lax.axis_size(axis))
        ok = fits if ok is None else ok & fits
        where[axis] = place
    return ok, where


SIDES = (-1, 1)
LINKS = (
    [(("gy", a),) for a in SIDES]
    + [(("gz", b),) for b in SIDES]
    + [(("gy", a), ("gz", b)) for b in SIDES for a in SIDES]
    + [(("gx", a),) for a in SIDES]
)
MIRROR = [1, 0, 3, 2, 7, 6, 5, 4, 9, 8]


def greet(links):
    barrier = pltpu.get_barrier_semaphore()
    peers = 0
    for link in links:
        ok, where = near(link)
        peers = peers + ok.astype(jnp.int32)

        @pl.when(ok)
        def _():
            pl.semaphore_signal(barrier, inc=1, device_id=where, device_id_type=MESH)

    pl.semaphore_wait(barrier, peers)


class Field:
    def __init__(self, ext, depth, wide, send, recv, send_sem, recv_sem, land=None):
        self.ext, self.depth, self.wide = ext, depth, wide
        self.send, self.recv = send, recv
        self.send_sem, self.recv_sem = send_sem, recv_sem
        self.land = land
        self.nx = ext.shape[0] - 2 * depth
        self.ny = ext.shape[1] - 2 * wide
        self.nz = ext.shape[2] - 128

    def message(self, m):
        d, nx, ny, nz, h = self.depth, self.nx, self.ny, self.nz, self.wide
        ext = self.ext
        if m < 2:
            if h == 8:
                rows = (0, ny - h)[m]
                src = ext.at[pl.ds(d, nx), pl.ds(rows, h), pl.ds(0, nz)]
                place = (ny + h, ny)[m]
                got = ext.at[pl.ds(d, nx), pl.ds(place, h), pl.ds(0, nz)]
                other = ext.at[pl.ds(d, nx), pl.ds((ny, ny + h)[m], h), pl.ds(0, nz)]
            else:
                src = self.send[0].at[m]
                got = self.recv[0].at[m]
                other = self.recv[0].at[1 - m]
        elif m < 4:
            src = self.send[1].at[m - 2]
            got = self.recv[1].at[m - 2]
            other = self.recv[1].at[3 - m]
        elif m < 8:
            b, a = divmod(m - 4, 2)
            src = self.send[1].at[b, pl.ds((0, ny - 8)[a], 8)]
            got = self.recv[2].at[b, a]
            other = self.recv[2].at[1 - b, 1 - a]
        else:
            a = m - 8
            src = ext.at[pl.ds((d, nx)[a], d)]
            if self.land is None:
                got = ext.at[pl.ds((0, d + nx)[a], d)]
                other = ext.at[pl.ds((d + nx, 0)[a], d)]
            else:
                got = self.land.at[a]
                other = self.land.at[1 - a]
        return src, other, got

    def copy(self, m, incoming):
        src, other, got = self.message(m)
        k = m if incoming else MIRROR[m]
        return pltpu.make_async_remote_copy(
            src_ref=got if incoming else src,
            dst_ref=got if incoming else other,
            send_sem=self.send_sem.at[m],
            recv_sem=self.recv_sem.at[k],
            device_id=near(LINKS[m])[1],
            device_id_type=MESH,
        )

    def start(self, which):
        for m in which:
            @pl.when(near(LINKS[m])[0])
            def _():
                self.copy(m, False).start()

    def finish(self, which):
        for m in which:
            ok = near(LINKS[m])[0]

            @pl.when(ok)
            def _():
                self.copy(m, False).wait_send()
                self.copy(m, True).wait_recv()

            @pl.when(jnp.logical_not(ok))
            def _():
                got = self.message(m)[2]
                got[...] = jnp.zeros(got.shape, jnp.float32)

    def pack(self):
        d, nx, ny, nz, h = self.depth, self.nx, self.ny, self.nz, self.wide
        ext = self.ext
        if h != 8:
            sub = lax.broadcasted_iota(jnp.int32, (8, nz), 0)

            def pair(t, carry):
                one, two = d + 2 * t, d + 2 * t + 1
                low = jnp.where(sub < h, ext[one, :8, :nz], pltpu.roll(ext[two, :8, :nz], h, 0))
                high = jnp.where(
                    sub < h, pltpu.roll(ext[one, ny - 8 : ny, :nz], h, 0), ext[two, ny - 8 : ny, :nz]
                )
                self.send[0][0, t] = low
                self.send[0][1, t] = high
                return carry

            lax.fori_loop(0, nx // 2, pair, 0)
        group = lax.broadcasted_iota(jnp.int32, (ny, 128), 1) // (2 * h)

        def slab(x, carry):
            low, high = carry
            mine = group == x
            shift = 2 * h * x + h
            low = jnp.where(mine, pltpu.roll(ext[d + x, :ny, :128], shift, 1), low)
            high = jnp.where(mine, pltpu.roll(ext[d + x, :ny, nz - 128 : nz], shift, 1), high)
            return low, high

        zero = jnp.zeros((ny, 128), jnp.float32)
        low, high = lax.fori_loop(0, nx, slab, (zero, zero))
        self.send[1][0] = low
        self.send[1][1] = high

    def unpack(self):
        d, nx, ny, nz, h = self.depth, self.nx, self.ny, self.nz, self.wide
        ext = self.ext
        if h != 8:
            sub = lax.broadcasted_iota(jnp.int32, (8, nz), 0)

            def pair(t, carry):
                minus, plus = self.recv[0][0, t], self.recv[0][1, t]
                ext[d + 2 * t, ny : ny + 8, :nz] = jnp.where(sub < h, plus, pltpu.roll(minus, h, 0))
                ext[d + 2 * t + 1, ny : ny + 8, :nz] = jnp.where(
                    sub < h, pltpu.roll(plus, h, 0), minus
                )
                return carry

            lax.fori_loop(0, nx // 2, pair, 0)
        ends = []
        for b in range(2):
            corner = (self.recv[2][b, 1], self.recv[2][b, 0])
            if h == 8:
                ends.append(jnp.concatenate([self.recv[1][b], *corner], axis=0))
            else:
                sub = lax.broadcasted_iota(jnp.int32, (8, 128), 0)
                ends.append(
                    jnp.concatenate([self.recv[1][b], jnp.where(sub < h, *corner)], axis=0)
                )
        lane = lax.broadcasted_iota(jnp.int32, ends[0].shape, 1)
        both = jnp.where(lane % (2 * h) < h, ends[0], ends[1])
        edge = (lane < h) | (lane >= 128 - h)

        def slab(x, carry):
            moved = pltpu.roll(both, 128 - h - 2 * h * x, 1)
            ext[d + x, :, nz : nz + 128] = jnp.where(edge, moved, 0.0)
            return carry

        lax.fori_loop(0, nx, slab, 0)


def exchange(fields, between=None):
    for field in fields:
        field.pack()
        field.start(range(8))
    if between is not None:
        between()
    for field in fields:
        field.finish(range(8))
        field.unpack()
        field.start((8, 9))
    for field in fields:
        field.finish((8, 9))


def pooled(src, pairs, into, after):
    nx, ny, nz = src.shape
    depth = COARSE

    def add(j, carry):
        pairs[j] = src[2 * j] + src[2 * j + 1]
        return carry

    lax.fori_loop(0, nx // 2, add, 0)
    flat = pairs[...].reshape(nx // 2 * ny, nz)

    def halves(rows, cols, dim):
        r = lax.broadcasted_iota(jnp.int32, (rows, cols), dim)
        c = lax.broadcasted_iota(jnp.int32, (rows, cols), 1 - dim)
        return (r == jnp.right_shift(c, 1)).astype(jnp.float32).astype(jnp.bfloat16)

    along_z = halves(nz, nz // 2, 1)
    along_y = halves(nx // 2 * ny // 2, nx // 2 * ny, 0)
    flat = sum(jnp.dot(p, along_z, preferred_element_type=jnp.float32) for p in split3(flat))
    flat = sum(jnp.dot(along_y, p, preferred_element_type=jnp.float32) for p in split3(flat))
    out = after(0.5 * flat).reshape(nx // 2, ny // 2, nz // 2)
    into[depth : depth + nx // 2, : ny // 2, : nz // 2] = out


def cycle_kernel(
    forcing, shift, pressure,
    rhs, inverse, one, two, update, land, crhs, cinverse, cone, ctwo, cupdate, remain, pairs,
    ysend, yrecv, zsend, zrecv, yzrecv, czsend, czrecv, cyzrecv, send_sem, recv_sem,
):
    greet(LINKS)
    nx, ny, nz = forcing.shape

    def fine(k, ext, landing=None):
        return Field(
            ext, FINE, 4, (ysend.at[k], zsend.at[k]), (yrecv.at[k], zrecv.at[k], yzrecv.at[k]),
            send_sem.at[k], recv_sem.at[k], landing,
        )

    def coarse(k, ext):
        return Field(
            ext, COARSE, 8, (None, czsend.at[k]), (None, czrecv.at[k], cyzrecv.at[k]),
            send_sem.at[3 + k], recv_sem.at[3 + k],
        )

    def load(x, carry):
        rhs[FINE + x, :ny, :nz] = forcing[x]
        inverse[FINE + x, :ny, :nz] = 1.0 / (6.0 + shift[x])
        return carry

    lax.fori_loop(0, nx, load, 0)
    pooled(shift, pairs, cinverse, lambda total: 1.0 / (6.0 + total))
    exchange([fine(0, rhs), fine(1, inverse), coarse(0, cinverse)])

    slabs = nx + 2 * FINE
    pairs_of = factors(SMOOTH)
    bufs = (one, two)
    begin(rhs, inverse, one, update, slabs)
    for k in range(1, SMOOTH):
        sweep(rhs, inverse, bufs[(k - 1) % 2], bufs[k % 2], update, k, slabs - k, pairs_of[k])
    smooth = bufs[(SMOOTH - 1) % 2]
    other = bufs[SMOOTH % 2]

    def residual(x, carry):
        cells = smooth[x]
        total = rhs[x] + beside(smooth, x, cells)
        remain[x - FINE] = total[:ny, :nz] - (6.0 + shift[x - FINE]) * cells[:ny, :nz]
        return carry

    lax.fori_loop(FINE, FINE + nx, residual, 0)
    pooled(remain, pairs, crhs, lambda total: total)
    exchange([fine(2, smooth, land), coarse(1, crhs)])

    cslabs = crhs.shape[0]
    pairs_of = factors(COARSE_SMOOTH)
    cbufs = (cone, ctwo)
    begin(crhs, cinverse, cone, cupdate, cslabs)
    for k in range(1, COARSE_SMOOTH):
        sweep(
            crhs, cinverse, cbufs[(k - 1) % 2], cbufs[k % 2], cupdate, k, cslabs - k, pairs_of[k]
        )
    fix = cbufs[(COARSE_SMOOTH - 1) % 2]

    low = COARSE - (FINE + 1) // 2
    count = cslabs - 2 * low
    cny, cnz = fix.shape[1:]
    fny, fnz = smooth.shape[1:]
    flat = fix[low : low + count].reshape(count * cny, cnz)

    def fan(shape, fine_dim, per_f, per_c, core, jump):
        f = lax.broadcasted_iota(jnp.int32, shape, fine_dim)
        c = lax.broadcasted_iota(jnp.int32, shape, 1 - fine_dim)
        block = 0
        for g in range(1, shape[fine_dim] // per_f):
            block = block + (f >= g * per_f).astype(jnp.int32)
        inner = f - block * per_f
        target = jnp.right_shift(inner, 1) + jnp.where(inner >= core, jump, 0) + block * per_c
        return (c == target).astype(jnp.float32).astype(jnp.bfloat16)

    fan_y = fan((count * fny, count * cny), 0, fny, cny, ny + 4, cny - fny // 2)
    fan_z = fan((cnz, fnz), 1, fnz, cnz, nz + 64, cnz - fnz // 2)
    tall = sum(jnp.dot(fan_y, p, preferred_element_type=jnp.float32) for p in split3(flat))
    full = sum(jnp.dot(p, fan_z, preferred_element_type=jnp.float32) for p in split3(tall))
    for j in range(count):
        part = full[j * fny : (j + 1) * fny]
        for half in range(2):
            x = FINE + 2 * (low + j - COARSE) + half
            if 0 <= x < FINE:
                smooth[x] = land[0, x] + part
            elif FINE <= x < FINE + nx:
                smooth[x] = smooth[x] + part
            elif FINE + nx <= x < slabs:
                smooth[x] = land[1, x - FINE - nx] + part

    pairs_of = factors(SMOOTH)
    bufs = (smooth, other)

    def keep(x, cells):
        pressure[x - FINE] = cells[:ny, :nz]

    for k in range(SMOOTH):
        sweep(
            rhs, inverse, bufs[k % 2], bufs[(k + 1) % 2], update,
            k + 1, slabs - k - 1, pairs_of[k], keep if k == SMOOTH - 1 else None,
        )


def cycle(forcing, shift):
    nx, ny, nz = forcing.shape
    cx, cy, cz = nx // 2, ny // 2, nz // 2

    def buf(*shape):
        return pltpu.VMEM(shape, jnp.float32)

    wide = buf(nx + 2 * FINE, ny + 8, nz + 128)
    cwide = buf(cx + 2 * COARSE, cy + 16, cz + 128)
    vmem = pl.BlockSpec(memory_space=pltpu.VMEM)
    return pl.pallas_call(
        cycle_kernel,
        in_specs=[vmem] * 2,
        out_specs=vmem,
        out_shape=jax.ShapeDtypeStruct(forcing.shape, jnp.float32),
        scratch_shapes=[wide] * 5
        + [buf(2, FINE, ny + 8, nz + 128)]
        + [cwide] * 5
        + [buf(nx, ny, nz), buf(cx, ny, nz)]
        + [buf(3, 2, nx // 2, 8, nz)] * 2
        + [buf(3, 2, ny, 128)] * 2
        + [buf(3, 2, 2, 8, 128)]
        + [buf(2, 2, cy, 128)] * 2
        + [buf(2, 2, 2, 8, 128)]
        + [pltpu.SemaphoreType.DMA((5, 10))] * 2,
        compiler_params=pltpu.CompilerParams(
            collective_id=1, has_side_effects=True, vmem_limit_bytes=60 * 2**20
        ),
    )(forcing, shift)


BIN = 256


def hot_rows(index, rows, dtype=jnp.bfloat16):
    r = lax.broadcasted_iota(jnp.int32, (rows, index.shape[1]), 0)
    if rows > BIN:
        return r == index
    return r.astype(jnp.float32).astype(dtype) == index.astype(jnp.float32).astype(dtype)


def points_kernel(
    ndevice, capacity, nbin, pos_ref, nrm_ref, ten_ref, wgt_ref, con_ref, own_ref, cel_ref,
    force_ref, packed_ref, carry_ref,
):
    chunk = 4 * LANES
    nhi = capacity // BIN
    per = packed_ref.shape[0] // ndevice
    cells_per_bin = BIN * BIN
    npoint = ten_ref.shape[1]
    zero = jnp.zeros((), jnp.bfloat16)

    def classes(here):
        return own_ref[:, here] + ndevice * jnp.right_shift(cel_ref[:, here], 16)

    def count(i, total):
        here = pl.ds(pl.multiple_of(i * chunk, chunk), chunk)
        hot = hot_rows(classes(here), nbin * ndevice)
        return total + jnp.sum(jnp.where(hot, 1.0, 0.0).astype(jnp.float32), axis=1, keepdims=True)

    counts = lax.fori_loop(
        0, npoint // chunk, count, jnp.zeros((nbin * ndevice, 1), jnp.float32)
    )
    base = jnp.zeros((ndevice, 1), jnp.float32)
    for b in range(nbin):
        carry_ref[b * ndevice : (b + 1) * ndevice] = base
        base = base + counts[b * ndevice : (b + 1) * ndevice]
    packed_ref[...] = jnp.zeros_like(packed_ref)
    before = (
        lax.broadcasted_iota(jnp.int32, (chunk, chunk), 0)
        < lax.broadcasted_iota(jnp.int32, (chunk, chunk), 1)
    ).astype(jnp.float32).astype(jnp.bfloat16)

    def step(i, carry):
        start = pl.multiple_of(i * chunk, chunk)
        jumps = []
        for sub in range(chunk // LANES):
            base = pl.multiple_of(start + sub * LANES, LANES)
            here = pl.ds(base, LANES)
            lower = pos_ref[:, here]
            upper = pos_ref[:, pl.ds(base + LANES, LANES)]
            centre_pos = jnp.concatenate([lower[:, HALO:], upper[:, :HALO]], axis=1)
            total = jnp.zeros_like(lower)
            for which in range(con_ref.shape[0]):
                index = con_ref[which : which + 1, here] - base
                wide = jnp.broadcast_to(index, lower.shape)
                low = jnp.bitwise_and(wide, LANES - 1)
                near_by = jnp.take_along_axis(lower, low, axis=1, mode="promise_in_bounds")
                far = jnp.take_along_axis(upper, low, axis=1, mode="promise_in_bounds")
                picked = jnp.where(wide < LANES, near_by, far)
                total = total + wgt_ref[which : which + 1, here] * (picked - centre_pos)
            force = ten_ref[:, here] * total[:3]
            force_ref[:, here] = force
            jumps.append(jnp.sum(force * nrm_ref[:, here], axis=0, keepdims=True))
        jump = jnp.concatenate(jumps, axis=1)

        here = pl.ds(start, chunk)
        hot = hot_rows(classes(here), nbin * ndevice)
        ones = jnp.where(hot, jnp.ones((), jnp.bfloat16), zero)
        earlier = jnp.dot(ones, before, preferred_element_type=jnp.float32) + carry_ref[...]
        wide_ones = ones.astype(jnp.float32)
        rank = jnp.sum(wide_ones * earlier, axis=0, keepdims=True).astype(jnp.int32)
        carry_ref[...] = carry_ref[...] + jnp.sum(wide_ones, axis=1, keepdims=True)
        slot = hot_rows(jnp.bitwise_and(rank, BIN - 1), BIN)
        slots = jnp.where(slot, jnp.ones((), jnp.bfloat16), zero)
        row = own_ref[:, here] * per + jnp.right_shift(rank, 8)
        here_value = hot_rows(row, packed_ref.shape[0])
        here_cell = hot_rows(row + per // 2, packed_ref.shape[0])
        cell = cel_ref[:, here] + 1
        total = packed_ref[...]
        for piece, bits in zip(split3(jump), (0, 8, 16)):
            digit = jnp.left_shift(jnp.bitwise_and(jnp.right_shift(cell, bits), 255), bits)
            digit = digit.astype(jnp.float32).astype(jnp.bfloat16)
            left = jnp.where(here_value, piece, jnp.where(here_cell, digit, zero))
            total = total + lax.dot_general(
                left, slots, (((1,), (1,)), ((), ())), preferred_element_type=jnp.float32
            )
        packed_ref[...] = total
        return carry

    lax.fori_loop(0, npoint // chunk, step, 0)


def points(
    padded, normals, tension, edge_weight, relative, owner_ids, cell_map, ndevice, capacity, nbin
):
    npoint = tension.shape[0]
    padded = jnp.concatenate([padded, jnp.zeros((5, padded.shape[1]), jnp.float32)], axis=0)
    per = max(8, 2 * (capacity // BIN))
    vmem = pl.BlockSpec(memory_space=pltpu.VMEM)
    return pl.pallas_call(
        functools.partial(points_kernel, ndevice, capacity, nbin),
        in_specs=[vmem] * 7,
        out_specs=[vmem] * 2,
        out_shape=[
            jax.ShapeDtypeStruct((3, npoint), jnp.float32),
            jax.ShapeDtypeStruct((ndevice * per, BIN), jnp.float32),
        ],
        scratch_shapes=[pltpu.VMEM((nbin * ndevice, 1), jnp.float32)],
        cost_estimate=pl.CostEstimate(
            flops=2 * npoint * capacity * 6 * ndevice, bytes_accessed=40000000, transcendentals=0
        ),
    )(
        padded, normals, tension[None], edge_weight, relative, owner_ids[None], cell_map[None]
    )


GROUP = 8


def scatter_kernel(nbin, rhs_ref, got_ref, out_ref, acc_ref, flat_ref, ends_ref, bound_ref, sem):
    nrow, nz = rhs_ref.shape
    nsource = bound_ref.shape[0]
    per = got_ref.shape[0] // nsource
    chunks = per // 2 * (BIN // LANES)
    rows = nrow // nbin
    nflat = got_ref.shape[0]
    for half in range(BIN // LANES):
        flat_ref[half * nflat : (half + 1) * nflat] = got_ref[:, half * LANES : (half + 1) * LANES]
    got = got_ref[...].reshape(nsource, per, BIN)
    cell_row = lax.broadcasted_iota(jnp.int32, got.shape, 1) >= per // 2
    used = cell_row & (got > 0.0)
    lane = lax.broadcasted_iota(jnp.int32, (nsource, LANES), 1)
    ends = jnp.zeros((nsource, LANES), jnp.float32)
    for b in range(nbin):
        inside = jnp.where(used & (got <= float((b + 1) * BIN * BIN)), 1.0, 0.0)
        total = jnp.sum(jnp.sum(inside, axis=1), axis=1, keepdims=True)
        ends = jnp.where(lane == b + 1, total, ends)
    ends_ref[...] = ends.astype(jnp.int32)
    copy = pltpu.make_async_copy(ends_ref, bound_ref, sem)
    copy.start()
    copy.wait()
    level = lax.broadcasted_iota(jnp.int32, (BIN, LANES), 0).astype(jnp.float32)
    level = level.astype(jnp.bfloat16)
    zero, unit = jnp.zeros((), jnp.bfloat16), jnp.ones((), jnp.bfloat16)

    def quarter(b, carry):
        def span(source):
            at = jnp.minimum(source, nsource - 1)
            first = jnp.minimum(jnp.right_shift(bound_ref[at, b], 7), chunks - 1)
            last = jnp.right_shift(bound_ref[at, b + 1] + LANES - 1, 7)
            return first, jnp.maximum(last, first + 1)

        acc_ref[...] = jnp.zeros_like(acc_ref)

        def work(state):
            source, chunk, last = state
            highs, lows, cols = [], [], []
            for _ in range(GROUP):
                at = jnp.minimum(source, nsource - 1)
                row = jnp.bitwise_and(chunk, 1) * nflat + at * per + jnp.right_shift(chunk, 1)
                value = flat_ref[pl.ds(row, 1)]
                cell = flat_ref[pl.ds(row + per // 2, 1)].astype(jnp.int32) - 1
                fits = (jnp.right_shift(cell, 16) == b) & (source < nsource)
                half = jnp.bitwise_and(jnp.right_shift(cell, 8), 1)
                place = half * rows + jnp.bitwise_and(jnp.right_shift(cell, 9), rows - 1)
                place = jnp.where(fits, place, BIN).astype(jnp.float32).astype(jnp.bfloat16)
                col = jnp.bitwise_and(cell, BIN - 1).astype(jnp.float32).astype(jnp.bfloat16)
                first = value.astype(jnp.bfloat16)
                second = (value - first.astype(jnp.float32)).astype(jnp.bfloat16)
                same = level == place
                highs.append(jnp.where(same, first, zero))
                lows.append(jnp.where(same, second, zero))
                cols.append(jnp.where(level == col, unit, zero))
                over = chunk + 1 >= last
                source = jnp.where(over, source + 1, source)
                following = span(source)
                chunk = jnp.where(over, following[0], chunk + 1)
                last = jnp.where(over, following[1], last)
            high = jnp.concatenate(highs, axis=1)
            low = jnp.concatenate(lows, axis=1)
            right = jnp.concatenate(cols, axis=1)
            dims = (((1,), (1,)), ((), ()))
            acc_ref[...] += lax.dot_general(
                high, right, dims, preferred_element_type=jnp.float32
            ) + lax.dot_general(low, right, dims, preferred_element_type=jnp.float32)
            return source, chunk, last

        lax.while_loop(lambda state: state[0] < nsource, work, (jnp.int32(0), *span(0)))
        here = pl.ds(pl.multiple_of(b * rows, rows), rows)
        for half in range(2):
            cols = slice(half * BIN, (half + 1) * BIN)
            out_ref[here, cols] = rhs_ref[here, cols] + acc_ref[half * rows : (half + 1) * rows]
        return carry

    lax.fori_loop(0, nbin, quarter, 0)


def scatter(rhs, got, nsource, nbin):
    nx, ny, nz = rhs.shape
    nrow = nx * ny
    vmem = pl.BlockSpec(memory_space=pltpu.VMEM)
    out = pl.pallas_call(
        functools.partial(scatter_kernel, nbin),
        in_specs=[vmem] * 2,
        out_specs=vmem,
        out_shape=jax.ShapeDtypeStruct((nrow, nz), jnp.float32),
        scratch_shapes=[
            pltpu.VMEM((BIN, BIN), jnp.float32),
            pltpu.VMEM((got.size // LANES, LANES), jnp.float32),
            pltpu.VMEM((nsource, LANES), jnp.int32),
            pltpu.SMEM((nsource, LANES), jnp.int32),
            pltpu.SemaphoreType.DMA,
        ],
        cost_estimate=pl.CostEstimate(
            flops=4 * nrow * nz * got.size // 4, bytes_accessed=4000000, transcendentals=0
        ),
    )(rhs.reshape(nrow, nz), got)
    return out.reshape(nx, ny, nz)


def body(
    pressure_rhs,
    shift_diag,
    positions,
    normals,
    tension,
    edge_weight,
    owner_map,
    cell_map,
    connectivity,
):
    npoint = positions.shape[1]
    ndevice = lax.axis_size(("gx", "gy", "gz"))
    total = npoint * ndevice
    begin = lax.axis_index(("gx", "gy", "gz")) * npoint
    padded = padded_2(positions, ((("gx", "gy", "gz"), 1, HALO),), True)
    relative = (connectivity - begin + HALO + total) % total
    capacity = 4 * npoint // ndevice
    nbin = pressure_rhs.size // (BIN * BIN)
    surface_force, packed = points(
        padded, normals, tension, edge_weight, relative, owner_map[:, 0], cell_map,
        ndevice, capacity, nbin,
    )
    got = lax.all_to_all(packed, ("gx", "gy", "gz"), split_axis=0, concat_axis=0, tiled=True)
    forcing = scatter(pressure_rhs, got, ndevice, nbin)
    pressure = cycle(forcing, shift_diag)
    return (pressure, surface_force)


def solution(mesh):
    return jax.shard_map(
        body,
        mesh=mesh,
        in_specs=(
            P("gx", "gy", "gz"),
            P("gx", "gy", "gz"),
            P(None, ("gx", "gy", "gz")),
            P(None, ("gx", "gy", "gz")),
            P(("gx", "gy", "gz")),
            P(None, ("gx", "gy", "gz")),
            P(("gx", "gy", "gz"), None),
            P(("gx", "gy", "gz")),
            P(None, ("gx", "gy", "gz")),
        ),
        out_specs=(P("gx", "gy", "gz"), P(None, ("gx", "gy", "gz"))),
        check_vma=False,
    )
```

```python
import functools

import jax
import jax.numpy as jnp
from jax import lax
from jax.experimental import pallas as pl
from jax.experimental.pallas import tpu as pltpu
from jax.sharding import PartitionSpec as P

HALO = 64
SMOOTH = 3
COARSE_SMOOTH = 4
LANES = 2 * HALO


centre = 1.125
spread = 0.875


def factors(sweeps):
    ratio = centre / spread
    fac = 1.0 / ratio
    pairs = [(0.0, 1.0 / centre)]
    for _ in range(1, sweeps):
        fac_new = 1.0 / (2.0 * ratio - fac)
        pairs.append((fac_new * fac, 2.0 * fac_new / spread))
        fac = fac_new
    return pairs


def split3(x):
    a = x.astype(jnp.bfloat16)
    rest = x - a.astype(jnp.float32)
    b = rest.astype(jnp.bfloat16)
    c = (rest - b.astype(jnp.float32)).astype(jnp.bfloat16)
    return a, b, c


MESH = pl.DeviceIdType.MESH
FINE = SMOOTH
COARSE = COARSE_SMOOTH - 1 + (SMOOTH + 1) // 2


UNROLL = 4
VMEM_LIMIT = 36 * 2**20


def around(src, x, r):
    ny, nz = src.shape[1:]
    sub = lax.broadcasted_iota(jnp.int32, (8, nz), 0)
    here = slice(r, r + 8)
    below, above = (r - 8) % ny, (r + 8) % ny
    cells = src[x, here]
    total = src[x - 1, here] + src[x + 1, here]
    total = total + (
        pltpu.roll(jnp.where(sub == 7, src[x, below : below + 8], cells), 1, 0)
        + pltpu.roll(jnp.where(sub == 0, src[x, above : above + 8], cells), 7, 0)
    )
    return cells, total + (pltpu.roll(cells, 1, 1) + pltpu.roll(cells, nz - 1, 1))


def sweep(rhs, inverse, src, dst, update, first, last, pair, keep=None):
    old, new = pair
    rows = src.shape[1] if keep is None else keep.shape[1]

    def slab(x, carry):
        for r in range(0, rows, 8):
            here = slice(r, r + 8)
            cells, total = around(src, x, r)
            change = new * (inverse[x, here] * (rhs[x, here] + total) - cells)
            if old:
                change = change + old * update[x, here]
            if keep is None:
                update[x, here] = change
                dst[x, here] = cells + change
            else:
                keep[x - first, here] = (cells + change)[:, : keep.shape[2]]
        return carry

    lax.fori_loop(first, last, slab, 0, unroll=UNROLL)


def begin(rhs, inverse, dst, update, slabs):
    def slab(x, carry):
        change = inverse[x] * rhs[x] * (1.0 / centre)
        update[x] = change
        dst[x] = change
        return carry

    lax.fori_loop(0, slabs, slab, 0, unroll=2)


def near(axes):
    ok = None
    where = {}
    for axis, step in axes:
        place = lax.axis_index(axis) + step
        fits = (place >= 0) & (place < lax.axis_size(axis))
        ok = fits if ok is None else ok & fits
        where[axis] = place
    return ok, where


SIDES = (-1, 1)
LINKS = (
    [(("gy", a),) for a in SIDES]
    + [(("gz", b),) for b in SIDES]
    + [(("gy", a), ("gz", b)) for b in SIDES for a in SIDES]
    + [(("gx", a),) for a in SIDES]
)
MIRROR = [1, 0, 3, 2, 7, 6, 5, 4, 9, 8]


def greet(links):
    barrier = pltpu.get_barrier_semaphore()
    peers = 0
    for link in links:
        ok, where = near(link)
        peers = peers + ok.astype(jnp.int32)

        @pl.when(ok)
        def _():
            pl.semaphore_signal(barrier, inc=1, device_id=where, device_id_type=MESH)

    pl.semaphore_wait(barrier, peers)


class Field:
    def __init__(self, ext, depth, wide, send, recv, send_sem, recv_sem, land=None):
        self.ext, self.depth, self.wide = ext, depth, wide
        self.send, self.recv = send, recv
        self.send_sem, self.recv_sem = send_sem, recv_sem
        self.land = land
        self.nx = ext.shape[0] - 2 * depth
        self.ny = ext.shape[1] - 2 * wide
        self.nz = ext.shape[2] - 128

    def message(self, m):
        d, nx, ny, nz, h = self.depth, self.nx, self.ny, self.nz, self.wide
        ext = self.ext
        if m < 2:
            if h == 8:
                rows = (0, ny - h)[m]
                src = ext.at[pl.ds(d, nx), pl.ds(rows, h), pl.ds(0, nz)]
                place = (ny + h, ny)[m]
                got = ext.at[pl.ds(d, nx), pl.ds(place, h), pl.ds(0, nz)]
                other = ext.at[pl.ds(d, nx), pl.ds((ny, ny + h)[m], h), pl.ds(0, nz)]
            else:
                src = self.send[0].at[m]
                got = self.recv[0].at[m]
                other = self.recv[0].at[1 - m]
        elif m < 4:
            src = self.send[1].at[m - 2]
            got = self.recv[1].at[m - 2]
            other = self.recv[1].at[3 - m]
        elif m < 8:
            b, a = divmod(m - 4, 2)
            src = self.send[1].at[b, pl.ds((0, ny - 8)[a], 8)]
            got = self.recv[2].at[b, a]
            other = self.recv[2].at[1 - b, 1 - a]
        else:
            a = m - 8
            src = ext.at[pl.ds((d, nx)[a], d)]
            if self.land is None:
                got = ext.at[pl.ds((0, d + nx)[a], d)]
                other = ext.at[pl.ds((d + nx, 0)[a], d)]
            else:
                got = self.land.at[a]
                other = self.land.at[1 - a]
        return src, other, got

    def copy(self, m, incoming):
        src, other, got = self.message(m)
        k = m if incoming else MIRROR[m]
        return pltpu.make_async_remote_copy(
            src_ref=got if incoming else src,
            dst_ref=got if incoming else other,
            send_sem=self.send_sem.at[m],
            recv_sem=self.recv_sem.at[k],
            device_id=near(LINKS[m])[1],
            device_id_type=MESH,
        )

    def start(self, which):
        for m in which:
            @pl.when(near(LINKS[m])[0])
            def _():
                self.copy(m, False).start()

    def finish(self, which):
        for m in which:
            ok = near(LINKS[m])[0]

            @pl.when(ok)
            def _():
                self.copy(m, False).wait_send()
                self.copy(m, True).wait_recv()

            @pl.when(jnp.logical_not(ok))
            def _():
                got = self.message(m)[2]
                got[...] = jnp.zeros(got.shape, jnp.float32)

    def pack(self):
        d, nx, ny, nz, h = self.depth, self.nx, self.ny, self.nz, self.wide
        ext = self.ext
        if h != 8:
            for x in range(nx):
                at = slice(d * (x % 8), d * (x % 8) + d)
                self.send[0][0, x // 8, at] = ext[d + x, :d, :nz]
                self.send[0][1, x // 8, at] = ext[d + x, ny - d : ny, :nz]
        group = lax.broadcasted_iota(jnp.int32, (ny, 128), 1) // (2 * h)

        def slab(x, carry):
            low, high = carry
            mine = group == x
            shift = 2 * h * x + h
            low = jnp.where(mine, pltpu.roll(ext[d + x, :ny, :128], shift, 1), low)
            high = jnp.where(mine, pltpu.roll(ext[d + x, :ny, nz - 128 : nz], shift, 1), high)
            return low, high

        zero = jnp.zeros((ny, 128), jnp.float32)
        low, high = lax.fori_loop(0, nx, slab, (zero, zero), unroll=8)
        self.send[1][0] = low
        self.send[1][1] = high

    def unpack(self):
        d, nx, ny, nz, h = self.depth, self.nx, self.ny, self.nz, self.wide
        ext = self.ext
        if h != 8:
            for x in range(nx):
                at = slice(d * (x % 8), d * (x % 8) + d)
                ext[d + x, ny : ny + d, :nz] = self.recv[0][1, x // 8, at]
                ext[d + x, ny + 8 - d : ny + 8, :nz] = self.recv[0][0, x // 8, at]
        ends = []
        for b in range(2):
            corner = (self.recv[2][b, 1], self.recv[2][b, 0])
            if h == 8:
                ends.append(jnp.concatenate([self.recv[1][b], *corner], axis=0))
            else:
                sub = lax.broadcasted_iota(jnp.int32, (8, 128), 0)
                ends.append(
                    jnp.concatenate([self.recv[1][b], jnp.where(sub < h, *corner)], axis=0)
                )
        lane = lax.broadcasted_iota(jnp.int32, ends[0].shape, 1)
        both = jnp.where(lane % (2 * h) < h, ends[0], ends[1])
        edge = (lane < h) | (lane >= 128 - h)

        def slab(x, carry):
            moved = pltpu.roll(both, 128 - h - 2 * h * x, 1)
            ext[d + x, :, nz : nz + 128] = jnp.where(edge, moved, 0.0)
            return carry

        lax.fori_loop(0, nx, slab, 0, unroll=8)


def pair_up(src, pairs):
    def add(j, carry):
        pairs[j] = src[2 * j] + src[2 * j + 1]
        return carry

    lax.fori_loop(0, pairs.shape[0], add, 0)


def pooled(pairs, into, after):
    cx, ny, nz = pairs.shape
    depth = COARSE
    flat = pairs[...].reshape(cx * ny, nz)

    def halves(rows, cols, dim):
        r = lax.broadcasted_iota(jnp.int32, (rows, cols), dim)
        c = lax.broadcasted_iota(jnp.int32, (rows, cols), 1 - dim)
        return (r == jnp.right_shift(c, 1)).astype(jnp.float32).astype(jnp.bfloat16)

    along_z = halves(nz, nz // 2, 1)
    along_y = halves(cx * ny // 2, cx * ny, 0)
    flat = sum(jnp.dot(p, along_z, preferred_element_type=jnp.float32) for p in split3(flat))
    flat = sum(jnp.dot(along_y, p, preferred_element_type=jnp.float32) for p in split3(flat))
    out = after(0.5 * flat).reshape(cx, ny // 2, nz // 2)
    into[depth : depth + cx, : ny // 2, : nz // 2] = out


def fine_field(ext, bufs, sems, landing=None):
    ysend, yrecv, zsend, zrecv, yzrecv = bufs
    return Field(ext, FINE, 4, (ysend, zsend), (yrecv, zrecv, yzrecv), *sems, landing)


def coarse_field(ext, bufs, sems):
    zsend, zrecv, yzrecv = bufs
    return Field(ext, COARSE, 8, (None, zsend), (None, zrecv, yzrecv), *sems)


def buf(*shape):
    return pltpu.VMEM(shape, jnp.float32)


def wide_shapes(nx, ny, nz):
    cx, cy, cz = nx // 2, ny // 2, nz // 2
    return (
        (nx + 2 * FINE, ny + 8, nz + 128),
        (cx + 2 * COARSE, cy + 16, cz + 128),
    )


def fine_scratch(nx, ny, nz):
    rows = (2, nx // 8, 8 * FINE, nz)
    return [buf(*rows)] * 2 + [buf(2, ny, 128)] * 2 + [buf(2, 2, 8, 128)]


def coarse_scratch(nx, ny, nz):
    return [buf(2, ny // 2, 128)] * 2 + [buf(2, 2, 8, 128)]


FIRST, LAST = range(8), (8, 9)


def cycle_kernel(forcing, shift, inverse, cinverse, pressure, *scratch):
    (rhs, one, two, update, land, crhs, cone, ctwo, cupdate, pairs), scratch = (
        scratch[:10], scratch[10:],
    )
    bufs_a, bufs_b, bufs_c = scratch[:5], scratch[5:10], scratch[10:13]
    send_sem, recv_sem = scratch[13:]
    nx, ny, nz = forcing.shape
    sems = [(send_sem.at[k], recv_sem.at[k]) for k in range(3)]

    def load(x, carry):
        rhs[FINE + x, :ny, :nz] = forcing[x]
        return carry

    lax.fori_loop(0, nx, load, 0, unroll=2)
    field = fine_field(rhs, bufs_a, sems[0])
    field.pack()
    greet(LINKS)
    field.start(FIRST)
    field.finish(FIRST)
    field.unpack()
    field.start(LAST)
    field.finish(LAST)

    slabs = nx + 2 * FINE
    pairs_of = factors(SMOOTH)
    bufs = (one, two)
    begin(rhs, inverse, one, update, slabs)
    for k in range(1, SMOOTH):
        sweep(rhs, inverse, bufs[(k - 1) % 2], bufs[k % 2], update, k, slabs - k, pairs_of[k])
    smooth = bufs[(SMOOTH - 1) % 2]
    other = bufs[SMOOTH % 2]

    def residual(j, carry):
        for r in range(0, ny, 8):
            here = slice(r, r + 8)
            both = 0.0
            for half in range(2):
                x = 2 * j + half
                cells, total = around(smooth, FINE + x, r)
                total = total[:, :nz] + rhs[FINE + x, here, :nz]
                both = both + (total - (6.0 + shift[x, here]) * cells[:, :nz])
            pairs[j, here] = both
        return carry

    lax.fori_loop(0, nx // 2, residual, 0, unroll=2)
    pooled(pairs, crhs, lambda total: total)
    coarse = coarse_field(crhs, bufs_c, sems[2])
    coarse.pack()
    coarse.start(FIRST)
    field = fine_field(smooth, bufs_b, sems[1], land)
    field.pack()
    field.start(FIRST)
    cslabs = crhs.shape[0]
    low = COARSE - (FINE + 1) // 2
    count = cslabs - 2 * low
    cny, cnz = crhs.shape[1:]
    fny, fnz = smooth.shape[1:]

    def fan(shape, fine_dim, per_f, per_c, core, jump):
        f = lax.broadcasted_iota(jnp.int32, shape, fine_dim)
        c = lax.broadcasted_iota(jnp.int32, shape, 1 - fine_dim)
        block = 0
        for g in range(1, shape[fine_dim] // per_f):
            block = block + (f >= g * per_f).astype(jnp.int32)
        inner = f - block * per_f
        target = jnp.right_shift(inner, 1) + jnp.where(inner >= core, jump, 0) + block * per_c
        return (c == target).astype(jnp.float32).astype(jnp.bfloat16)

    fan_y = fan((count * fny, count * cny), 0, fny, cny, ny + 4, cny - fny // 2)
    fan_z = fan((cnz, fnz), 1, fnz, cnz, nz + 64, cnz - fnz // 2)
    coarse.finish(FIRST)
    coarse.unpack()
    coarse.start(LAST)
    field.finish(FIRST)
    field.unpack()
    field.start(LAST)
    coarse.finish(LAST)

    pairs_of = factors(COARSE_SMOOTH)
    cbufs = (cone, ctwo)
    begin(crhs, cinverse, cone, cupdate, cslabs)
    for k in range(1, COARSE_SMOOTH):
        sweep(
            crhs, cinverse, cbufs[(k - 1) % 2], cbufs[k % 2], cupdate, k, cslabs - k, pairs_of[k]
        )
    fix = cbufs[(COARSE_SMOOTH - 1) % 2]

    field.finish(LAST)
    flat = fix[low : low + count].reshape(count * cny, cnz)

    tall = sum(jnp.dot(fan_y, p, preferred_element_type=jnp.float32) for p in split3(flat))
    full = sum(jnp.dot(p, fan_z, preferred_element_type=jnp.float32) for p in split3(tall))
    for j in range(count):
        part = full[j * fny : (j + 1) * fny]
        for half in range(2):
            x = FINE + 2 * (low + j - COARSE) + half
            if 0 <= x < FINE:
                smooth[x] = land[0, x] + part
            elif FINE <= x < FINE + nx:
                smooth[x] = smooth[x] + part
            elif FINE + nx <= x < slabs:
                smooth[x] = land[1, x - FINE - nx] + part

    pairs_of = factors(SMOOTH)
    bufs = (smooth, other)

    for k in range(SMOOTH):
        sweep(
            rhs, inverse, bufs[k % 2], bufs[(k + 1) % 2], update,
            k + 1, slabs - k - 1, pairs_of[k], pressure if k == SMOOTH - 1 else None,
        )


def cycle(forcing, shift, inverse, cinverse):
    nx, ny, nz = forcing.shape
    wide, cwide = (buf(*shape) for shape in wide_shapes(nx, ny, nz))
    vmem = pl.BlockSpec(memory_space=pltpu.VMEM)
    return pl.pallas_call(
        cycle_kernel,
        in_specs=[vmem] * 4,
        out_specs=vmem,
        out_shape=jax.ShapeDtypeStruct(forcing.shape, jnp.float32),
        scratch_shapes=[wide] * 4
        + [buf(2, FINE, ny + 8, nz + 128)]
        + [cwide] * 4
        + [buf(nx // 2, ny, nz)]
        + fine_scratch(nx, ny, nz) * 2
        + coarse_scratch(nx, ny, nz)
        + [pltpu.SemaphoreType.DMA((3, 10))] * 2,
        compiler_params=pltpu.CompilerParams(
            collective_id=1, has_side_effects=True, vmem_limit_bytes=VMEM_LIMIT
        ),
    )(forcing, shift, inverse, cinverse)


BIN = 256
AXES = ("gx", "gy", "gz")


def hot_rows(index, rows, dtype=jnp.bfloat16):
    r = lax.broadcasted_iota(jnp.int32, (rows, index.shape[1]), 0)
    if rows > BIN:
        return r == index
    return r.astype(jnp.float32).astype(dtype) == index.astype(jnp.float32).astype(dtype)


def place_of(index):
    where = {}
    for axis in reversed(AXES):
        count = lax.axis_size(axis)
        where[axis] = lax.rem(index, count)
        index = lax.div(index, count)
    return where


def front_kernel(
    ndevice, capacity, nbin, pos_ref, nrm_ref, ten_ref, wgt_ref, con_ref, own_ref, cel_ref, shift,
    force_ref, got_ref, inverse, cinverse, *scratch,
):
    (packed_ref, carry_ref, rank_ref, jump_ref, pad_ref, psend, precv, pairs), scratch = (
        scratch[:8], scratch[8:],
    )
    fine_bufs, coarse_bufs = scratch[:5], scratch[5:8]
    send_sem, recv_sem, all_send, all_recv, pos_send, pos_recv = scratch[8:]
    chunk = 4 * LANES
    per = packed_ref.shape[0] // ndevice
    npoint = ten_ref.shape[1]
    nx, ny, nz = shift.shape
    zero, unit = jnp.zeros((), jnp.bfloat16), jnp.ones((), jnp.bfloat16)
    me = lax.axis_index(AXES)
    barrier = pltpu.get_barrier_semaphore()

    def other(p):
        return lax.rem(me + p, ndevice)

    def hello(p, carry):
        pl.semaphore_signal(barrier, inc=1, device_id=place_of(other(p)), device_id_type=MESH)
        return carry

    lax.fori_loop(1, ndevice, hello, 0)

    def load(x, carry):
        inverse[FINE + x, :ny, :nz] = 1.0 / (6.0 + shift[x])
        return carry

    lax.fori_loop(0, nx, load, 0, unroll=2)
    pair_up(shift, pairs)
    pooled(pairs, cinverse, lambda total: 1.0 / (6.0 + total))
    fine = fine_field(inverse, fine_bufs, (send_sem.at[0], recv_sem.at[0]))
    coarse = coarse_field(cinverse, coarse_bufs, (send_sem.at[1], recv_sem.at[1]))
    fine.pack()
    coarse.pack()
    psend[0, :3] = pos_ref[:, npoint - LANES :]
    psend[1, :3] = pos_ref[:, :LANES]

    def spread_out(j, carry):
        lower = pos_ref[:, pl.ds(pl.multiple_of(j * LANES - LANES, LANES), LANES)]
        upper = pos_ref[:, pl.ds(pl.multiple_of(j * LANES, LANES), LANES)]
        both = jnp.concatenate([lower[:, HALO:], upper[:, :HALO]], axis=1)
        pad_ref[:3, pl.ds(pl.multiple_of(j * LANES, LANES), LANES)] = both
        return carry

    lax.fori_loop(1, npoint // LANES, spread_out, 0, unroll=7)

    pl.semaphore_wait(barrier, ndevice - 1)

    def edge(side, incoming):
        return pltpu.make_async_remote_copy(
            src_ref=psend.at[side],
            dst_ref=precv.at[side],
            send_sem=pos_send.at[side],
            recv_sem=pos_recv.at[side],
            device_id=place_of(other((1, ndevice - 1)[side])),
            device_id_type=MESH,
        )

    for side in range(2):
        edge(side, False).start()
    fine.start(FIRST)
    coarse.start(FIRST)

    def classes(here):
        return own_ref[:, here] + ndevice * jnp.right_shift(cel_ref[:, here], 16)

    def count(i, total):
        here = pl.ds(pl.multiple_of(i * chunk, chunk), chunk)
        hot = jnp.where(hot_rows(classes(here), nbin * ndevice), 1.0, 0.0).astype(jnp.float32)
        return total + (
            hot[:, :LANES] + hot[:, LANES : 2 * LANES]
            + (hot[:, 2 * LANES : 3 * LANES] + hot[:, 3 * LANES :])
        )

    counts = lax.fori_loop(
        0, npoint // chunk, count, jnp.zeros((nbin * ndevice, LANES), jnp.float32), unroll=2
    )
    counts = jnp.sum(counts, axis=1, keepdims=True)
    base = jnp.zeros((ndevice, 1), jnp.float32)
    for b in range(nbin):
        carry_ref[b * ndevice : (b + 1) * ndevice] = base
        base = base + counts[b * ndevice : (b + 1) * ndevice]
    before = (
        lax.broadcasted_iota(jnp.int32, (chunk, chunk), 0)
        < lax.broadcasted_iota(jnp.int32, (chunk, chunk), 1)
    ).astype(jnp.float32).astype(jnp.bfloat16)

    def order(i, carry):
        here = pl.ds(pl.multiple_of(i * chunk, chunk), chunk)
        ones = jnp.where(hot_rows(classes(here), nbin * ndevice), unit, zero)
        earlier = jnp.dot(ones, before, preferred_element_type=jnp.float32) + carry
        wide = ones.astype(jnp.float32)
        rank_ref[:, here] = jnp.sum(wide * earlier, axis=0, keepdims=True).astype(jnp.int32)
        return carry + jnp.sum(wide, axis=1, keepdims=True)

    lax.fori_loop(0, npoint // chunk, order, carry_ref[...], unroll=2)

    for side in range(2):
        edge(side, True).wait_send()
        edge(side, True).wait_recv()
    pad_ref[:3, :LANES] = jnp.concatenate(
        [precv[0, :3, HALO:], pos_ref[:, :HALO]], axis=1
    )
    pad_ref[:3, npoint:] = jnp.concatenate(
        [pos_ref[:, npoint - HALO :], precv[1, :3, :HALO]], axis=1
    )
    begin_at = me * npoint
    everything = npoint * ndevice

    def pull(i, carry):
        for sub in range(2):
            base = pl.multiple_of(i * 2 * LANES + sub * LANES, LANES)
            here = pl.ds(base, LANES)
            lower = pad_ref[:, here]
            upper = pad_ref[:, pl.ds(base + LANES, LANES)]
            centre_pos = jnp.concatenate([lower[:, HALO:], upper[:, :HALO]], axis=1)
            index = con_ref[:, here] - begin_at + HALO
            index = jnp.where(index < 0, index + everything, index)
            index = jnp.where(index >= everything, index - everything, index) - base
            total = jnp.zeros_like(lower)
            for which in range(con_ref.shape[0]):
                wide = jnp.broadcast_to(index[which : which + 1], lower.shape)
                low = jnp.bitwise_and(wide, LANES - 1)
                near_by = jnp.take_along_axis(lower, low, axis=1, mode="promise_in_bounds")
                far = jnp.take_along_axis(upper, low, axis=1, mode="promise_in_bounds")
                picked = jnp.where(wide < LANES, near_by, far)
                total = total + wgt_ref[which : which + 1, here] * (picked - centre_pos)
            force = ten_ref[:, here] * total[:3]
            force_ref[:, here] = force
            jump_ref[:, here] = jnp.sum(force * nrm_ref[:, here], axis=0, keepdims=True)
        return carry

    lax.fori_loop(0, npoint // (2 * LANES), pull, 0, unroll=2)

    fine.finish(FIRST)
    fine.unpack()
    fine.start(LAST)
    coarse.finish(FIRST)
    coarse.unpack()
    coarse.start(LAST)

    packed_ref[...] = jnp.zeros_like(packed_ref)

    def pack(i, carry):
        here = pl.ds(pl.multiple_of(i * chunk, chunk), chunk)
        rank = rank_ref[:, here]
        slots = jnp.where(hot_rows(jnp.bitwise_and(rank, BIN - 1), BIN), unit, zero)
        row = own_ref[:, here] * per + jnp.right_shift(rank, 8)
        here_value = hot_rows(row, packed_ref.shape[0])
        here_cell = hot_rows(row + per // 2, packed_ref.shape[0])
        cell = cel_ref[:, here] + 1
        total = packed_ref[...]
        for piece, bits in zip(split3(jump_ref[:, here]), (0, 8, 16)):
            digit = jnp.left_shift(jnp.bitwise_and(jnp.right_shift(cell, bits), 255), bits)
            digit = digit.astype(jnp.float32).astype(jnp.bfloat16)
            left = jnp.where(here_value, piece, jnp.where(here_cell, digit, zero))
            total = total + lax.dot_general(
                left, slots, (((1,), (1,)), ((), ())), preferred_element_type=jnp.float32
            )
        packed_ref[...] = total
        return carry

    lax.fori_loop(0, npoint // chunk, pack, 0, unroll=2)

    def rows_of(device):
        return pl.ds(pl.multiple_of(device * per, per), per)

    def deal(p, incoming):
        return pltpu.make_async_remote_copy(
            src_ref=packed_ref.at[rows_of(other(p))],
            dst_ref=got_ref.at[rows_of(other(ndevice - p) if incoming else me)],
            send_sem=all_send.at[p],
            recv_sem=all_recv.at[p],
            device_id=place_of(other(p)),
            device_id_type=MESH,
        )

    def send(p, carry):
        deal(p, False).start()
        return carry

    lax.fori_loop(1, ndevice, send, 0)
    got_ref[rows_of(me)] = packed_ref[rows_of(me)]
    fine.finish(LAST)
    coarse.finish(LAST)

    def receive(p, carry):
        deal(p, False).wait_send()
        deal(p, True).wait_recv()
        return carry

    lax.fori_loop(1, ndevice, receive, 0)


def front(
    positions, normals, tension, edge_weight, connectivity, owner_ids, cell_map, shift,
    ndevice, capacity, nbin,
):
    npoint = tension.shape[0]
    nx, ny, nz = shift.shape
    per = max(8, 2 * (capacity // BIN))
    vmem = pl.BlockSpec(memory_space=pltpu.VMEM)
    wide, cwide = wide_shapes(nx, ny, nz)
    return pl.pallas_call(
        functools.partial(front_kernel, ndevice, capacity, nbin),
        in_specs=[vmem] * 8,
        out_specs=[vmem] * 4,
        out_shape=[
            jax.ShapeDtypeStruct(shape, jnp.float32)
            for shape in ((3, npoint), (ndevice * per, BIN), wide, cwide)
        ],
        scratch_shapes=[
            buf(ndevice * per, BIN),
            buf(nbin * ndevice, 1),
            pltpu.VMEM((1, npoint), jnp.int32),
            buf(1, npoint),
            buf(8, npoint + LANES),
            buf(2, 8, LANES),
            buf(2, 8, LANES),
            buf(nx // 2, ny, nz),
        ]
        + fine_scratch(nx, ny, nz)
        + coarse_scratch(nx, ny, nz)
        + [pltpu.SemaphoreType.DMA((2, 10))] * 2
        + [pltpu.SemaphoreType.DMA((ndevice,))] * 2
        + [pltpu.SemaphoreType.DMA((2,))] * 2,
        compiler_params=pltpu.CompilerParams(
            collective_id=0, has_side_effects=True, vmem_limit_bytes=VMEM_LIMIT
        ),
    )(
        positions, normals, tension[None], edge_weight, connectivity, owner_ids[None],
        cell_map[None], shift,
    )


GROUP = 8


def scatter_kernel(nbin, rhs_ref, got_ref, out_ref, acc_ref, flat_ref, ends_ref, bound_ref, sem):
    nrow, nz = rhs_ref.shape
    nsource = bound_ref.shape[0]
    per = got_ref.shape[0] // nsource
    chunks = per // 2 * (BIN // LANES)
    rows = nrow // nbin
    nflat = got_ref.shape[0]
    for half in range(BIN // LANES):
        flat_ref[half * nflat : (half + 1) * nflat] = got_ref[:, half * LANES : (half + 1) * LANES]
    got = got_ref[...].reshape(nsource, per, BIN)
    cell_row = lax.broadcasted_iota(jnp.int32, got.shape, 1) >= per // 2
    used = cell_row & (got > 0.0)
    lane = lax.broadcasted_iota(jnp.int32, (nsource, LANES), 1)
    ends = jnp.zeros((nsource, LANES), jnp.float32)
    for b in range(nbin):
        inside = jnp.where(used & (got <= float((b + 1) * BIN * BIN)), 1.0, 0.0)
        total = jnp.sum(jnp.sum(inside, axis=1), axis=1, keepdims=True)
        ends = jnp.where(lane == b + 1, total, ends)
    ends_ref[...] = ends.astype(jnp.int32)
    copy = pltpu.make_async_copy(ends_ref, bound_ref, sem)
    copy.start()
    copy.wait()
    level = lax.broadcasted_iota(jnp.int32, (BIN, LANES), 0).astype(jnp.float32)
    level = level.astype(jnp.bfloat16)
    zero, unit = jnp.zeros((), jnp.bfloat16), jnp.ones((), jnp.bfloat16)

    def quarter(b, carry):
        def span(source):
            at = jnp.minimum(source, nsource - 1)
            first = jnp.minimum(jnp.right_shift(bound_ref[at, b], 7), chunks - 1)
            last = jnp.right_shift(bound_ref[at, b + 1] + LANES - 1, 7)
            return first, jnp.maximum(last, first + 1)

        acc_ref[...] = jnp.zeros_like(acc_ref)

        def work(state):
            source, chunk, last = state
            highs, lows, cols = [], [], []
            for _ in range(GROUP):
                at = jnp.minimum(source, nsource - 1)
                row = jnp.bitwise_and(chunk, 1) * nflat + at * per + jnp.right_shift(chunk, 1)
                value = flat_ref[pl.ds(row, 1)]
                cell = flat_ref[pl.ds(row + per // 2, 1)].astype(jnp.int32) - 1
                fits = (jnp.right_shift(cell, 16) == b) & (source < nsource)
                half = jnp.bitwise_and(jnp.right_shift(cell, 8), 1)
                place = half * rows + jnp.bitwise_and(jnp.right_shift(cell, 9), rows - 1)
                place = jnp.where(fits, place, BIN).astype(jnp.float32).astype(jnp.bfloat16)
                col = jnp.bitwise_and(cell, BIN - 1).astype(jnp.float32).astype(jnp.bfloat16)
                first = value.astype(jnp.bfloat16)
                second = (value - first.astype(jnp.float32)).astype(jnp.bfloat16)
                same = level == place
                highs.append(jnp.where(same, first, zero))
                lows.append(jnp.where(same, second, zero))
                cols.append(jnp.where(level == col, unit, zero))
                over = chunk + 1 >= last
                source = jnp.where(over, source + 1, source)
                following = span(source)
                chunk = jnp.where(over, following[0], chunk + 1)
                last = jnp.where(over, following[1], last)
            high = jnp.concatenate(highs, axis=1)
            low = jnp.concatenate(lows, axis=1)
            right = jnp.concatenate(cols, axis=1)
            dims = (((1,), (1,)), ((), ()))
            acc_ref[...] += lax.dot_general(
                high, right, dims, preferred_element_type=jnp.float32
            ) + lax.dot_general(low, right, dims, preferred_element_type=jnp.float32)
            return source, chunk, last

        lax.while_loop(lambda state: state[0] < nsource, work, (jnp.int32(0), *span(0)))
        here = pl.ds(pl.multiple_of(b * rows, rows), rows)
        for half in range(2):
            cols = slice(half * BIN, (half + 1) * BIN)
            out_ref[here, cols] = rhs_ref[here, cols] + acc_ref[half * rows : (half + 1) * rows]
        return carry

    lax.fori_loop(0, nbin, quarter, 0)


def scatter(rhs, got, nsource, nbin):
    nx, ny, nz = rhs.shape
    nrow = nx * ny
    vmem = pl.BlockSpec(memory_space=pltpu.VMEM)
    out = pl.pallas_call(
        functools.partial(scatter_kernel, nbin),
        in_specs=[vmem] * 2,
        out_specs=vmem,
        out_shape=jax.ShapeDtypeStruct((nrow, nz), jnp.float32),
        scratch_shapes=[
            pltpu.VMEM((BIN, BIN), jnp.float32),
            pltpu.VMEM((got.size // LANES, LANES), jnp.float32),
            pltpu.VMEM((nsource, LANES), jnp.int32),
            pltpu.SMEM((nsource, LANES), jnp.int32),
            pltpu.SemaphoreType.DMA,
        ],
        cost_estimate=pl.CostEstimate(
            flops=4 * nrow * nz * got.size // 4, bytes_accessed=4000000, transcendentals=0
        ),
    )(rhs.reshape(nrow, nz), got)
    return out.reshape(nx, ny, nz)


def body(
    pressure_rhs,
    shift_diag,
    positions,
    normals,
    tension,
    edge_weight,
    owner_map,
    cell_map,
    connectivity,
):
    npoint = positions.shape[1]
    ndevice = lax.axis_size(AXES)
    capacity = 4 * npoint // ndevice
    nbin = pressure_rhs.size // (BIN * BIN)
    surface_force, got, inverse, cinverse = front(
        positions, normals, tension, edge_weight, connectivity, owner_map[:, 0], cell_map,
        shift_diag, ndevice, capacity, nbin,
    )
    forcing = scatter(pressure_rhs, got, ndevice, nbin)
    pressure = cycle(forcing, shift_diag, inverse, cinverse)
    return (pressure, surface_force)


def solution(mesh):
    return jax.shard_map(
        body,
        mesh=mesh,
        in_specs=(
            P("gx", "gy", "gz"),
            P("gx", "gy", "gz"),
            P(None, ("gx", "gy", "gz")),
            P(None, ("gx", "gy", "gz")),
            P(("gx", "gy", "gz")),
            P(None, ("gx", "gy", "gz")),
            P(("gx", "gy", "gz"), None),
            P(("gx", "gy", "gz")),
            P(None, ("gx", "gy", "gz")),
        ),
        out_specs=(P("gx", "gy", "gz"), P(None, ("gx", "gy", "gz"))),
        check_vma=False,
    )
```

```python
import functools

import jax
import jax.numpy as jnp
from jax import lax
from jax.experimental import pallas as pl
from jax.experimental.pallas import tpu as pltpu
from jax.sharding import PartitionSpec as P

HALO = 64
SMOOTH = 3
COARSE_SMOOTH = 4
LANES = 2 * HALO


centre = 1.125
spread = 0.875


def factors(sweeps):
    ratio = centre / spread
    fac = 1.0 / ratio
    pairs = [(0.0, 1.0 / centre)]
    for _ in range(1, sweeps):
        fac_new = 1.0 / (2.0 * ratio - fac)
        pairs.append((fac_new * fac, 2.0 * fac_new / spread))
        fac = fac_new
    return pairs


def split3(x):
    a = x.astype(jnp.bfloat16)
    rest = x - a.astype(jnp.float32)
    b = rest.astype(jnp.bfloat16)
    c = (rest - b.astype(jnp.float32)).astype(jnp.bfloat16)
    return a, b, c


MESH = pl.DeviceIdType.MESH
FINE = SMOOTH
COARSE = COARSE_SMOOTH - 1 + (SMOOTH + 1) // 2


UNROLL = 4
VMEM_LIMIT = 36 * 2**20


def around(src, x, r):
    ny, nz = src.shape[1:]
    sub = lax.broadcasted_iota(jnp.int32, (8, nz), 0)
    here = slice(r, r + 8)
    below, above = (r - 8) % ny, (r + 8) % ny
    cells = src[x, here]
    total = src[x - 1, here] + src[x + 1, here]
    total = total + (
        pltpu.roll(jnp.where(sub == 7, src[x, below : below + 8], cells), 1, 0)
        + pltpu.roll(jnp.where(sub == 0, src[x, above : above + 8], cells), 7, 0)
    )
    return cells, total + (pltpu.roll(cells, 1, 1) + pltpu.roll(cells, nz - 1, 1))


def sweep(rhs, inverse, src, dst, update, first, last, pair, keep=None):
    old, new = pair
    rows = src.shape[1] if keep is None else keep.shape[1]

    def slab(x, carry):
        for r in range(0, rows, 8):
            here = slice(r, r + 8)
            cells, total = around(src, x, r)
            change = new * (inverse[x, here] * (rhs[x, here] + total) - cells)
            if old:
                change = change + old * update[x, here]
            if keep is None:
                update[x, here] = change
                dst[x, here] = cells + change
            else:
                keep[x - first, here] = (cells + change)[:, : keep.shape[2]]
        return carry

    lax.fori_loop(first, last, slab, 0, unroll=UNROLL)


def begin(rhs, inverse, dst, update, slabs):
    def slab(x, carry):
        change = inverse[x] * rhs[x] * (1.0 / centre)
        update[x] = change
        dst[x] = change
        return carry

    lax.fori_loop(0, slabs, slab, 0, unroll=2)


def near(axes):
    ok = None
    where = {}
    for axis, step in axes:
        place = lax.axis_index(axis) + step
        fits = (place >= 0) & (place < lax.axis_size(axis))
        ok = fits if ok is None else ok & fits
        where[axis] = place
    return ok, where


SIDES = (-1, 1)
LINKS = (
    [(("gy", a),) for a in SIDES]
    + [(("gz", b),) for b in SIDES]
    + [(("gy", a), ("gz", b)) for b in SIDES for a in SIDES]
    + [(("gx", a),) for a in SIDES]
)
MIRROR = [1, 0, 3, 2, 7, 6, 5, 4, 9, 8]


def greet(links):
    barrier = pltpu.get_barrier_semaphore()
    peers = 0
    for link in links:
        ok, where = near(link)
        peers = peers + ok.astype(jnp.int32)

        @pl.when(ok)
        def _():
            pl.semaphore_signal(barrier, inc=1, device_id=where, device_id_type=MESH)

    pl.semaphore_wait(barrier, peers)


class Field:
    def __init__(self, ext, depth, wide, send, recv, send_sem, recv_sem, land=None):
        self.ext, self.depth, self.wide = ext, depth, wide
        self.send, self.recv = send, recv
        self.send_sem, self.recv_sem = send_sem, recv_sem
        self.land = land
        self.nx = ext.shape[0] - 2 * depth
        self.ny = ext.shape[1] - 2 * wide
        self.nz = ext.shape[2] - 128

    def message(self, m):
        d, nx, ny, nz, h = self.depth, self.nx, self.ny, self.nz, self.wide
        ext = self.ext
        if m < 2:
            if h == 8:
                rows = (0, ny - h)[m]
                src = ext.at[pl.ds(d, nx), pl.ds(rows, h), pl.ds(0, nz)]
                place = (ny + h, ny)[m]
                got = ext.at[pl.ds(d, nx), pl.ds(place, h), pl.ds(0, nz)]
                other = ext.at[pl.ds(d, nx), pl.ds((ny, ny + h)[m], h), pl.ds(0, nz)]
            else:
                src = self.send[0].at[m]
                got = self.recv[0].at[m]
                other = self.recv[0].at[1 - m]
        elif m < 4:
            src = self.send[1].at[m - 2]
            got = self.recv[1].at[m - 2]
            other = self.recv[1].at[3 - m]
        elif m < 8:
            b, a = divmod(m - 4, 2)
            src = self.send[1].at[b, pl.ds((0, ny - 8)[a], 8)]
            got = self.recv[2].at[b, a]
            other = self.recv[2].at[1 - b, 1 - a]
        else:
            a = m - 8
            src = ext.at[pl.ds((d, nx)[a], d)]
            if self.land is None:
                got = ext.at[pl.ds((0, d + nx)[a], d)]
                other = ext.at[pl.ds((d + nx, 0)[a], d)]
            else:
                got = self.land.at[a]
                other = self.land.at[1 - a]
        return src, other, got

    def copy(self, m, incoming):
        src, other, got = self.message(m)
        k = m if incoming else MIRROR[m]
        return pltpu.make_async_remote_copy(
            src_ref=got if incoming else src,
            dst_ref=got if incoming else other,
            send_sem=self.send_sem.at[m],
            recv_sem=self.recv_sem.at[k],
            device_id=near(LINKS[m])[1],
            device_id_type=MESH,
        )

    def start(self, which):
        for m in which:
            @pl.when(near(LINKS[m])[0])
            def _():
                self.copy(m, False).start()

    def finish(self, which):
        for m in which:
            ok = near(LINKS[m])[0]

            @pl.when(ok)
            def _():
                self.copy(m, False).wait_send()
                self.copy(m, True).wait_recv()

            @pl.when(jnp.logical_not(ok))
            def _():
                got = self.message(m)[2]
                got[...] = jnp.zeros(got.shape, jnp.float32)

    def pack(self):
        d, nx, ny, nz, h = self.depth, self.nx, self.ny, self.nz, self.wide
        ext = self.ext
        if h != 8:
            for x in range(nx):
                at = slice(d * (x % 8), d * (x % 8) + d)
                self.send[0][0, x // 8, at] = ext[d + x, :d, :nz]
                self.send[0][1, x // 8, at] = ext[d + x, ny - d : ny, :nz]
        group = lax.broadcasted_iota(jnp.int32, (ny, 128), 1) // (2 * h)

        def slab(x, carry):
            low, high = carry
            mine = group == x
            shift = 2 * h * x + h
            low = jnp.where(mine, pltpu.roll(ext[d + x, :ny, :128], shift, 1), low)
            high = jnp.where(mine, pltpu.roll(ext[d + x, :ny, nz - 128 : nz], shift, 1), high)
            return low, high

        zero = jnp.zeros((ny, 128), jnp.float32)
        low, high = lax.fori_loop(0, nx, slab, (zero, zero), unroll=8)
        self.send[1][0] = low
        self.send[1][1] = high

    def unpack(self):
        d, nx, ny, nz, h = self.depth, self.nx, self.ny, self.nz, self.wide
        ext = self.ext
        if h != 8:
            for x in range(nx):
                at = slice(d * (x % 8), d * (x % 8) + d)
                ext[d + x, ny : ny + d, :nz] = self.recv[0][1, x // 8, at]
                ext[d + x, ny + 8 - d : ny + 8, :nz] = self.recv[0][0, x // 8, at]
        ends = []
        for b in range(2):
            corner = (self.recv[2][b, 1], self.recv[2][b, 0])
            if h == 8:
                ends.append(jnp.concatenate([self.recv[1][b], *corner], axis=0))
            else:
                sub = lax.broadcasted_iota(jnp.int32, (8, 128), 0)
                ends.append(
                    jnp.concatenate([self.recv[1][b], jnp.where(sub < h, *corner)], axis=0)
                )
        lane = lax.broadcasted_iota(jnp.int32, ends[0].shape, 1)
        both = jnp.where(lane % (2 * h) < h, ends[0], ends[1])
        edge = (lane < h) | (lane >= 128 - h)

        def slab(x, carry):
            moved = pltpu.roll(both, 128 - h - 2 * h * x, 1)
            ext[d + x, :, nz : nz + 128] = jnp.where(edge, moved, 0.0)
            return carry

        lax.fori_loop(0, nx, slab, 0, unroll=8)


def pair_up(src, pairs):
    def add(j, carry):
        pairs[j] = src[2 * j] + src[2 * j + 1]
        return carry

    lax.fori_loop(0, pairs.shape[0], add, 0)


def pooled(pairs, into, after):
    cx, ny, nz = pairs.shape
    depth = COARSE
    flat = pairs[...].reshape(cx * ny, nz)

    def halves(rows, cols, dim):
        r = lax.broadcasted_iota(jnp.int32, (rows, cols), dim)
        c = lax.broadcasted_iota(jnp.int32, (rows, cols), 1 - dim)
        return (r == jnp.right_shift(c, 1)).astype(jnp.float32).astype(jnp.bfloat16)

    along_z = halves(nz, nz // 2, 1)
    along_y = halves(cx * ny // 2, cx * ny, 0)
    flat = sum(jnp.dot(p, along_z, preferred_element_type=jnp.float32) for p in split3(flat))
    flat = sum(jnp.dot(along_y, p, preferred_element_type=jnp.float32) for p in split3(flat))
    out = after(0.5 * flat).reshape(cx, ny // 2, nz // 2)
    into[depth : depth + cx, : ny // 2, : nz // 2] = out


def fine_field(ext, bufs, sems, landing=None):
    ysend, yrecv, zsend, zrecv, yzrecv = bufs
    return Field(ext, FINE, 4, (ysend, zsend), (yrecv, zrecv, yzrecv), *sems, landing)


def coarse_field(ext, bufs, sems):
    zsend, zrecv, yzrecv = bufs
    return Field(ext, COARSE, 8, (None, zsend), (None, zrecv, yzrecv), *sems)


def buf(*shape):
    return pltpu.VMEM(shape, jnp.float32)


def wide_shapes(nx, ny, nz):
    cx, cy, cz = nx // 2, ny // 2, nz // 2
    return (
        (nx + 2 * FINE, ny + 8, nz + 128),
        (cx + 2 * COARSE, cy + 16, cz + 128),
    )


def fine_scratch(nx, ny, nz):
    rows = (2, nx // 8, 8 * FINE, nz)
    return [buf(*rows)] * 2 + [buf(2, ny, 128)] * 2 + [buf(2, 2, 8, 128)]


def coarse_scratch(nx, ny, nz):
    return [buf(2, ny // 2, 128)] * 2 + [buf(2, 2, 8, 128)]


FIRST, LAST = range(8), (8, 9)


def cycle_kernel(forcing, shift_hbm, inverse, cinverse, pressure, *scratch):
    shift, load_sem, scratch = scratch[0], scratch[-1], scratch[1:-1]
    fetch = pltpu.make_async_copy(shift_hbm, shift, load_sem)
    fetch.start()
    (rhs, one, two, update, land, crhs, cone, ctwo, cupdate, pairs), scratch = (
        scratch[:10], scratch[10:],
    )
    bufs_a, bufs_b, bufs_c = scratch[:5], scratch[5:10], scratch[10:13]
    send_sem, recv_sem = scratch[13:]
    nx, ny, nz = forcing.shape
    sems = [(send_sem.at[k], recv_sem.at[k]) for k in range(3)]

    def load(x, carry):
        rhs[FINE + x, :ny, :nz] = forcing[x]
        return carry

    lax.fori_loop(0, nx, load, 0, unroll=2)
    field = fine_field(rhs, bufs_a, sems[0])
    field.pack()
    greet(LINKS)
    field.start(FIRST)
    field.finish(FIRST)
    field.unpack()
    field.start(LAST)
    field.finish(LAST)

    slabs = nx + 2 * FINE
    pairs_of = factors(SMOOTH)
    bufs = (one, two)
    begin(rhs, inverse, one, update, slabs)
    for k in range(1, SMOOTH):
        sweep(rhs, inverse, bufs[(k - 1) % 2], bufs[k % 2], update, k, slabs - k, pairs_of[k])
    smooth = bufs[(SMOOTH - 1) % 2]
    other = bufs[SMOOTH % 2]

    fetch.wait()

    def residual(j, carry):
        for r in range(0, ny, 8):
            here = slice(r, r + 8)
            both = 0.0
            for half in range(2):
                x = 2 * j + half
                cells, total = around(smooth, FINE + x, r)
                total = total[:, :nz] + rhs[FINE + x, here, :nz]
                both = both + (total - (6.0 + shift[x, here]) * cells[:, :nz])
            pairs[j, here] = both
        return carry

    lax.fori_loop(0, nx // 2, residual, 0, unroll=2)
    pooled(pairs, crhs, lambda total: total)
    coarse = coarse_field(crhs, bufs_c, sems[2])
    coarse.pack()
    coarse.start(FIRST)
    field = fine_field(smooth, bufs_b, sems[1], land)
    field.pack()
    field.start(FIRST)
    cslabs = crhs.shape[0]
    low = COARSE - (FINE + 1) // 2
    count = cslabs - 2 * low
    cny, cnz = crhs.shape[1:]
    fny, fnz = smooth.shape[1:]

    def fan(shape, fine_dim, per_f, per_c, core, jump):
        f = lax.broadcasted_iota(jnp.int32, shape, fine_dim)
        c = lax.broadcasted_iota(jnp.int32, shape, 1 - fine_dim)
        block = 0
        for g in range(1, shape[fine_dim] // per_f):
            block = block + (f >= g * per_f).astype(jnp.int32)
        inner = f - block * per_f
        target = jnp.right_shift(inner, 1) + jnp.where(inner >= core, jump, 0) + block * per_c
        return (c == target).astype(jnp.float32).astype(jnp.bfloat16)

    fan_y = fan((count * fny, count * cny), 0, fny, cny, ny + 4, cny - fny // 2)
    fan_z = fan((cnz, fnz), 1, fnz, cnz, nz + 64, cnz - fnz // 2)
    coarse.finish(FIRST)
    coarse.unpack()
    coarse.start(LAST)
    field.finish(FIRST)
    field.unpack()
    field.start(LAST)
    coarse.finish(LAST)

    pairs_of = factors(COARSE_SMOOTH)
    cbufs = (cone, ctwo)
    begin(crhs, cinverse, cone, cupdate, cslabs)
    for k in range(1, COARSE_SMOOTH):
        sweep(
            crhs, cinverse, cbufs[(k - 1) % 2], cbufs[k % 2], cupdate, k, cslabs - k, pairs_of[k]
        )
    fix = cbufs[(COARSE_SMOOTH - 1) % 2]

    field.finish(LAST)
    flat = fix[low : low + count].reshape(count * cny, cnz)

    tall = sum(jnp.dot(fan_y, p, preferred_element_type=jnp.float32) for p in split3(flat))
    full = sum(jnp.dot(p, fan_z, preferred_element_type=jnp.float32) for p in split3(tall))
    for j in range(count):
        part = full[j * fny : (j + 1) * fny]
        for half in range(2):
            x = FINE + 2 * (low + j - COARSE) + half
            if 0 <= x < FINE:
                smooth[x] = land[0, x] + part
            elif FINE <= x < FINE + nx:
                smooth[x] = smooth[x] + part
            elif FINE + nx <= x < slabs:
                smooth[x] = land[1, x - FINE - nx] + part

    pairs_of = factors(SMOOTH)
    bufs = (smooth, other)

    for k in range(SMOOTH):
        sweep(
            rhs, inverse, bufs[k % 2], bufs[(k + 1) % 2], update,
            k + 1, slabs - k - 1, pairs_of[k], pressure if k == SMOOTH - 1 else None,
        )


def cycle(forcing, shift, inverse, cinverse):
    nx, ny, nz = forcing.shape
    wide, cwide = (buf(*shape) for shape in wide_shapes(nx, ny, nz))
    vmem = pl.BlockSpec(memory_space=pltpu.VMEM)
    return pl.pallas_call(
        cycle_kernel,
        in_specs=[vmem, pl.BlockSpec(memory_space=pltpu.HBM), vmem, vmem],
        out_specs=vmem,
        out_shape=jax.ShapeDtypeStruct(forcing.shape, jnp.float32),
        scratch_shapes=[buf(nx, ny, nz)]
        + [wide] * 4
        + [buf(2, FINE, ny + 8, nz + 128)]
        + [cwide] * 4
        + [buf(nx // 2, ny, nz)]
        + fine_scratch(nx, ny, nz) * 2
        + coarse_scratch(nx, ny, nz)
        + [pltpu.SemaphoreType.DMA((3, 10))] * 2
        + [pltpu.SemaphoreType.DMA],
        compiler_params=pltpu.CompilerParams(
            collective_id=1, has_side_effects=True, vmem_limit_bytes=VMEM_LIMIT
        ),
    )(forcing, in_hbm(shift), inverse, cinverse)


BIN = 256
AXES = ("gx", "gy", "gz")


def in_hbm(x):
    return pltpu.with_memory_space_constraint(x, pltpu.HBM)


def hot_rows(index, rows, dtype=jnp.bfloat16):
    r = lax.broadcasted_iota(jnp.int32, (rows, index.shape[1]), 0)
    if rows > BIN:
        return r == index
    return r.astype(jnp.float32).astype(dtype) == index.astype(jnp.float32).astype(dtype)


def place_of(index):
    where = {}
    for axis in reversed(AXES):
        count = lax.axis_size(axis)
        where[axis] = lax.rem(index, count)
        index = lax.div(index, count)
    return where


def front_kernel(
    ndevice, capacity, nbin, *refs
):
    sources, refs = refs[:8], refs[8:]
    (force_ref, got_ref, inverse, cinverse), refs = refs[:4], refs[4:]
    (pos_ref, nrm_ref, ten_ref, wgt_ref, con_ref, own_ref, cel_ref, shift), scratch = (
        refs[:8], refs[8:],
    )
    load_sem, scratch = scratch[-1], scratch[:-1]

    def fetch(k):
        return pltpu.make_async_copy(sources[k], refs[k], load_sem.at[k])

    for k in (7, 0, 5, 6, 4, 3, 2, 1):
        fetch(k).start()
    (packed_ref, carry_ref, rank_ref, jump_ref, pad_ref, psend, precv, pairs), scratch = (
        scratch[:8], scratch[8:],
    )
    fine_bufs, coarse_bufs = scratch[:5], scratch[5:8]
    send_sem, recv_sem, all_send, all_recv, pos_send, pos_recv = scratch[8:]
    chunk = 4 * LANES
    per = packed_ref.shape[0] // ndevice
    npoint = ten_ref.shape[1]
    nx, ny, nz = shift.shape
    zero, unit = jnp.zeros((), jnp.bfloat16), jnp.ones((), jnp.bfloat16)
    me = lax.axis_index(AXES)
    barrier = pltpu.get_barrier_semaphore()

    def other(p):
        return lax.rem(me + p, ndevice)

    def hello(p, carry):
        pl.semaphore_signal(barrier, inc=1, device_id=place_of(other(p)), device_id_type=MESH)
        return carry

    lax.fori_loop(1, ndevice, hello, 0)

    fetch(7).wait()

    def load(x, carry):
        inverse[FINE + x, :ny, :nz] = 1.0 / (6.0 + shift[x])
        return carry

    lax.fori_loop(0, nx, load, 0, unroll=2)
    pair_up(shift, pairs)
    pooled(pairs, cinverse, lambda total: 1.0 / (6.0 + total))
    fine = fine_field(inverse, fine_bufs, (send_sem.at[0], recv_sem.at[0]))
    coarse = coarse_field(cinverse, coarse_bufs, (send_sem.at[1], recv_sem.at[1]))
    fine.pack()
    coarse.pack()
    fetch(0).wait()
    psend[0, :3] = pos_ref[:, npoint - LANES :]
    psend[1, :3] = pos_ref[:, :LANES]

    def spread_out(j, carry):
        lower = pos_ref[:, pl.ds(pl.multiple_of(j * LANES - LANES, LANES), LANES)]
        upper = pos_ref[:, pl.ds(pl.multiple_of(j * LANES, LANES), LANES)]
        both = jnp.concatenate([lower[:, HALO:], upper[:, :HALO]], axis=1)
        pad_ref[:3, pl.ds(pl.multiple_of(j * LANES, LANES), LANES)] = both
        return carry

    lax.fori_loop(1, npoint // LANES, spread_out, 0, unroll=7)

    pl.semaphore_wait(barrier, ndevice - 1)

    def edge(side, incoming):
        return pltpu.make_async_remote_copy(
            src_ref=psend.at[side],
            dst_ref=precv.at[side],
            send_sem=pos_send.at[side],
            recv_sem=pos_recv.at[side],
            device_id=place_of(other((1, ndevice - 1)[side])),
            device_id_type=MESH,
        )

    for side in range(2):
        edge(side, False).start()
    fine.start(FIRST)
    coarse.start(FIRST)

    def classes(here):
        return own_ref[:, here] + ndevice * jnp.right_shift(cel_ref[:, here], 16)

    def count(i, total):
        here = pl.ds(pl.multiple_of(i * chunk, chunk), chunk)
        hot = jnp.where(hot_rows(classes(here), nbin * ndevice), 1.0, 0.0).astype(jnp.float32)
        return total + (
            hot[:, :LANES] + hot[:, LANES : 2 * LANES]
            + (hot[:, 2 * LANES : 3 * LANES] + hot[:, 3 * LANES :])
        )

    for k in (5, 6):
        fetch(k).wait()
    counts = lax.fori_loop(
        0, npoint // chunk, count, jnp.zeros((nbin * ndevice, LANES), jnp.float32), unroll=2
    )
    counts = jnp.sum(counts, axis=1, keepdims=True)
    base = jnp.zeros((ndevice, 1), jnp.float32)
    for b in range(nbin):
        carry_ref[b * ndevice : (b + 1) * ndevice] = base
        base = base + counts[b * ndevice : (b + 1) * ndevice]
    before = (
        lax.broadcasted_iota(jnp.int32, (chunk, chunk), 0)
        < lax.broadcasted_iota(jnp.int32, (chunk, chunk), 1)
    ).astype(jnp.float32).astype(jnp.bfloat16)

    def order(i, carry):
        here = pl.ds(pl.multiple_of(i * chunk, chunk), chunk)
        ones = jnp.where(hot_rows(classes(here), nbin * ndevice), unit, zero)
        earlier = jnp.dot(ones, before, preferred_element_type=jnp.float32) + carry
        wide = ones.astype(jnp.float32)
        rank_ref[:, here] = jnp.sum(wide * earlier, axis=0, keepdims=True).astype(jnp.int32)
        return carry + jnp.sum(wide, axis=1, keepdims=True)

    lax.fori_loop(0, npoint // chunk, order, carry_ref[...], unroll=2)

    for k in (4, 3, 2, 1):
        fetch(k).wait()
    for side in range(2):
        edge(side, True).wait_send()
        edge(side, True).wait_recv()
    pad_ref[:3, :LANES] = jnp.concatenate(
        [precv[0, :3, HALO:], pos_ref[:, :HALO]], axis=1
    )
    pad_ref[:3, npoint:] = jnp.concatenate(
        [pos_ref[:, npoint - HALO :], precv[1, :3, :HALO]], axis=1
    )
    begin_at = me * npoint
    everything = npoint * ndevice

    def pull(i, carry):
        for sub in range(2):
            base = pl.multiple_of(i * 2 * LANES + sub * LANES, LANES)
            here = pl.ds(base, LANES)
            lower = pad_ref[:, here]
            upper = pad_ref[:, pl.ds(base + LANES, LANES)]
            centre_pos = jnp.concatenate([lower[:, HALO:], upper[:, :HALO]], axis=1)
            index = con_ref[:, here] - begin_at + HALO
            index = jnp.where(index < 0, index + everything, index)
            index = jnp.where(index >= everything, index - everything, index) - base
            total = jnp.zeros_like(lower)
            for which in range(con_ref.shape[0]):
                wide = jnp.broadcast_to(index[which : which + 1], lower.shape)
                low = jnp.bitwise_and(wide, LANES - 1)
                near_by = jnp.take_along_axis(lower, low, axis=1, mode="promise_in_bounds")
                far = jnp.take_along_axis(upper, low, axis=1, mode="promise_in_bounds")
                picked = jnp.where(wide < LANES, near_by, far)
                total = total + wgt_ref[which : which + 1, here] * (picked - centre_pos)
            force = ten_ref[:, here] * total[:3]
            force_ref[:, here] = force
            jump_ref[:, here] = jnp.sum(force * nrm_ref[:, here], axis=0, keepdims=True)
        return carry

    lax.fori_loop(0, npoint // (2 * LANES), pull, 0, unroll=2)

    fine.finish(FIRST)
    fine.unpack()
    fine.start(LAST)
    coarse.finish(FIRST)
    coarse.unpack()
    coarse.start(LAST)

    packed_ref[...] = jnp.zeros_like(packed_ref)

    def pack(i, carry):
        here = pl.ds(pl.multiple_of(i * chunk, chunk), chunk)
        rank = rank_ref[:, here]
        slots = jnp.where(hot_rows(jnp.bitwise_and(rank, BIN - 1), BIN), unit, zero)
        row = own_ref[:, here] * per + jnp.right_shift(rank, 8)
        here_value = hot_rows(row, packed_ref.shape[0])
        here_cell = hot_rows(row + per // 2, packed_ref.shape[0])
        cell = cel_ref[:, here] + 1
        total = packed_ref[...]
        for piece, bits in zip(split3(jump_ref[:, here]), (0, 8, 16)):
            digit = jnp.left_shift(jnp.bitwise_and(jnp.right_shift(cell, bits), 255), bits)
            digit = digit.astype(jnp.float32).astype(jnp.bfloat16)
            left = jnp.where(here_value, piece, jnp.where(here_cell, digit, zero))
            total = total + lax.dot_general(
                left, slots, (((1,), (1,)), ((), ())), preferred_element_type=jnp.float32
            )
        packed_ref[...] = total
        return carry

    lax.fori_loop(0, npoint // chunk, pack, 0, unroll=2)

    def rows_of(device):
        return pl.ds(pl.multiple_of(device * per, per), per)

    def deal(p, incoming):
        return pltpu.make_async_remote_copy(
            src_ref=packed_ref.at[rows_of(other(p))],
            dst_ref=got_ref.at[rows_of(other(ndevice - p) if incoming else me)],
            send_sem=all_send.at[p],
            recv_sem=all_recv.at[p],
            device_id=place_of(other(p)),
            device_id_type=MESH,
        )

    def send(p, carry):
        deal(p, False).start()
        return carry

    lax.fori_loop(1, ndevice, send, 0)
    got_ref[rows_of(me)] = packed_ref[rows_of(me)]
    fine.finish(LAST)
    coarse.finish(LAST)

    def receive(p, carry):
        deal(p, False).wait_send()
        deal(p, True).wait_recv()
        return carry

    lax.fori_loop(1, ndevice, receive, 0)


def front(
    positions, normals, tension, edge_weight, connectivity, owner_ids, cell_map, shift,
    ndevice, capacity, nbin,
):
    npoint = tension.shape[0]
    nx, ny, nz = shift.shape
    per = max(8, 2 * (capacity // BIN))
    vmem = pl.BlockSpec(memory_space=pltpu.VMEM)
    wide, cwide = wide_shapes(nx, ny, nz)
    return pl.pallas_call(
        functools.partial(front_kernel, ndevice, capacity, nbin),
        in_specs=[pl.BlockSpec(memory_space=pltpu.HBM)] * 8,
        out_specs=[vmem] * 4,
        out_shape=[
            jax.ShapeDtypeStruct(shape, jnp.float32)
            for shape in ((3, npoint), (ndevice * per, BIN), wide, cwide)
        ],
        scratch_shapes=[
            buf(3, npoint),
            buf(3, npoint),
            buf(1, npoint),
            buf(*edge_weight.shape),
            pltpu.VMEM(connectivity.shape, jnp.int32),
            pltpu.VMEM((1, npoint), jnp.int32),
            pltpu.VMEM((1, npoint), jnp.int32),
            buf(nx, ny, nz),
            buf(ndevice * per, BIN),
            buf(nbin * ndevice, 1),
            pltpu.VMEM((1, npoint), jnp.int32),
            buf(1, npoint),
            buf(8, npoint + LANES),
            buf(2, 8, LANES),
            buf(2, 8, LANES),
            buf(nx // 2, ny, nz),
        ]
        + fine_scratch(nx, ny, nz)
        + coarse_scratch(nx, ny, nz)
        + [pltpu.SemaphoreType.DMA((2, 10))] * 2
        + [pltpu.SemaphoreType.DMA((ndevice,))] * 2
        + [pltpu.SemaphoreType.DMA((2,))] * 2
        + [pltpu.SemaphoreType.DMA((8,))],
        compiler_params=pltpu.CompilerParams(
            collective_id=0, has_side_effects=True, vmem_limit_bytes=20 * 2**20
        ),
    )(
        *map(
            in_hbm,
            (
                positions, normals, tension[None], edge_weight, connectivity, owner_ids[None],
                cell_map[None], shift,
            ),
        )
    )


GROUP = 24


def scatter_kernel(
    nbin, rhs_hbm, got_ref, force_ref, out_ref, force_hbm,
    rhs_ref, acc_ref, flat_ref, ends_ref, bound_ref, sems,
):
    nrow, nz = rhs_ref.shape
    fetch = pltpu.make_async_copy(rhs_hbm, rhs_ref, sems.at[1])
    fetch.start()
    put = pltpu.make_async_copy(force_ref, force_hbm, sems.at[2])
    put.start()
    nsource = bound_ref.shape[0]
    per = got_ref.shape[0] // nsource
    chunks = per // 2 * (BIN // LANES)
    rows = nrow // nbin
    nflat = got_ref.shape[0]
    for half in range(BIN // LANES):
        flat_ref[half * nflat : (half + 1) * nflat] = got_ref[:, half * LANES : (half + 1) * LANES]
    got = got_ref[...].reshape(nsource, per, BIN)
    cell_row = lax.broadcasted_iota(jnp.int32, got.shape, 1) >= per // 2
    used = cell_row & (got > 0.0)
    lane = lax.broadcasted_iota(jnp.int32, (nsource, LANES), 1)
    ends = jnp.zeros((nsource, LANES), jnp.float32)
    for b in range(nbin):
        inside = jnp.where(used & (got <= float((b + 1) * BIN * BIN)), 1.0, 0.0)
        total = jnp.sum(jnp.sum(inside, axis=1), axis=1, keepdims=True)
        ends = jnp.where(lane == b + 1, total, ends)
    ends_ref[...] = ends.astype(jnp.int32)
    copy = pltpu.make_async_copy(ends_ref, bound_ref, sems.at[0])
    copy.start()
    copy.wait()
    fetch.wait()
    level = lax.broadcasted_iota(jnp.int32, (BIN, LANES), 0).astype(jnp.float32)
    level = level.astype(jnp.bfloat16)
    zero, unit = jnp.zeros((), jnp.bfloat16), jnp.ones((), jnp.bfloat16)

    def quarter(b, carry):
        def span(source):
            at = jnp.minimum(source, nsource - 1)
            first = jnp.minimum(jnp.right_shift(bound_ref[at, b], 7), chunks - 1)
            last = jnp.right_shift(bound_ref[at, b + 1] + LANES - 1, 7)
            return first, jnp.maximum(last, first + 1)

        acc_ref[...] = jnp.zeros_like(acc_ref)

        def work(state):
            source, chunk, last = state
            highs, lows, cols = [], [], []
            for _ in range(GROUP):
                at = jnp.minimum(source, nsource - 1)
                row = jnp.bitwise_and(chunk, 1) * nflat + at * per + jnp.right_shift(chunk, 1)
                value = flat_ref[pl.ds(row, 1)]
                cell = flat_ref[pl.ds(row + per // 2, 1)].astype(jnp.int32) - 1
                fits = (jnp.right_shift(cell, 16) == b) & (source < nsource)
                half = jnp.bitwise_and(jnp.right_shift(cell, 8), 1)
                place = half * rows + jnp.bitwise_and(jnp.right_shift(cell, 9), rows - 1)
                place = jnp.where(fits, place, BIN).astype(jnp.float32).astype(jnp.bfloat16)
                col = jnp.bitwise_and(cell, BIN - 1).astype(jnp.float32).astype(jnp.bfloat16)
                first = value.astype(jnp.bfloat16)
                second = (value - first.astype(jnp.float32)).astype(jnp.bfloat16)
                same = level == place
                highs.append(jnp.where(same, first, zero))
                lows.append(jnp.where(same, second, zero))
                cols.append(jnp.where(level == col, unit, zero))
                over = chunk + 1 >= last
                source = jnp.where(over, source + 1, source)
                following = span(source)
                chunk = jnp.where(over, following[0], chunk + 1)
                last = jnp.where(over, following[1], last)
            high = jnp.concatenate(highs, axis=1)
            low = jnp.concatenate(lows, axis=1)
            right = jnp.concatenate(cols, axis=1)
            dims = (((1,), (1,)), ((), ()))
            acc_ref[...] += lax.dot_general(
                high, right, dims, preferred_element_type=jnp.float32
            ) + lax.dot_general(low, right, dims, preferred_element_type=jnp.float32)
            return source, chunk, last

        lax.while_loop(lambda state: state[0] < nsource, work, (jnp.int32(0), *span(0)))
        here = pl.ds(pl.multiple_of(b * rows, rows), rows)
        for half in range(2):
            cols = slice(half * BIN, (half + 1) * BIN)
            out_ref[here, cols] = rhs_ref[here, cols] + acc_ref[half * rows : (half + 1) * rows]
        return carry

    lax.fori_loop(0, nbin, quarter, 0)
    put.wait()


def scatter(rhs, got, force, nsource, nbin):
    nx, ny, nz = rhs.shape
    nrow = nx * ny
    vmem = pl.BlockSpec(memory_space=pltpu.VMEM)
    hbm = pl.BlockSpec(memory_space=pltpu.HBM)
    out, force = pl.pallas_call(
        functools.partial(scatter_kernel, nbin),
        in_specs=[hbm, vmem, vmem],
        out_specs=[vmem, hbm],
        out_shape=[
            jax.ShapeDtypeStruct((nrow, nz), jnp.float32),
            jax.ShapeDtypeStruct(force.shape, jnp.float32),
        ],
        scratch_shapes=[
            pltpu.VMEM((nrow, nz), jnp.float32),
            pltpu.VMEM((BIN, BIN), jnp.float32),
            pltpu.VMEM((got.size // LANES, LANES), jnp.float32),
            pltpu.VMEM((nsource, LANES), jnp.int32),
            pltpu.SMEM((nsource, LANES), jnp.int32),
            pltpu.SemaphoreType.DMA((3,)),
        ],
        compiler_params=pltpu.CompilerParams(vmem_limit_bytes=24 * 2**20),
        cost_estimate=pl.CostEstimate(
            flops=4 * nrow * nz * got.size // 4, bytes_accessed=4000000, transcendentals=0
        ),
    )(in_hbm(rhs.reshape(nrow, nz)), got, force)
    return out.reshape(nx, ny, nz), force


def body(
    pressure_rhs,
    shift_diag,
    positions,
    normals,
    tension,
    edge_weight,
    owner_map,
    cell_map,
    connectivity,
):
    npoint = positions.shape[1]
    ndevice = lax.axis_size(AXES)
    capacity = 4 * npoint // ndevice
    nbin = pressure_rhs.size // (BIN * BIN)
    surface_force, got, inverse, cinverse = front(
        positions, normals, tension, edge_weight, connectivity, owner_map[:, 0], cell_map,
        shift_diag, ndevice, capacity, nbin,
    )
    forcing, surface_force = scatter(pressure_rhs, got, surface_force, ndevice, nbin)
    pressure = cycle(forcing, shift_diag, inverse, cinverse)
    return (pressure, surface_force)


def solution(mesh):
    return jax.shard_map(
        body,
        mesh=mesh,
        in_specs=(
            P("gx", "gy", "gz"),
            P("gx", "gy", "gz"),
            P(None, ("gx", "gy", "gz")),
            P(None, ("gx", "gy", "gz")),
            P(("gx", "gy", "gz")),
            P(None, ("gx", "gy", "gz")),
            P(("gx", "gy", "gz"), None),
            P(("gx", "gy", "gz")),
            P(None, ("gx", "gy", "gz")),
        ),
        out_specs=(P("gx", "gy", "gz"), P(None, ("gx", "gy", "gz"))),
        check_vma=False,
    )
```

```python
import functools

import jax
import jax.numpy as jnp
from jax import lax
from jax.experimental import pallas as pl
from jax.experimental.pallas import tpu as pltpu
from jax.sharding import PartitionSpec as P

HALO = 64
SMOOTH = 3
COARSE_SMOOTH = 4
LANES = 2 * HALO


centre = 1.125
spread = 0.875


def factors(sweeps):
    ratio = centre / spread
    fac = 1.0 / ratio
    pairs = [(0.0, 1.0 / centre)]
    for _ in range(1, sweeps):
        fac_new = 1.0 / (2.0 * ratio - fac)
        pairs.append((fac_new * fac, 2.0 * fac_new / spread))
        fac = fac_new
    return pairs


def split3(x):
    a = x.astype(jnp.bfloat16)
    rest = x - a.astype(jnp.float32)
    b = rest.astype(jnp.bfloat16)
    c = (rest - b.astype(jnp.float32)).astype(jnp.bfloat16)
    return a, b, c


MESH = pl.DeviceIdType.MESH
FINE = SMOOTH
COARSE = COARSE_SMOOTH - 1 + (SMOOTH + 1) // 2


UNROLL = 4
VMEM_LIMIT = 36 * 2**20


def around(src, x, r):
    ny, nz = src.shape[1:]
    sub = lax.broadcasted_iota(jnp.int32, (8, nz), 0)
    here = slice(r, r + 8)
    below, above = (r - 8) % ny, (r + 8) % ny
    cells = src[x, here]
    total = src[x - 1, here] + src[x + 1, here]
    total = total + (
        pltpu.roll(jnp.where(sub == 7, src[x, below : below + 8], cells), 1, 0)
        + pltpu.roll(jnp.where(sub == 0, src[x, above : above + 8], cells), 7, 0)
    )
    return cells, total + (pltpu.roll(cells, 1, 1) + pltpu.roll(cells, nz - 1, 1))


def sweep(rhs, inverse, src, dst, update, first, last, pair, keep=None):
    old, new = pair
    rows = src.shape[1] if keep is None else keep.shape[1]

    def slab(x, carry):
        for r in range(0, rows, 8):
            here = slice(r, r + 8)
            cells, total = around(src, x, r)
            change = new * (inverse[x, here] * (rhs[x, here] + total) - cells)
            if old:
                change = change + old * update[x, here]
            if keep is None:
                update[x, here] = change
                dst[x, here] = cells + change
            else:
                keep[x - first, here] = (cells + change)[:, : keep.shape[2]]
        return carry

    lax.fori_loop(first, last, slab, 0, unroll=UNROLL)


def begin(rhs, inverse, dst, update, slabs):
    def slab(x, carry):
        change = inverse[x] * rhs[x] * (1.0 / centre)
        update[x] = change
        dst[x] = change
        return carry

    lax.fori_loop(0, slabs, slab, 0, unroll=2)


def near(axes):
    ok = None
    where = {}
    for axis, step in axes:
        place = lax.axis_index(axis) + step
        fits = (place >= 0) & (place < lax.axis_size(axis))
        ok = fits if ok is None else ok & fits
        where[axis] = place
    return ok, where


SIDES = (-1, 1)
LINKS = (
    [(("gy", a),) for a in SIDES]
    + [(("gz", b),) for b in SIDES]
    + [(("gy", a), ("gz", b)) for b in SIDES for a in SIDES]
    + [(("gx", a),) for a in SIDES]
)
MIRROR = [1, 0, 3, 2, 7, 6, 5, 4, 9, 8]


def greet(links):
    barrier = pltpu.get_barrier_semaphore()
    peers = 0
    for link in links:
        ok, where = near(link)
        peers = peers + ok.astype(jnp.int32)

        @pl.when(ok)
        def _():
            pl.semaphore_signal(barrier, inc=1, device_id=where, device_id_type=MESH)

    pl.semaphore_wait(barrier, peers)


class Field:
    def __init__(self, ext, depth, wide, send, recv, send_sem, recv_sem, land=None):
        self.ext, self.depth, self.wide = ext, depth, wide
        self.send, self.recv = send, recv
        self.send_sem, self.recv_sem = send_sem, recv_sem
        self.land = land
        self.nx = ext.shape[0] - 2 * depth
        self.ny = ext.shape[1] - 2 * wide
        self.nz = ext.shape[2] - 128

    def message(self, m):
        d, nx, ny, nz, h = self.depth, self.nx, self.ny, self.nz, self.wide
        ext = self.ext
        if m < 2:
            if h == 8:
                rows = (0, ny - h)[m]
                src = ext.at[pl.ds(d, nx), pl.ds(rows, h), pl.ds(0, nz)]
                place = (ny + h, ny)[m]
                got = ext.at[pl.ds(d, nx), pl.ds(place, h), pl.ds(0, nz)]
                other = ext.at[pl.ds(d, nx), pl.ds((ny, ny + h)[m], h), pl.ds(0, nz)]
            else:
                src = self.send[0].at[m]
                got = self.recv[0].at[m]
                other = self.recv[0].at[1 - m]
        elif m < 4:
            src = self.send[1].at[m - 2]
            got = self.recv[1].at[m - 2]
            other = self.recv[1].at[3 - m]
        elif m < 8:
            b, a = divmod(m - 4, 2)
            src = self.send[1].at[b, pl.ds((0, ny - 8)[a], 8)]
            got = self.recv[2].at[b, a]
            other = self.recv[2].at[1 - b, 1 - a]
        else:
            a = m - 8
            src = ext.at[pl.ds((d, nx)[a], d)]
            if self.land is None:
                got = ext.at[pl.ds((0, d + nx)[a], d)]
                other = ext.at[pl.ds((d + nx, 0)[a], d)]
            else:
                got = self.land.at[a]
                other = self.land.at[1 - a]
        return src, other, got

    def copy(self, m, incoming):
        src, other, got = self.message(m)
        k = m if incoming else MIRROR[m]
        return pltpu.make_async_remote_copy(
            src_ref=got if incoming else src,
            dst_ref=got if incoming else other,
            send_sem=self.send_sem.at[m],
            recv_sem=self.recv_sem.at[k],
            device_id=near(LINKS[m])[1],
            device_id_type=MESH,
        )

    def start(self, which):
        for m in which:
            @pl.when(near(LINKS[m])[0])
            def _():
                self.copy(m, False).start()

    def finish(self, which):
        for m in which:
            ok = near(LINKS[m])[0]

            @pl.when(ok)
            def _():
                self.copy(m, False).wait_send()
                self.copy(m, True).wait_recv()

            @pl.when(jnp.logical_not(ok))
            def _():
                got = self.message(m)[2]
                got[...] = jnp.zeros(got.shape, jnp.float32)

    def pack(self):
        d, nx, ny, nz, h = self.depth, self.nx, self.ny, self.nz, self.wide
        ext = self.ext
        if h != 8:
            for x in range(nx):
                at = slice(d * (x % 8), d * (x % 8) + d)
                self.send[0][0, x // 8, at] = ext[d + x, :d, :nz]
                self.send[0][1, x // 8, at] = ext[d + x, ny - d : ny, :nz]
        group = lax.broadcasted_iota(jnp.int32, (ny, 128), 1) // (2 * h)

        def slab(x, carry):
            low, high = carry
            mine = group == x
            shift = 2 * h * x + h
            low = jnp.where(mine, pltpu.roll(ext[d + x, :ny, :128], shift, 1), low)
            high = jnp.where(mine, pltpu.roll(ext[d + x, :ny, nz - 128 : nz], shift, 1), high)
            return low, high

        zero = jnp.zeros((ny, 128), jnp.float32)
        low, high = lax.fori_loop(0, nx, slab, (zero, zero), unroll=8)
        self.send[1][0] = low
        self.send[1][1] = high

    def unpack(self):
        d, nx, ny, nz, h = self.depth, self.nx, self.ny, self.nz, self.wide
        ext = self.ext
        if h != 8:
            for x in range(nx):
                at = slice(d * (x % 8), d * (x % 8) + d)
                ext[d + x, ny : ny + d, :nz] = self.recv[0][1, x // 8, at]
                ext[d + x, ny + 8 - d : ny + 8, :nz] = self.recv[0][0, x // 8, at]
        ends = []
        for b in range(2):
            corner = (self.recv[2][b, 1], self.recv[2][b, 0])
            if h == 8:
                ends.append(jnp.concatenate([self.recv[1][b], *corner], axis=0))
            else:
                sub = lax.broadcasted_iota(jnp.int32, (8, 128), 0)
                ends.append(
                    jnp.concatenate([self.recv[1][b], jnp.where(sub < h, *corner)], axis=0)
                )
        lane = lax.broadcasted_iota(jnp.int32, ends[0].shape, 1)
        both = jnp.where(lane % (2 * h) < h, ends[0], ends[1])
        edge = (lane < h) | (lane >= 128 - h)

        def slab(x, carry):
            moved = pltpu.roll(both, 128 - h - 2 * h * x, 1)
            ext[d + x, :, nz : nz + 128] = jnp.where(edge, moved, 0.0)
            return carry

        lax.fori_loop(0, nx, slab, 0, unroll=8)


def pair_up(src, pairs):
    def add(j, carry):
        pairs[j] = src[2 * j] + src[2 * j + 1]
        return carry

    lax.fori_loop(0, pairs.shape[0], add, 0)


def pooled(pairs, into, after):
    cx, ny, nz = pairs.shape
    depth = COARSE
    flat = pairs[...].reshape(cx * ny, nz)

    def halves(rows, cols, dim):
        r = lax.broadcasted_iota(jnp.int32, (rows, cols), dim)
        c = lax.broadcasted_iota(jnp.int32, (rows, cols), 1 - dim)
        return (r == jnp.right_shift(c, 1)).astype(jnp.float32).astype(jnp.bfloat16)

    along_z = halves(nz, nz // 2, 1)
    along_y = halves(cx * ny // 2, cx * ny, 0)
    flat = sum(jnp.dot(p, along_z, preferred_element_type=jnp.float32) for p in split3(flat))
    flat = sum(jnp.dot(along_y, p, preferred_element_type=jnp.float32) for p in split3(flat))
    out = after(0.5 * flat).reshape(cx, ny // 2, nz // 2)
    into[depth : depth + cx, : ny // 2, : nz // 2] = out


def fine_field(ext, bufs, sems, landing=None):
    ysend, yrecv, zsend, zrecv, yzrecv = bufs
    return Field(ext, FINE, 4, (ysend, zsend), (yrecv, zrecv, yzrecv), *sems, landing)


def coarse_field(ext, bufs, sems):
    zsend, zrecv, yzrecv = bufs
    return Field(ext, COARSE, 8, (None, zsend), (None, zrecv, yzrecv), *sems)


def buf(*shape):
    return pltpu.VMEM(shape, jnp.float32)


def wide_shapes(nx, ny, nz):
    cx, cy, cz = nx // 2, ny // 2, nz // 2
    return (
        (nx + 2 * FINE, ny + 8, nz + 128),
        (cx + 2 * COARSE, cy + 16, cz + 128),
    )


def fine_scratch(nx, ny, nz):
    rows = (2, nx // 8, 8 * FINE, nz)
    return [buf(*rows)] * 2 + [buf(2, ny, 128)] * 2 + [buf(2, 2, 8, 128)]


def coarse_scratch(nx, ny, nz):
    return [buf(2, ny // 2, 128)] * 2 + [buf(2, 2, 8, 128)]


FIRST, LAST = range(8), (8, 9)


def cycle_kernel(forcing, shift_hbm, inverse, cinverse, pressure, *scratch):
    shift, load_sem, scratch = scratch[0], scratch[-1], scratch[1:-1]
    fetch = pltpu.make_async_copy(shift_hbm, shift, load_sem)
    fetch.start()
    (rhs, one, two, update, land, crhs, cone, ctwo, cupdate, pairs), scratch = (
        scratch[:10], scratch[10:],
    )
    bufs_a, bufs_b, bufs_c = scratch[:5], scratch[5:10], scratch[10:13]
    send_sem, recv_sem = scratch[13:]
    nx, ny, nz = forcing.shape
    sems = [(send_sem.at[k], recv_sem.at[k]) for k in range(3)]

    def load(x, carry):
        rhs[FINE + x, :ny, :nz] = forcing[x]
        return carry

    lax.fori_loop(0, nx, load, 0, unroll=2)
    field = fine_field(rhs, bufs_a, sems[0])
    field.pack()
    greet(LINKS)
    field.start(FIRST)
    field.finish(FIRST)
    field.unpack()
    field.start(LAST)
    field.finish(LAST)

    slabs = nx + 2 * FINE
    pairs_of = factors(SMOOTH)
    bufs = (one, two)
    begin(rhs, inverse, one, update, slabs)
    for k in range(1, SMOOTH):
        sweep(rhs, inverse, bufs[(k - 1) % 2], bufs[k % 2], update, k, slabs - k, pairs_of[k])
    smooth = bufs[(SMOOTH - 1) % 2]
    other = bufs[SMOOTH % 2]

    fetch.wait()

    def residual(j, carry):
        for r in range(0, ny, 8):
            here = slice(r, r + 8)
            both = 0.0
            for half in range(2):
                x = 2 * j + half
                cells, total = around(smooth, FINE + x, r)
                total = total[:, :nz] + rhs[FINE + x, here, :nz]
                both = both + (total - (6.0 + shift[x, here]) * cells[:, :nz])
            pairs[j, here] = both
        return carry

    lax.fori_loop(0, nx // 2, residual, 0, unroll=2)
    pooled(pairs, crhs, lambda total: total)
    coarse = coarse_field(crhs, bufs_c, sems[2])
    coarse.pack()
    coarse.start(FIRST)
    field = fine_field(smooth, bufs_b, sems[1], land)
    field.pack()
    field.start(FIRST)
    cslabs = crhs.shape[0]
    low = COARSE - (FINE + 1) // 2
    count = cslabs - 2 * low
    cny, cnz = crhs.shape[1:]
    fny, fnz = smooth.shape[1:]

    def fan(shape, fine_dim, per_f, per_c, core, jump):
        f = lax.broadcasted_iota(jnp.int32, shape, fine_dim)
        c = lax.broadcasted_iota(jnp.int32, shape, 1 - fine_dim)
        block = 0
        for g in range(1, shape[fine_dim] // per_f):
            block = block + (f >= g * per_f).astype(jnp.int32)
        inner = f - block * per_f
        target = jnp.right_shift(inner, 1) + jnp.where(inner >= core, jump, 0) + block * per_c
        return (c == target).astype(jnp.float32).astype(jnp.bfloat16)

    fan_y = fan((count * fny, count * cny), 0, fny, cny, ny + 4, cny - fny // 2)
    fan_z = fan((cnz, fnz), 1, fnz, cnz, nz + 64, cnz - fnz // 2)
    coarse.finish(FIRST)
    coarse.unpack()
    coarse.start(LAST)
    field.finish(FIRST)
    field.unpack()
    field.start(LAST)
    coarse.finish(LAST)

    pairs_of = factors(COARSE_SMOOTH)
    cbufs = (cone, ctwo)
    begin(crhs, cinverse, cone, cupdate, cslabs)
    for k in range(1, COARSE_SMOOTH):
        sweep(
            crhs, cinverse, cbufs[(k - 1) % 2], cbufs[k % 2], cupdate, k, cslabs - k, pairs_of[k]
        )
    fix = cbufs[(COARSE_SMOOTH - 1) % 2]

    field.finish(LAST)
    flat = fix[low : low + count].reshape(count * cny, cnz)

    tall = sum(jnp.dot(fan_y, p, preferred_element_type=jnp.float32) for p in split3(flat))
    full = sum(jnp.dot(p, fan_z, preferred_element_type=jnp.float32) for p in split3(tall))
    for j in range(count):
        part = full[j * fny : (j + 1) * fny]
        for half in range(2):
            x = FINE + 2 * (low + j - COARSE) + half
            if 0 <= x < FINE:
                smooth[x] = land[0, x] + part
            elif FINE <= x < FINE + nx:
                smooth[x] = smooth[x] + part
            elif FINE + nx <= x < slabs:
                smooth[x] = land[1, x - FINE - nx] + part

    pairs_of = factors(SMOOTH)
    bufs = (smooth, other)

    for k in range(SMOOTH):
        sweep(
            rhs, inverse, bufs[k % 2], bufs[(k + 1) % 2], update,
            k + 1, slabs - k - 1, pairs_of[k], pressure if k == SMOOTH - 1 else None,
        )


def cycle(forcing, shift, inverse, cinverse):
    nx, ny, nz = forcing.shape
    wide, cwide = (buf(*shape) for shape in wide_shapes(nx, ny, nz))
    vmem = pl.BlockSpec(memory_space=pltpu.VMEM)
    return pl.pallas_call(
        cycle_kernel,
        in_specs=[vmem, pl.BlockSpec(memory_space=pltpu.HBM), vmem, vmem],
        out_specs=vmem,
        out_shape=jax.ShapeDtypeStruct(forcing.shape, jnp.float32),
        scratch_shapes=[buf(nx, ny, nz)]
        + [wide] * 4
        + [buf(2, FINE, ny + 8, nz + 128)]
        + [cwide] * 4
        + [buf(nx // 2, ny, nz)]
        + fine_scratch(nx, ny, nz) * 2
        + coarse_scratch(nx, ny, nz)
        + [pltpu.SemaphoreType.DMA((3, 10))] * 2
        + [pltpu.SemaphoreType.DMA],
        compiler_params=pltpu.CompilerParams(
            collective_id=1, has_side_effects=True, vmem_limit_bytes=VMEM_LIMIT
        ),
    )(forcing, in_hbm(shift), inverse, cinverse)


BIN = 256
AXES = ("gx", "gy", "gz")


def in_hbm(x):
    return pltpu.with_memory_space_constraint(x, pltpu.HBM)


def hot_rows(index, rows, dtype=jnp.bfloat16):
    r = lax.broadcasted_iota(jnp.int32, (rows, index.shape[1]), 0)
    if rows > BIN:
        return r == index
    return r.astype(jnp.float32).astype(dtype) == index.astype(jnp.float32).astype(dtype)


def place_of(index):
    where = {}
    for axis in reversed(AXES):
        count = lax.axis_size(axis)
        where[axis] = lax.rem(index, count)
        index = lax.div(index, count)
    return where


def front_kernel(
    ndevice, nbin, *refs
):
    sources, refs = refs[:8], refs[8:]
    (force_ref, got_ref, inverse, cinverse), refs = refs[:4], refs[4:]
    (pos_ref, nrm_ref, ten_ref, wgt_ref, con_ref, own_ref, cel_ref, shift), scratch = (
        refs[:8], refs[8:],
    )
    load_sem, scratch = scratch[-1], scratch[:-1]

    def fetch(k):
        return pltpu.make_async_copy(sources[k], refs[k], load_sem.at[k])

    for k in (7, 0, 5, 6, 4, 3, 2, 1):
        fetch(k).start()
    (packed_ref, total_ref, carry_ref, rank_ref, jump_ref, pad_ref, psend, precv, pairs), scratch = (
        scratch[:9], scratch[9:],
    )
    fine_bufs, coarse_bufs = scratch[:5], scratch[5:8]
    send_sem, recv_sem, all_send, all_recv, pos_send, pos_recv = scratch[8:]
    chunk = 4 * LANES
    split = 4
    per = 2 * split
    npoint = ten_ref.shape[1]
    nx, ny, nz = shift.shape
    zero, unit = jnp.zeros((), jnp.bfloat16), jnp.ones((), jnp.bfloat16)
    me = lax.axis_index(AXES)
    barrier = pltpu.get_barrier_semaphore()

    def other(p):
        return lax.rem(me + p, ndevice)

    def hello(p, carry):
        pl.semaphore_signal(barrier, inc=1, device_id=place_of(other(p)), device_id_type=MESH)
        return carry

    lax.fori_loop(1, ndevice, hello, 0)

    fetch(0).wait()
    psend[0, :3] = pos_ref[:, npoint - LANES :]
    psend[1, :3] = pos_ref[:, :LANES]

    def spread_out(j, carry):
        lower = pos_ref[:, pl.ds(pl.multiple_of(j * LANES - LANES, LANES), LANES)]
        upper = pos_ref[:, pl.ds(pl.multiple_of(j * LANES, LANES), LANES)]
        both = jnp.concatenate([lower[:, HALO:], upper[:, :HALO]], axis=1)
        pad_ref[:3, pl.ds(pl.multiple_of(j * LANES, LANES), LANES)] = both
        return carry

    lax.fori_loop(1, npoint // LANES, spread_out, 0, unroll=7)

    def edge(side, incoming):
        return pltpu.make_async_remote_copy(
            src_ref=psend.at[side],
            dst_ref=precv.at[side],
            send_sem=pos_send.at[side],
            recv_sem=pos_recv.at[side],
            device_id=place_of(other((1, ndevice - 1)[side])),
            device_id_type=MESH,
        )

    def classes(here):
        return own_ref[:, here] + ndevice * jnp.right_shift(cel_ref[:, here], 16)

    def count(i, total):
        here = pl.ds(pl.multiple_of(i * chunk, chunk), chunk)
        hot = jnp.where(hot_rows(classes(here), nbin * ndevice), 1.0, 0.0).astype(jnp.float32)
        return total + (
            hot[:, :LANES] + hot[:, LANES : 2 * LANES]
            + (hot[:, 2 * LANES : 3 * LANES] + hot[:, 3 * LANES :])
        )

    for k in (5, 6):
        fetch(k).wait()
    counts = lax.fori_loop(
        0, npoint // chunk, count, jnp.zeros((nbin * ndevice, LANES), jnp.float32), unroll=2
    )
    counts = jnp.sum(counts, axis=1, keepdims=True)
    base = jnp.zeros((ndevice, 1), jnp.float32)
    for b in range(nbin):
        carry_ref[b * ndevice : (b + 1) * ndevice] = base
        base = base + counts[b * ndevice : (b + 1) * ndevice]
    before = (
        lax.broadcasted_iota(jnp.int32, (chunk, chunk), 0)
        < lax.broadcasted_iota(jnp.int32, (chunk, chunk), 1)
    ).astype(jnp.float32).astype(jnp.bfloat16)

    def order(i, carry):
        here = pl.ds(pl.multiple_of(i * chunk, chunk), chunk)
        ones = jnp.where(hot_rows(classes(here), nbin * ndevice), unit, zero)
        earlier = jnp.dot(ones, before, preferred_element_type=jnp.float32) + carry
        wide = ones.astype(jnp.float32)
        rank_ref[:, here] = jnp.sum(wide * earlier, axis=0, keepdims=True).astype(jnp.int32)
        return carry + jnp.sum(wide, axis=1, keepdims=True)

    lax.fori_loop(0, npoint // chunk, order, carry_ref[...], unroll=2)

    pl.semaphore_wait(barrier, ndevice - 1)

    for side in range(2):
        edge(side, False).start()
    def rows_of(device):
        return pl.ds(pl.multiple_of(device * per, per), per)

    def deal(part, p, incoming):
        return pltpu.make_async_remote_copy(
            src_ref=packed_ref.at[part, rows_of(other(p))],
            dst_ref=got_ref.at[part, rows_of(other(ndevice - p) if incoming else me)],
            send_sem=all_send.at[part, p],
            recv_sem=all_recv.at[part, p],
            device_id=place_of(other(p)),
            device_id_type=MESH,
        )

    def send(part):
        def one(p, carry):
            deal(part, p, False).start()
            return carry

        lax.fori_loop(1, ndevice, one, 0)

    def pack(part, pieces):
        total_ref[...] = jnp.zeros_like(total_ref)

        def some(i, carry):
            here = pl.ds(pl.multiple_of(i * chunk, chunk), chunk)
            rank = rank_ref[:, here]
            slots = jnp.where(hot_rows(jnp.bitwise_and(rank, BIN - 1), BIN), unit, zero)
            row = own_ref[:, here] * split + jnp.right_shift(rank, 8)
            hot = hot_rows(row, total_ref.shape[0])
            total = total_ref[...]
            for piece in pieces(here):
                left = jnp.where(hot, piece, zero)
                total = total + lax.dot_general(
                    left, slots, (((1,), (1,)), ((), ())), preferred_element_type=jnp.float32
                )
            total_ref[...] = total
            return carry

        lax.fori_loop(0, npoint // chunk, some, 0, unroll=2)
        sub = lax.broadcasted_iota(jnp.int32, (per, LANES), 0)
        for t in range(ndevice // 2):
            one = total_ref[t * per : t * per + per, :LANES]
            two = total_ref[t * per : t * per + per, LANES:]
            at = 2 * t * per
            packed_ref[part, at : at + per] = jnp.where(sub < split, one, pltpu.roll(two, split, 0))
            packed_ref[part, at + per : at + 2 * per] = jnp.where(
                sub < split, pltpu.roll(one, split, 0), two
            )

    def digits(here):
        cell = cel_ref[:, here] + 1
        for bits in (0, 8, 16):
            digit = jnp.left_shift(jnp.bitwise_and(jnp.right_shift(cell, bits), 255), bits)
            yield digit.astype(jnp.float32).astype(jnp.bfloat16)

    pack(1, digits)
    send(1)
    fetch(7).wait()

    def load(x, carry):
        inverse[FINE + x, :ny, :nz] = 1.0 / (6.0 + shift[x])
        return carry

    lax.fori_loop(0, nx, load, 0, unroll=2)
    pair_up(shift, pairs)
    pooled(pairs, cinverse, lambda total: 1.0 / (6.0 + total))
    fine = fine_field(inverse, fine_bufs, (send_sem.at[0], recv_sem.at[0]))
    coarse = coarse_field(cinverse, coarse_bufs, (send_sem.at[1], recv_sem.at[1]))
    fine.pack()
    coarse.pack()
    fine.start(FIRST)
    coarse.start(FIRST)
    for k in (4, 3, 2, 1):
        fetch(k).wait()
    for side in range(2):
        edge(side, True).wait_send()
        edge(side, True).wait_recv()
    pad_ref[:3, :LANES] = jnp.concatenate(
        [precv[0, :3, HALO:], pos_ref[:, :HALO]], axis=1
    )
    pad_ref[:3, npoint:] = jnp.concatenate(
        [pos_ref[:, npoint - HALO :], precv[1, :3, :HALO]], axis=1
    )
    begin_at = me * npoint
    everything = npoint * ndevice

    def pull(i, carry):
        for sub in range(2):
            base = pl.multiple_of(i * 2 * LANES + sub * LANES, LANES)
            here = pl.ds(base, LANES)
            lower = pad_ref[:, here]
            upper = pad_ref[:, pl.ds(base + LANES, LANES)]
            centre_pos = jnp.concatenate([lower[:, HALO:], upper[:, :HALO]], axis=1)
            index = con_ref[:, here] - begin_at + HALO
            index = jnp.where(index < 0, index + everything, index)
            index = jnp.where(index >= everything, index - everything, index) - base
            total = jnp.zeros_like(lower)
            for which in range(con_ref.shape[0]):
                wide = jnp.broadcast_to(index[which : which + 1], lower.shape)
                low = jnp.bitwise_and(wide, LANES - 1)
                near_by = jnp.take_along_axis(lower, low, axis=1, mode="promise_in_bounds")
                far = jnp.take_along_axis(upper, low, axis=1, mode="promise_in_bounds")
                picked = jnp.where(wide < LANES, near_by, far)
                total = total + wgt_ref[which : which + 1, here] * (picked - centre_pos)
            force = ten_ref[:, here] * total[:3]
            force_ref[:, here] = force
            jump_ref[:, here] = jnp.sum(force * nrm_ref[:, here], axis=0, keepdims=True)
        return carry

    lax.fori_loop(0, npoint // (2 * LANES), pull, 0, unroll=2)

    pack(0, lambda here: split3(jump_ref[:, here])[:2])
    send(0)
    for part in range(2):
        got_ref[part, rows_of(me)] = packed_ref[part, rows_of(me)]
    fine.finish(FIRST)
    fine.unpack()
    fine.start(LAST)
    coarse.finish(FIRST)
    coarse.unpack()
    coarse.start(LAST)
    fine.finish(LAST)
    coarse.finish(LAST)

    def receive(p, carry):
        for part in range(2):
            deal(part, p, False).wait_send()
            deal(part, p, True).wait_recv()
        return carry

    lax.fori_loop(1, ndevice, receive, 0)


def front(
    positions, normals, tension, edge_weight, connectivity, owner_ids, cell_map, shift,
    ndevice, nbin,
):
    npoint = tension.shape[0]
    nx, ny, nz = shift.shape
    vmem = pl.BlockSpec(memory_space=pltpu.VMEM)
    wide, cwide = wide_shapes(nx, ny, nz)
    return pl.pallas_call(
        functools.partial(front_kernel, ndevice, nbin),
        in_specs=[pl.BlockSpec(memory_space=pltpu.HBM)] * 8,
        out_specs=[vmem] * 4,
        out_shape=[
            jax.ShapeDtypeStruct(shape, jnp.float32)
            for shape in ((3, npoint), (2, 8 * ndevice, LANES), wide, cwide)
        ],
        scratch_shapes=[
            buf(3, npoint),
            buf(3, npoint),
            buf(1, npoint),
            buf(*edge_weight.shape),
            pltpu.VMEM(connectivity.shape, jnp.int32),
            pltpu.VMEM((1, npoint), jnp.int32),
            pltpu.VMEM((1, npoint), jnp.int32),
            buf(nx, ny, nz),
            buf(2, 8 * ndevice, LANES),
            buf(4 * ndevice, BIN),
            buf(nbin * ndevice, 1),
            pltpu.VMEM((1, npoint), jnp.int32),
            buf(1, npoint),
            buf(8, npoint + LANES),
            buf(2, 8, LANES),
            buf(2, 8, LANES),
            buf(nx // 2, ny, nz),
        ]
        + fine_scratch(nx, ny, nz)
        + coarse_scratch(nx, ny, nz)
        + [pltpu.SemaphoreType.DMA((2, 10))] * 2
        + [pltpu.SemaphoreType.DMA((2, ndevice))] * 2
        + [pltpu.SemaphoreType.DMA((2,))] * 2
        + [pltpu.SemaphoreType.DMA((8,))],
        compiler_params=pltpu.CompilerParams(
            collective_id=0, has_side_effects=True, vmem_limit_bytes=20 * 2**20
        ),
    )(
        *map(
            in_hbm,
            (
                positions, normals, tension[None], edge_weight, connectivity, owner_ids[None],
                cell_map[None], shift,
            ),
        )
    )


GROUP = 24


def scatter_kernel(
    nbin, rhs_hbm, got_ref, force_ref, out_ref, force_hbm,
    rhs_ref, acc_ref, ends_ref, bound_ref, sems,
):
    nrow, nz = rhs_ref.shape
    fetch = pltpu.make_async_copy(rhs_hbm, rhs_ref, sems.at[1])
    fetch.start()
    put = pltpu.make_async_copy(force_ref, force_hbm, sems.at[2])
    put.start()
    nsource = bound_ref.shape[0]
    per = got_ref.shape[1] // nsource
    chunks = per
    rows = nrow // nbin
    got = got_ref[1].reshape(nsource, per, LANES)
    used = got > 0.0
    lane = lax.broadcasted_iota(jnp.int32, (nsource, LANES), 1)
    ends = jnp.zeros((nsource, LANES), jnp.float32)
    for b in range(nbin):
        inside = jnp.where(used & (got <= float((b + 1) * BIN * BIN)), 1.0, 0.0)
        total = jnp.sum(jnp.sum(inside, axis=1), axis=1, keepdims=True)
        ends = jnp.where(lane == b + 1, total, ends)
    ends_ref[...] = ends.astype(jnp.int32)
    copy = pltpu.make_async_copy(ends_ref, bound_ref, sems.at[0])
    copy.start()
    copy.wait()
    fetch.wait()
    level = lax.broadcasted_iota(jnp.int32, (BIN, LANES), 0).astype(jnp.float32)
    level = level.astype(jnp.bfloat16)
    zero, unit = jnp.zeros((), jnp.bfloat16), jnp.ones((), jnp.bfloat16)

    def quarter(b, carry):
        def span(source):
            at = jnp.minimum(source, nsource - 1)
            first = jnp.minimum(jnp.right_shift(bound_ref[at, b], 7), chunks - 1)
            last = jnp.right_shift(bound_ref[at, b + 1] + LANES - 1, 7)
            return first, jnp.maximum(last, first + 1)

        acc_ref[...] = jnp.zeros_like(acc_ref)

        def work(state):
            source, chunk, last = state
            highs, lows, cols = [], [], []
            for _ in range(GROUP):
                at = jnp.minimum(source, nsource - 1)
                half = jnp.bitwise_and(chunk, 1)
                row = at * per + half * (per // 2) + jnp.right_shift(chunk, 1)
                value = got_ref[0, pl.ds(row, 1)]
                cell = got_ref[1, pl.ds(row, 1)].astype(jnp.int32) - 1
                fits = (jnp.right_shift(cell, 16) == b) & (source < nsource)
                half = jnp.bitwise_and(jnp.right_shift(cell, 8), 1)
                place = half * rows + jnp.bitwise_and(jnp.right_shift(cell, 9), rows - 1)
                place = jnp.where(fits, place, BIN).astype(jnp.float32).astype(jnp.bfloat16)
                col = jnp.bitwise_and(cell, BIN - 1).astype(jnp.float32).astype(jnp.bfloat16)
                first = value.astype(jnp.bfloat16)
                second = (value - first.astype(jnp.float32)).astype(jnp.bfloat16)
                same = level == place
                highs.append(jnp.where(same, first, zero))
                lows.append(jnp.where(same, second, zero))
                cols.append(jnp.where(level == col, unit, zero))
                over = chunk + 1 >= last
                source = jnp.where(over, source + 1, source)
                following = span(source)
                chunk = jnp.where(over, following[0], chunk + 1)
                last = jnp.where(over, following[1], last)
            high = jnp.concatenate(highs, axis=1)
            low = jnp.concatenate(lows, axis=1)
            right = jnp.concatenate(cols, axis=1)
            dims = (((1,), (1,)), ((), ()))
            acc_ref[...] += lax.dot_general(
                high, right, dims, preferred_element_type=jnp.float32
            ) + lax.dot_general(low, right, dims, preferred_element_type=jnp.float32)
            return source, chunk, last

        lax.while_loop(lambda state: state[0] < nsource, work, (jnp.int32(0), *span(0)))
        here = pl.ds(pl.multiple_of(b * rows, rows), rows)
        for half in range(2):
            cols = slice(half * BIN, (half + 1) * BIN)
            out_ref[here, cols] = rhs_ref[here, cols] + acc_ref[half * rows : (half + 1) * rows]
        return carry

    lax.fori_loop(0, nbin, quarter, 0)
    put.wait()


def scatter(rhs, got, force, nsource, nbin):
    nx, ny, nz = rhs.shape
    nrow = nx * ny
    vmem = pl.BlockSpec(memory_space=pltpu.VMEM)
    hbm = pl.BlockSpec(memory_space=pltpu.HBM)
    out, force = pl.pallas_call(
        functools.partial(scatter_kernel, nbin),
        in_specs=[hbm, vmem, vmem],
        out_specs=[vmem, hbm],
        out_shape=[
            jax.ShapeDtypeStruct((nrow, nz), jnp.float32),
            jax.ShapeDtypeStruct(force.shape, jnp.float32),
        ],
        scratch_shapes=[
            pltpu.VMEM((nrow, nz), jnp.float32),
            pltpu.VMEM((BIN, BIN), jnp.float32),
            pltpu.VMEM((nsource, LANES), jnp.int32),
            pltpu.SMEM((nsource, LANES), jnp.int32),
            pltpu.SemaphoreType.DMA((3,)),
        ],
        compiler_params=pltpu.CompilerParams(vmem_limit_bytes=24 * 2**20),
        cost_estimate=pl.CostEstimate(
            flops=4 * nrow * nz * got.size // 2, bytes_accessed=4000000, transcendentals=0
        ),
    )(in_hbm(rhs.reshape(nrow, nz)), got, force)
    return out.reshape(nx, ny, nz), force


def body(
    pressure_rhs,
    shift_diag,
    positions,
    normals,
    tension,
    edge_weight,
    owner_map,
    cell_map,
    connectivity,
):
    ndevice = lax.axis_size(AXES)
    nbin = pressure_rhs.size // (BIN * BIN)
    surface_force, got, inverse, cinverse = front(
        positions, normals, tension, edge_weight, connectivity, owner_map[:, 0], cell_map,
        shift_diag, ndevice, nbin,
    )
    forcing, surface_force = scatter(pressure_rhs, got, surface_force, ndevice, nbin)
    pressure = cycle(forcing, shift_diag, inverse, cinverse)
    return (pressure, surface_force)


def solution(mesh):
    return jax.shard_map(
        body,
        mesh=mesh,
        in_specs=(
            P("gx", "gy", "gz"),
            P("gx", "gy", "gz"),
            P(None, ("gx", "gy", "gz")),
            P(None, ("gx", "gy", "gz")),
            P(("gx", "gy", "gz")),
            P(None, ("gx", "gy", "gz")),
            P(("gx", "gy", "gz"), None),
            P(("gx", "gy", "gz")),
            P(None, ("gx", "gy", "gz")),
        ),
        out_specs=(P("gx", "gy", "gz"), P(None, ("gx", "gy", "gz"))),
        check_vma=False,
    )
```

```python
import functools

import jax
import jax.numpy as jnp
from jax import lax
from jax.experimental import pallas as pl
from jax.experimental.pallas import tpu as pltpu
from jax.sharding import PartitionSpec as P

HALO = 64
SMOOTH = 3
COARSE_SMOOTH = 4
LANES = 2 * HALO


centre = 1.125
spread = 0.875


def factors(sweeps):
    ratio = centre / spread
    fac = 1.0 / ratio
    pairs = [(0.0, 1.0 / centre)]
    for _ in range(1, sweeps):
        fac_new = 1.0 / (2.0 * ratio - fac)
        pairs.append((fac_new * fac, 2.0 * fac_new / spread))
        fac = fac_new
    return pairs


def split3(x):
    a = x.astype(jnp.bfloat16)
    rest = x - a.astype(jnp.float32)
    b = rest.astype(jnp.bfloat16)
    c = (rest - b.astype(jnp.float32)).astype(jnp.bfloat16)
    return a, b, c


MESH = pl.DeviceIdType.MESH
FINE = SMOOTH
COARSE = COARSE_SMOOTH - 1 + (SMOOTH + 1) // 2


UNROLL = 4
VMEM_LIMIT = 36 * 2**20


def around(src, x, r):
    ny, nz = src.shape[1:]
    sub = lax.broadcasted_iota(jnp.int32, (8, nz), 0)
    here = slice(r, r + 8)
    below, above = (r - 8) % ny, (r + 8) % ny
    cells = src[x, here]
    total = src[x - 1, here] + src[x + 1, here]
    total = total + (
        pltpu.roll(jnp.where(sub == 7, src[x, below : below + 8], cells), 1, 0)
        + pltpu.roll(jnp.where(sub == 0, src[x, above : above + 8], cells), 7, 0)
    )
    return cells, total + (pltpu.roll(cells, 1, 1) + pltpu.roll(cells, nz - 1, 1))


def sweep(rhs, inverse, src, dst, update, first, last, pair, keep=None):
    old, new = pair
    rows = src.shape[1] if keep is None else keep.shape[1]

    def slab(x, carry):
        for r in range(0, rows, 8):
            here = slice(r, r + 8)
            cells, total = around(src, x, r)
            change = new * (inverse[x, here] * (rhs[x, here] + total) - cells)
            if old:
                change = change + old * update[x, here]
            if keep is None:
                update[x, here] = change
                dst[x, here] = cells + change
            else:
                keep[x - first, here] = (cells + change)[:, : keep.shape[2]]
        return carry

    lax.fori_loop(first, last, slab, 0, unroll=UNROLL)


def begin(rhs, inverse, dst, update, slabs):
    def slab(x, carry):
        change = inverse[x] * rhs[x] * (1.0 / centre)
        update[x] = change
        dst[x] = change
        return carry

    lax.fori_loop(0, slabs, slab, 0, unroll=2)


def near(axes):
    ok = None
    where = {}
    for axis, step in axes:
        place = lax.axis_index(axis) + step
        fits = (place >= 0) & (place < lax.axis_size(axis))
        ok = fits if ok is None else ok & fits
        where[axis] = place
    return ok, where


SIDES = (-1, 1)
LINKS = (
    [(("gy", a),) for a in SIDES]
    + [(("gz", b),) for b in SIDES]
    + [(("gy", a), ("gz", b)) for b in SIDES for a in SIDES]
    + [(("gx", a),) for a in SIDES]
)
MIRROR = [1, 0, 3, 2, 7, 6, 5, 4, 9, 8]


def greet(links):
    barrier = pltpu.get_barrier_semaphore()
    peers = 0
    for link in links:
        ok, where = near(link)
        peers = peers + ok.astype(jnp.int32)

        @pl.when(ok)
        def _():
            pl.semaphore_signal(barrier, inc=1, device_id=where, device_id_type=MESH)

    pl.semaphore_wait(barrier, peers)


class Field:
    def __init__(self, ext, depth, wide, send, recv, send_sem, recv_sem, land=None):
        self.ext, self.depth, self.wide = ext, depth, wide
        self.send, self.recv = send, recv
        self.send_sem, self.recv_sem = send_sem, recv_sem
        self.land = land
        self.nx = ext.shape[0] - 2 * depth
        self.ny = ext.shape[1] - 2 * wide
        self.nz = ext.shape[2] - 128

    def message(self, m):
        d, nx, ny, nz, h = self.depth, self.nx, self.ny, self.nz, self.wide
        ext = self.ext
        if m < 2:
            if h == 8:
                rows = (0, ny - h)[m]
                src = ext.at[pl.ds(d, nx), pl.ds(rows, h), pl.ds(0, nz)]
                place = (ny + h, ny)[m]
                got = ext.at[pl.ds(d, nx), pl.ds(place, h), pl.ds(0, nz)]
                other = ext.at[pl.ds(d, nx), pl.ds((ny, ny + h)[m], h), pl.ds(0, nz)]
            else:
                src = self.send[0].at[m]
                got = self.recv[0].at[m]
                other = self.recv[0].at[1 - m]
        elif m < 4:
            src = self.send[1].at[m - 2]
            got = self.recv[1].at[m - 2]
            other = self.recv[1].at[3 - m]
        elif m < 8:
            b, a = divmod(m - 4, 2)
            src = self.send[1].at[b, pl.ds((0, ny - 8)[a], 8)]
            got = self.recv[2].at[b, a]
            other = self.recv[2].at[1 - b, 1 - a]
        else:
            a = m - 8
            src = ext.at[pl.ds((d, nx)[a], d)]
            if self.land is None:
                got = ext.at[pl.ds((0, d + nx)[a], d)]
                other = ext.at[pl.ds((d + nx, 0)[a], d)]
            else:
                got = self.land.at[a]
                other = self.land.at[1 - a]
        return src, other, got

    def copy(self, m, incoming):
        src, other, got = self.message(m)
        k = m if incoming else MIRROR[m]
        return pltpu.make_async_remote_copy(
            src_ref=got if incoming else src,
            dst_ref=got if incoming else other,
            send_sem=self.send_sem.at[m],
            recv_sem=self.recv_sem.at[k],
            device_id=near(LINKS[m])[1],
            device_id_type=MESH,
        )

    def start(self, which):
        for m in which:
            @pl.when(near(LINKS[m])[0])
            def _():
                self.copy(m, False).start()

    def finish(self, which):
        for m in which:
            ok = near(LINKS[m])[0]

            @pl.when(ok)
            def _():
                self.copy(m, False).wait_send()
                self.copy(m, True).wait_recv()

            @pl.when(jnp.logical_not(ok))
            def _():
                got = self.message(m)[2]
                got[...] = jnp.zeros(got.shape, jnp.float32)

    def pack(self):
        d, nx, ny, nz, h = self.depth, self.nx, self.ny, self.nz, self.wide
        ext = self.ext
        if h != 8:
            for x in range(nx):
                at = slice(d * (x % 8), d * (x % 8) + d)
                self.send[0][0, x // 8, at] = ext[d + x, :d, :nz]
                self.send[0][1, x // 8, at] = ext[d + x, ny - d : ny, :nz]
        group = lax.broadcasted_iota(jnp.int32, (ny, 128), 1) // (2 * h)

        def slab(x, carry):
            low, high = carry
            mine = group == x
            shift = 2 * h * x + h
            low = jnp.where(mine, pltpu.roll(ext[d + x, :ny, :128], shift, 1), low)
            high = jnp.where(mine, pltpu.roll(ext[d + x, :ny, nz - 128 : nz], shift, 1), high)
            return low, high

        zero = jnp.zeros((ny, 128), jnp.float32)
        low, high = lax.fori_loop(0, nx, slab, (zero, zero), unroll=8)
        self.send[1][0] = low
        self.send[1][1] = high

    def unpack(self):
        d, nx, ny, nz, h = self.depth, self.nx, self.ny, self.nz, self.wide
        ext = self.ext
        if h != 8:
            for x in range(nx):
                at = slice(d * (x % 8), d * (x % 8) + d)
                ext[d + x, ny : ny + d, :nz] = self.recv[0][1, x // 8, at]
                ext[d + x, ny + 8 - d : ny + 8, :nz] = self.recv[0][0, x // 8, at]
        ends = []
        for b in range(2):
            corner = (self.recv[2][b, 1], self.recv[2][b, 0])
            if h == 8:
                ends.append(jnp.concatenate([self.recv[1][b], *corner], axis=0))
            else:
                sub = lax.broadcasted_iota(jnp.int32, (8, 128), 0)
                ends.append(
                    jnp.concatenate([self.recv[1][b], jnp.where(sub < h, *corner)], axis=0)
                )
        lane = lax.broadcasted_iota(jnp.int32, ends[0].shape, 1)
        both = jnp.where(lane % (2 * h) < h, ends[0], ends[1])
        edge = (lane < h) | (lane >= 128 - h)

        def slab(x, carry):
            moved = pltpu.roll(both, 128 - h - 2 * h * x, 1)
            ext[d + x, :, nz : nz + 128] = jnp.where(edge, moved, 0.0)
            return carry

        lax.fori_loop(0, nx, slab, 0, unroll=8)


def pair_up(src, pairs):
    def add(j, carry):
        pairs[j] = src[2 * j] + src[2 * j + 1]
        return carry

    lax.fori_loop(0, pairs.shape[0], add, 0)


def pooled(pairs, into, after):
    cx, ny, nz = pairs.shape
    depth = COARSE
    flat = pairs[...].reshape(cx * ny, nz)

    def halves(rows, cols, dim):
        r = lax.broadcasted_iota(jnp.int32, (rows, cols), dim)
        c = lax.broadcasted_iota(jnp.int32, (rows, cols), 1 - dim)
        return (r == jnp.right_shift(c, 1)).astype(jnp.float32).astype(jnp.bfloat16)

    along_z = halves(nz, nz // 2, 1)
    along_y = halves(cx * ny // 2, cx * ny, 0)
    flat = sum(jnp.dot(p, along_z, preferred_element_type=jnp.float32) for p in split3(flat)[:2])
    flat = sum(jnp.dot(along_y, p, preferred_element_type=jnp.float32) for p in split3(flat)[:2])
    out = after(0.5 * flat).reshape(cx, ny // 2, nz // 2)
    into[depth : depth + cx, : ny // 2, : nz // 2] = out


def fine_field(ext, bufs, sems, landing=None):
    ysend, yrecv, zsend, zrecv, yzrecv = bufs
    return Field(ext, FINE, 4, (ysend, zsend), (yrecv, zrecv, yzrecv), *sems, landing)


def coarse_field(ext, bufs, sems):
    zsend, zrecv, yzrecv = bufs
    return Field(ext, COARSE, 8, (None, zsend), (None, zrecv, yzrecv), *sems)


def buf(*shape):
    return pltpu.VMEM(shape, jnp.float32)


def wide_shapes(nx, ny, nz):
    cx, cy, cz = nx // 2, ny // 2, nz // 2
    return (
        (nx + 2 * FINE, ny + 8, nz + 128),
        (cx + 2 * COARSE, cy + 16, cz + 128),
    )


def fine_scratch(nx, ny, nz):
    rows = (2, nx // 8, 8 * FINE, nz)
    return [buf(*rows)] * 2 + [buf(2, ny, 128)] * 2 + [buf(2, 2, 8, 128)]


def coarse_scratch(nx, ny, nz):
    return [buf(2, ny // 2, 128)] * 2 + [buf(2, 2, 8, 128)]


FIRST, LAST = range(8), (8, 9)


def cycle_kernel(forcing, shift_hbm, inverse, cinverse, pressure, *scratch):
    shift, load_sem, scratch = scratch[0], scratch[-1], scratch[1:-1]
    fetch = pltpu.make_async_copy(shift_hbm, shift, load_sem)
    fetch.start()
    (rhs, one, two, update, land, crhs, cone, ctwo, cupdate, pairs), scratch = (
        scratch[:10], scratch[10:],
    )
    bufs_a, bufs_b, bufs_c = scratch[:5], scratch[5:10], scratch[10:13]
    send_sem, recv_sem = scratch[13:]
    nx, ny, nz = forcing.shape
    sems = [(send_sem.at[k], recv_sem.at[k]) for k in range(3)]

    def load(x, carry):
        rhs[FINE + x, :ny, :nz] = forcing[x]
        return carry

    lax.fori_loop(0, nx, load, 0, unroll=2)
    field = fine_field(rhs, bufs_a, sems[0])
    field.pack()
    greet(LINKS)
    field.start(FIRST)
    field.finish(FIRST)
    field.unpack()
    field.start(LAST)
    field.finish(LAST)

    slabs = nx + 2 * FINE
    pairs_of = factors(SMOOTH)
    bufs = (one, two)
    begin(rhs, inverse, one, update, slabs)
    for k in range(1, SMOOTH):
        sweep(rhs, inverse, bufs[(k - 1) % 2], bufs[k % 2], update, k, slabs - k, pairs_of[k])
    smooth = bufs[(SMOOTH - 1) % 2]
    other = bufs[SMOOTH % 2]

    fetch.wait()

    def residual(j, carry):
        for r in range(0, ny, 8):
            here = slice(r, r + 8)
            both = 0.0
            for half in range(2):
                x = 2 * j + half
                cells, total = around(smooth, FINE + x, r)
                total = total[:, :nz] + rhs[FINE + x, here, :nz]
                both = both + (total - (6.0 + shift[x, here]) * cells[:, :nz])
            pairs[j, here] = both
        return carry

    lax.fori_loop(0, nx // 2, residual, 0, unroll=2)
    pooled(pairs, crhs, lambda total: total)
    coarse = coarse_field(crhs, bufs_c, sems[2])
    coarse.pack()
    coarse.start(FIRST)
    field = fine_field(smooth, bufs_b, sems[1], land)
    field.pack()
    field.start(FIRST)
    cslabs = crhs.shape[0]
    low = COARSE - (FINE + 1) // 2
    count = cslabs - 2 * low
    cny, cnz = crhs.shape[1:]
    fny, fnz = smooth.shape[1:]

    def fan(shape, fine_dim, per_f, per_c, core, jump):
        f = lax.broadcasted_iota(jnp.int32, shape, fine_dim)
        c = lax.broadcasted_iota(jnp.int32, shape, 1 - fine_dim)
        block = 0
        for g in range(1, shape[fine_dim] // per_f):
            block = block + (f >= g * per_f).astype(jnp.int32)
        inner = f - block * per_f
        target = jnp.right_shift(inner, 1) + jnp.where(inner >= core, jump, 0) + block * per_c
        return (c == target).astype(jnp.float32).astype(jnp.bfloat16)

    fan_y = fan((count * fny, count * cny), 0, fny, cny, ny + 4, cny - fny // 2)
    fan_z = fan((cnz, fnz), 1, fnz, cnz, nz + 64, cnz - fnz // 2)
    coarse.finish(FIRST)
    coarse.unpack()
    coarse.start(LAST)
    coarse.finish(LAST)

    pairs_of = factors(COARSE_SMOOTH)
    cbufs = (cone, ctwo)
    begin(crhs, cinverse, cone, cupdate, cslabs)
    for k in range(1, COARSE_SMOOTH):
        sweep(
            crhs, cinverse, cbufs[(k - 1) % 2], cbufs[k % 2], cupdate, k, cslabs - k, pairs_of[k]
        )
    field.finish(FIRST)
    field.unpack()
    field.start(LAST)
    fix = cbufs[(COARSE_SMOOTH - 1) % 2]

    flat = fix[low : low + count].reshape(count * cny, cnz)

    tall = sum(jnp.dot(fan_y, p, preferred_element_type=jnp.float32) for p in split3(flat)[:2])
    full = sum(jnp.dot(p, fan_z, preferred_element_type=jnp.float32) for p in split3(tall)[:2])
    field.finish(LAST)
    for j in range(count):
        part = full[j * fny : (j + 1) * fny]
        for half in range(2):
            x = FINE + 2 * (low + j - COARSE) + half
            if 0 <= x < FINE:
                smooth[x] = land[0, x] + part
            elif FINE <= x < FINE + nx:
                smooth[x] = smooth[x] + part
            elif FINE + nx <= x < slabs:
                smooth[x] = land[1, x - FINE - nx] + part

    pairs_of = factors(SMOOTH)
    bufs = (smooth, other)

    for k in range(SMOOTH):
        sweep(
            rhs, inverse, bufs[k % 2], bufs[(k + 1) % 2], update,
            k + 1, slabs - k - 1, pairs_of[k], pressure if k == SMOOTH - 1 else None,
        )


def cycle(forcing, shift, inverse, cinverse):
    nx, ny, nz = forcing.shape
    wide, cwide = (buf(*shape) for shape in wide_shapes(nx, ny, nz))
    vmem = pl.BlockSpec(memory_space=pltpu.VMEM)
    return pl.pallas_call(
        cycle_kernel,
        in_specs=[vmem, pl.BlockSpec(memory_space=pltpu.HBM), vmem, vmem],
        out_specs=vmem,
        out_shape=jax.ShapeDtypeStruct(forcing.shape, jnp.float32),
        scratch_shapes=[buf(nx, ny, nz)]
        + [wide] * 4
        + [buf(2, FINE, ny + 8, nz + 128)]
        + [cwide] * 4
        + [buf(nx // 2, ny, nz)]
        + fine_scratch(nx, ny, nz) * 2
        + coarse_scratch(nx, ny, nz)
        + [pltpu.SemaphoreType.DMA((3, 10))] * 2
        + [pltpu.SemaphoreType.DMA],
        compiler_params=pltpu.CompilerParams(
            collective_id=1, has_side_effects=True, vmem_limit_bytes=VMEM_LIMIT
        ),
    )(forcing, in_hbm(shift), inverse, cinverse)


BIN = 256
BIN_SHIFT = 16
BIN_CELLS = 1 << BIN_SHIFT
AXES = ("gx", "gy", "gz")


def in_hbm(x):
    return pltpu.with_memory_space_constraint(x, pltpu.HBM)


def levels(rows):
    level = lax.broadcasted_iota(jnp.int32, (rows, LANES), 0)
    if rows > BIN:
        return level
    return level.astype(jnp.float32).astype(jnp.bfloat16)


def hot_rows(level, index, values=None):
    if level.dtype != jnp.int32:
        index = index.astype(jnp.float32).astype(jnp.bfloat16)
    columns = []
    for at in range(0, index.shape[1], LANES):
        here = slice(at, at + LANES)
        value = jnp.ones((), jnp.bfloat16) if values is None else values[:, here]
        same = level == index[:, here]
        columns.append(jnp.where(same, value, jnp.zeros((), jnp.bfloat16)))
    return jnp.concatenate(columns, axis=1)


def place_of(index):
    where = {}
    for axis in reversed(AXES):
        count = lax.axis_size(axis)
        where[axis] = lax.rem(index, count)
        index = lax.div(index, count)
    return where


def front_kernel(
    ndevice, nbin, *refs
):
    sources, refs = refs[:8], refs[8:]
    (force_ref, got_ref, inverse, cinverse), refs = refs[:4], refs[4:]
    (pos_ref, nrm_ref, ten_ref, wgt_ref, con_ref, own_ref, cel_ref, shift), scratch = (
        refs[:8], refs[8:],
    )
    load_sem, scratch = scratch[-1], scratch[:-1]

    def fetch(k):
        return pltpu.make_async_copy(sources[k], refs[k], load_sem.at[k])

    for k in (7, 0, 5, 6, 4, 3, 2, 1):
        fetch(k).start()
    (packed_ref, total_ref, carry_ref, rank_ref, jump_ref, pad_ref, psend, precv, pairs), scratch = (
        scratch[:9], scratch[9:],
    )
    fine_bufs, coarse_bufs = scratch[:5], scratch[5:8]
    send_sem, recv_sem, all_send, all_recv, pos_send, pos_recv = scratch[8:]
    chunk = 4 * LANES
    split = 4
    per = 2 * split
    npoint = ten_ref.shape[1]
    nx, ny, nz = shift.shape
    class_level, slot_level = levels(nbin * ndevice), levels(BIN)
    row_level = levels(total_ref.shape[0])
    me = lax.axis_index(AXES)
    barrier = pltpu.get_barrier_semaphore()

    def other(p):
        return lax.rem(me + p, ndevice)

    def hello(p, carry):
        pl.semaphore_signal(barrier, inc=1, device_id=place_of(other(p)), device_id_type=MESH)
        return carry

    lax.fori_loop(1, ndevice, hello, 0)

    fetch(0).wait()
    psend[0, :3] = pos_ref[:, npoint - LANES :]
    psend[1, :3] = pos_ref[:, :LANES]

    def spread_out(j, carry):
        lower = pos_ref[:, pl.ds(pl.multiple_of(j * LANES - LANES, LANES), LANES)]
        upper = pos_ref[:, pl.ds(pl.multiple_of(j * LANES, LANES), LANES)]
        both = jnp.concatenate([lower[:, HALO:], upper[:, :HALO]], axis=1)
        pad_ref[:3, pl.ds(pl.multiple_of(j * LANES, LANES), LANES)] = both
        return carry

    lax.fori_loop(1, npoint // LANES, spread_out, 0, unroll=7)

    def edge(side, incoming):
        return pltpu.make_async_remote_copy(
            src_ref=psend.at[side],
            dst_ref=precv.at[side],
            send_sem=pos_send.at[side],
            recv_sem=pos_recv.at[side],
            device_id=place_of(other((1, ndevice - 1)[side])),
            device_id_type=MESH,
        )

    def classes(here):
        return own_ref[:, here] + ndevice * jnp.right_shift(cel_ref[:, here], BIN_SHIFT)

    def count(i, total):
        here = pl.ds(pl.multiple_of(i * chunk, chunk), chunk)
        hot = hot_rows(class_level, classes(here)).astype(jnp.float32)
        return total + (
            hot[:, :LANES] + hot[:, LANES : 2 * LANES]
            + (hot[:, 2 * LANES : 3 * LANES] + hot[:, 3 * LANES :])
        )

    for k in (5, 6):
        fetch(k).wait()
    counts = lax.fori_loop(
        0, npoint // chunk, count, jnp.zeros((nbin * ndevice, LANES), jnp.float32), unroll=2
    )
    counts = jnp.sum(counts, axis=1, keepdims=True)
    base = jnp.zeros((ndevice, 1), jnp.float32)
    for b in range(nbin):
        carry_ref[b * ndevice : (b + 1) * ndevice] = base
        base = base + counts[b * ndevice : (b + 1) * ndevice]
    before = (
        lax.broadcasted_iota(jnp.int32, (chunk, chunk), 0)
        < lax.broadcasted_iota(jnp.int32, (chunk, chunk), 1)
    ).astype(jnp.float32).astype(jnp.bfloat16)

    def order(i, carry):
        here = pl.ds(pl.multiple_of(i * chunk, chunk), chunk)
        ones = hot_rows(class_level, classes(here))
        earlier = jnp.dot(ones, before, preferred_element_type=jnp.float32) + carry
        wide = ones.astype(jnp.float32)
        rank_ref[:, here] = jnp.sum(wide * earlier, axis=0, keepdims=True).astype(jnp.int32)
        return carry + jnp.sum(wide, axis=1, keepdims=True)

    lax.fori_loop(0, npoint // chunk, order, carry_ref[...], unroll=2)

    fetch(7).wait()

    def load(x, carry):
        inverse[FINE + x, :ny, :nz] = 1.0 / (6.0 + shift[x])
        return carry

    lax.fori_loop(0, nx, load, 0, unroll=2)
    pair_up(shift, pairs)
    pooled(pairs, cinverse, lambda total: 1.0 / (6.0 + total))
    fine = fine_field(inverse, fine_bufs, (send_sem.at[0], recv_sem.at[0]))
    coarse = coarse_field(cinverse, coarse_bufs, (send_sem.at[1], recv_sem.at[1]))
    fine.pack()
    coarse.pack()
    pl.semaphore_wait(barrier, ndevice - 1)

    for side in range(2):
        edge(side, False).start()
    fine.start(FIRST)
    coarse.start(FIRST)

    def rows_of(device):
        return pl.ds(pl.multiple_of(device * per, per), per)

    def deal(part, p, incoming):
        return pltpu.make_async_remote_copy(
            src_ref=packed_ref.at[part, rows_of(other(p))],
            dst_ref=got_ref.at[part, rows_of(other(ndevice - p) if incoming else me)],
            send_sem=all_send.at[part, p],
            recv_sem=all_recv.at[part, p],
            device_id=place_of(other(p)),
            device_id_type=MESH,
        )

    def send(part):
        def one(p, carry):
            deal(part, p, False).start()
            return carry

        lax.fori_loop(1, ndevice, one, 0)

    def pack(part, pieces):
        total_ref[...] = jnp.zeros_like(total_ref)

        big = npoint // 2

        def some(i, carry):
            here = pl.ds(pl.multiple_of(i * big, big), big)
            rank = rank_ref[:, here]
            slots = hot_rows(slot_level, jnp.bitwise_and(rank, BIN - 1))
            row = own_ref[:, here] * split + jnp.right_shift(rank, 8)
            left = [hot_rows(row_level, row, piece) for piece in pieces(here)]
            both = lax.dot_general(
                jnp.concatenate(left, axis=0), slots, (((1,), (1,)), ((), ())),
                preferred_element_type=jnp.float32,
            )
            count = total_ref.shape[0]
            total_ref[...] += sum(both[k * count : k * count + count] for k in range(len(left)))
            return carry

        lax.fori_loop(0, npoint // big, some, 0)
        sub = lax.broadcasted_iota(jnp.int32, (per, LANES), 0)
        for t in range(ndevice // 2):
            one = total_ref[t * per : t * per + per, :LANES]
            two = total_ref[t * per : t * per + per, LANES:]
            at = 2 * t * per
            packed_ref[part, at : at + per] = jnp.where(sub < split, one, pltpu.roll(two, split, 0))
            packed_ref[part, at + per : at + 2 * per] = jnp.where(
                sub < split, pltpu.roll(one, split, 0), two
            )

    def digits(here):
        cell = cel_ref[:, here] + 1
        for bits in (0, 8, 16):
            digit = jnp.left_shift(jnp.bitwise_and(jnp.right_shift(cell, bits), 255), bits)
            yield digit.astype(jnp.float32).astype(jnp.bfloat16)

    pack(1, digits)
    send(1)
    for k in (4, 3, 2, 1):
        fetch(k).wait()
    for side in range(2):
        edge(side, True).wait_send()
        edge(side, True).wait_recv()
    pad_ref[:3, :LANES] = jnp.concatenate(
        [precv[0, :3, HALO:], pos_ref[:, :HALO]], axis=1
    )
    pad_ref[:3, npoint:] = jnp.concatenate(
        [pos_ref[:, npoint - HALO :], precv[1, :3, :HALO]], axis=1
    )
    begin_at = me * npoint
    everything = npoint * ndevice

    def pull(i, carry):
        for sub in range(2):
            base = pl.multiple_of(i * 2 * LANES + sub * LANES, LANES)
            here = pl.ds(base, LANES)
            lower = pad_ref[:, here]
            upper = pad_ref[:, pl.ds(base + LANES, LANES)]
            centre_pos = jnp.concatenate([lower[:, HALO:], upper[:, :HALO]], axis=1)
            index = con_ref[:, here] - begin_at + HALO
            index = jnp.where(index < 0, index + everything, index)
            index = jnp.where(index >= everything, index - everything, index) - base
            total = jnp.zeros_like(lower)
            for which in range(con_ref.shape[0]):
                wide = jnp.broadcast_to(index[which : which + 1], lower.shape)
                low = jnp.bitwise_and(wide, LANES - 1)
                near_by = jnp.take_along_axis(lower, low, axis=1, mode="promise_in_bounds")
                far = jnp.take_along_axis(upper, low, axis=1, mode="promise_in_bounds")
                picked = jnp.where(wide < LANES, near_by, far)
                total = total + wgt_ref[which : which + 1, here] * (picked - centre_pos)
            force = ten_ref[:, here] * total[:3]
            force_ref[:, here] = force
            jump_ref[:, here] = jnp.sum(force * nrm_ref[:, here], axis=0, keepdims=True)
        return carry

    lax.fori_loop(0, npoint // (2 * LANES), pull, 0, unroll=4)

    pack(0, lambda here: split3(jump_ref[:, here])[:2])
    send(0)
    for part in range(2):
        got_ref[part, rows_of(me)] = packed_ref[part, rows_of(me)]
    fine.finish(FIRST)
    fine.unpack()
    fine.start(LAST)
    coarse.finish(FIRST)
    coarse.unpack()
    coarse.start(LAST)
    fine.finish(LAST)
    coarse.finish(LAST)

    def receive(p, carry):
        for part in range(2):
            deal(part, p, False).wait_send()
            deal(part, p, True).wait_recv()
        return carry

    lax.fori_loop(1, ndevice, receive, 0)


def front(
    positions, normals, tension, edge_weight, connectivity, owner_ids, cell_map, shift,
    ndevice, nbin,
):
    npoint = tension.shape[0]
    nx, ny, nz = shift.shape
    vmem = pl.BlockSpec(memory_space=pltpu.VMEM)
    wide, cwide = wide_shapes(nx, ny, nz)
    return pl.pallas_call(
        functools.partial(front_kernel, ndevice, nbin),
        in_specs=[pl.BlockSpec(memory_space=pltpu.HBM)] * 8,
        out_specs=[vmem] * 4,
        out_shape=[
            jax.ShapeDtypeStruct(shape, jnp.float32)
            for shape in ((3, npoint), (2, 8 * ndevice, LANES), wide, cwide)
        ],
        scratch_shapes=[
            buf(3, npoint),
            buf(3, npoint),
            buf(1, npoint),
            buf(*edge_weight.shape),
            pltpu.VMEM(connectivity.shape, jnp.int32),
            pltpu.VMEM((1, npoint), jnp.int32),
            pltpu.VMEM((1, npoint), jnp.int32),
            buf(nx, ny, nz),
            buf(2, 8 * ndevice, LANES),
            buf(4 * ndevice, BIN),
            buf(nbin * ndevice, 1),
            pltpu.VMEM((1, npoint), jnp.int32),
            buf(1, npoint),
            buf(8, npoint + LANES),
            buf(2, 8, LANES),
            buf(2, 8, LANES),
            buf(nx // 2, ny, nz),
        ]
        + fine_scratch(nx, ny, nz)
        + coarse_scratch(nx, ny, nz)
        + [pltpu.SemaphoreType.DMA((2, 10))] * 2
        + [pltpu.SemaphoreType.DMA((2, ndevice))] * 2
        + [pltpu.SemaphoreType.DMA((2,))] * 2
        + [pltpu.SemaphoreType.DMA((8,))],
        compiler_params=pltpu.CompilerParams(
            collective_id=0, has_side_effects=True, vmem_limit_bytes=20 * 2**20
        ),
    )(
        *map(
            in_hbm,
            (
                positions, normals, tension[None], edge_weight, connectivity, owner_ids[None],
                cell_map[None], shift,
            ),
        )
    )


GROUP = 24


def scatter_kernel(
    nbin, rhs_hbm, got_ref, force_ref, out_ref, force_hbm,
    rhs_ref, acc_ref, ends_ref, bound_ref, sems,
):
    nrow, nz = rhs_ref.shape
    fetch = pltpu.make_async_copy(rhs_hbm, rhs_ref, sems.at[1])
    fetch.start()
    put = pltpu.make_async_copy(force_ref, force_hbm, sems.at[2])
    put.start()
    nsource = bound_ref.shape[0]
    per = got_ref.shape[1] // nsource
    chunks = per
    rows = nrow // nbin
    got = got_ref[1].reshape(nsource, per, LANES)
    used = got > 0.0
    lane = lax.broadcasted_iota(jnp.int32, (nsource, LANES), 1)
    ends = jnp.zeros((nsource, LANES), jnp.float32)
    for b in range(nbin):
        inside = jnp.where(used & (got <= float((b + 1) * BIN_CELLS)), 1.0, 0.0)
        total = jnp.sum(jnp.sum(inside, axis=1), axis=1, keepdims=True)
        ends = jnp.where(lane == b + 1, total, ends)
    ends_ref[...] = ends.astype(jnp.int32)
    copy = pltpu.make_async_copy(ends_ref, bound_ref, sems.at[0])
    copy.start()
    copy.wait()
    fetch.wait()
    zero, unit = jnp.zeros((), jnp.bfloat16), jnp.ones((), jnp.bfloat16)
    row_level, col_level = levels(2 * rows), levels(BIN)

    def quarter(b, carry):
        def span(source):
            at = jnp.minimum(source, nsource - 1)
            first = jnp.minimum(jnp.right_shift(bound_ref[at, b], 7), chunks - 1)
            last = jnp.right_shift(bound_ref[at, b + 1] + LANES - 1, 7)
            return first, jnp.maximum(last, first + 1)

        acc_ref[...] = jnp.zeros_like(acc_ref)

        def work(state):
            source, chunk, last = state
            highs, lows, cols = [], [], []
            for _ in range(GROUP):
                at = jnp.minimum(source, nsource - 1)
                half = jnp.bitwise_and(chunk, 1)
                row = at * per + half * (per // 2) + jnp.right_shift(chunk, 1)
                value = got_ref[0, pl.ds(row, 1)]
                cell = got_ref[1, pl.ds(row, 1)].astype(jnp.int32) - 1
                fits = (jnp.right_shift(cell, BIN_SHIFT) == b) & (source < nsource)
                half = jnp.bitwise_and(jnp.right_shift(cell, 8), 1)
                place = half * rows + jnp.bitwise_and(jnp.right_shift(cell, 9), rows - 1)
                place = jnp.where(fits, place, 2 * rows).astype(jnp.float32).astype(jnp.bfloat16)
                col = jnp.bitwise_and(cell, BIN - 1).astype(jnp.float32).astype(jnp.bfloat16)
                first = value.astype(jnp.bfloat16)
                second = (value - first.astype(jnp.float32)).astype(jnp.bfloat16)
                same = row_level == place
                highs.append(jnp.where(same, first, zero))
                lows.append(jnp.where(same, second, zero))
                cols.append(jnp.where(col_level == col, unit, zero))
                over = chunk + 1 >= last
                source = jnp.where(over, source + 1, source)
                following = span(source)
                chunk = jnp.where(over, following[0], chunk + 1)
                last = jnp.where(over, following[1], last)
            left = jnp.concatenate(
                [jnp.concatenate(highs, axis=1), jnp.concatenate(lows, axis=1)], axis=0
            )
            both = lax.dot_general(
                left, jnp.concatenate(cols, axis=1), (((1,), (1,)), ((), ())),
                preferred_element_type=jnp.float32,
            )
            acc_ref[...] += both[: 2 * rows] + both[2 * rows :]
            return source, chunk, last

        lax.while_loop(lambda state: state[0] < nsource, work, (jnp.int32(0), *span(0)))
        here = pl.ds(pl.multiple_of(b * rows, rows), rows)
        for half in range(2):
            cols = slice(half * BIN, (half + 1) * BIN)
            out_ref[here, cols] = rhs_ref[here, cols] + acc_ref[half * rows : (half + 1) * rows]
        return carry

    lax.fori_loop(0, nbin, quarter, 0)
    put.wait()


def scatter(rhs, got, force, nsource, nbin):
    nx, ny, nz = rhs.shape
    nrow = nx * ny
    vmem = pl.BlockSpec(memory_space=pltpu.VMEM)
    hbm = pl.BlockSpec(memory_space=pltpu.HBM)
    out, force = pl.pallas_call(
        functools.partial(scatter_kernel, nbin),
        in_specs=[hbm, vmem, vmem],
        out_specs=[vmem, hbm],
        out_shape=[
            jax.ShapeDtypeStruct((nrow, nz), jnp.float32),
            jax.ShapeDtypeStruct(force.shape, jnp.float32),
        ],
        scratch_shapes=[
            pltpu.VMEM((nrow, nz), jnp.float32),
            pltpu.VMEM((2 * nrow // nbin, BIN), jnp.float32),
            pltpu.VMEM((nsource, LANES), jnp.int32),
            pltpu.SMEM((nsource, LANES), jnp.int32),
            pltpu.SemaphoreType.DMA((3,)),
        ],
        compiler_params=pltpu.CompilerParams(vmem_limit_bytes=24 * 2**20),
        cost_estimate=pl.CostEstimate(
            flops=4 * nrow * nz * got.size // 2, bytes_accessed=4000000, transcendentals=0
        ),
    )(in_hbm(rhs.reshape(nrow, nz)), got, force)
    return out.reshape(nx, ny, nz), force


def body(
    pressure_rhs,
    shift_diag,
    positions,
    normals,
    tension,
    edge_weight,
    owner_map,
    cell_map,
    connectivity,
):
    ndevice = lax.axis_size(AXES)
    nbin = pressure_rhs.size // BIN_CELLS
    surface_force, got, inverse, cinverse = front(
        positions, normals, tension, edge_weight, connectivity, owner_map[:, 0], cell_map,
        shift_diag, ndevice, nbin,
    )
    forcing, surface_force = scatter(pressure_rhs, got, surface_force, ndevice, nbin)
    pressure = cycle(forcing, shift_diag, inverse, cinverse)
    return (pressure, surface_force)


def solution(mesh):
    return jax.shard_map(
        body,
        mesh=mesh,
        in_specs=(
            P("gx", "gy", "gz"),
            P("gx", "gy", "gz"),
            P(None, ("gx", "gy", "gz")),
            P(None, ("gx", "gy", "gz")),
            P(("gx", "gy", "gz")),
            P(None, ("gx", "gy", "gz")),
            P(("gx", "gy", "gz"), None),
            P(("gx", "gy", "gz")),
            P(None, ("gx", "gy", "gz")),
        ),
        out_specs=(P("gx", "gy", "gz"), P(None, ("gx", "gy", "gz"))),
        check_vma=False,
    )
```

```python
import functools

import jax
import jax.numpy as jnp
from jax import lax
from jax.experimental import pallas as pl
from jax.experimental.pallas import tpu as pltpu
from jax.sharding import PartitionSpec as P

HALO = 64
SMOOTH = 3
COARSE_SMOOTH = 4
LANES = 2 * HALO


centre = 1.125
spread = 0.875


def factors(sweeps):
    ratio = centre / spread
    fac = 1.0 / ratio
    pairs = [(0.0, 1.0 / centre)]
    for _ in range(1, sweeps):
        fac_new = 1.0 / (2.0 * ratio - fac)
        pairs.append((fac_new * fac, 2.0 * fac_new / spread))
        fac = fac_new
    return pairs


def split3(x):
    a = x.astype(jnp.bfloat16)
    rest = x - a.astype(jnp.float32)
    b = rest.astype(jnp.bfloat16)
    c = (rest - b.astype(jnp.float32)).astype(jnp.bfloat16)
    return a, b, c


MESH = pl.DeviceIdType.MESH
FINE = SMOOTH
COARSE = COARSE_SMOOTH - 1 + (SMOOTH + 1) // 2


UNROLL = 4
VMEM_LIMIT = 36 * 2**20


def around(src, x, r):
    ny, nz = src.shape[1:]
    sub = lax.broadcasted_iota(jnp.int32, (8, nz), 0)
    here = slice(r, r + 8)
    below, above = (r - 8) % ny, (r + 8) % ny
    cells = src[x, here]
    total = src[x - 1, here] + src[x + 1, here]
    total = total + (
        pltpu.roll(jnp.where(sub == 7, src[x, below : below + 8], cells), 1, 0)
        + pltpu.roll(jnp.where(sub == 0, src[x, above : above + 8], cells), 7, 0)
    )
    return cells, total + (pltpu.roll(cells, 1, 1) + pltpu.roll(cells, nz - 1, 1))


def sweep(rhs, inverse, src, dst, update, first, last, pair, keep=None):
    old, new = pair
    rows = src.shape[1] if keep is None else keep.shape[1]

    def slab(x, carry):
        for r in range(0, rows, 8):
            here = slice(r, r + 8)
            cells, total = around(src, x, r)
            change = new * (inverse[x, here] * (rhs[x, here] + total) - cells)
            if old:
                change = change + old * update[x, here]
            if keep is None:
                update[x, here] = change
                dst[x, here] = cells + change
            else:
                keep[x - first, here] = (cells + change)[:, : keep.shape[2]]
        return carry

    lax.fori_loop(first, last, slab, 0, unroll=UNROLL)


def begin(rhs, inverse, dst, update, slabs):
    def slab(x, carry):
        change = inverse[x] * rhs[x] * (1.0 / centre)
        update[x] = change
        dst[x] = change
        return carry

    lax.fori_loop(0, slabs, slab, 0, unroll=2)


def near(axes):
    ok = None
    where = {}
    for axis, step in axes:
        place = lax.axis_index(axis) + step
        fits = (place >= 0) & (place < lax.axis_size(axis))
        ok = fits if ok is None else ok & fits
        where[axis] = place
    return ok, where


SIDES = (-1, 1)
LINKS = (
    [(("gy", a),) for a in SIDES]
    + [(("gz", b),) for b in SIDES]
    + [(("gy", a), ("gz", b)) for b in SIDES for a in SIDES]
    + [(("gx", a),) for a in SIDES]
)
MIRROR = [1, 0, 3, 2, 7, 6, 5, 4, 9, 8]


def greet(links):
    barrier = pltpu.get_barrier_semaphore()
    peers = 0
    for link in links:
        ok, where = near(link)
        peers = peers + ok.astype(jnp.int32)

        @pl.when(ok)
        def _():
            pl.semaphore_signal(barrier, inc=1, device_id=where, device_id_type=MESH)

    pl.semaphore_wait(barrier, peers)


class Field:
    def __init__(self, ext, depth, wide, send, recv, send_sem, recv_sem, land=None):
        self.ext, self.depth, self.wide = ext, depth, wide
        self.send, self.recv = send, recv
        self.send_sem, self.recv_sem = send_sem, recv_sem
        self.land = land
        self.nx = ext.shape[0] - 2 * depth
        self.ny = ext.shape[1] - 2 * wide
        self.nz = ext.shape[2] - 128

    def message(self, m):
        d, nx, ny, nz, h = self.depth, self.nx, self.ny, self.nz, self.wide
        ext = self.ext
        if m < 2:
            if h == 8:
                rows = (0, ny - h)[m]
                src = ext.at[pl.ds(d, nx), pl.ds(rows, h), pl.ds(0, nz)]
                place = (ny + h, ny)[m]
                got = ext.at[pl.ds(d, nx), pl.ds(place, h), pl.ds(0, nz)]
                other = ext.at[pl.ds(d, nx), pl.ds((ny, ny + h)[m], h), pl.ds(0, nz)]
            else:
                src = self.send[0].at[m]
                got = self.recv[0].at[m]
                other = self.recv[0].at[1 - m]
        elif m < 4:
            src = self.send[1].at[m - 2]
            got = self.recv[1].at[m - 2]
            other = self.recv[1].at[3 - m]
        elif m < 8:
            b, a = divmod(m - 4, 2)
            src = self.send[1].at[b, pl.ds((0, ny - 8)[a], 8)]
            got = self.recv[2].at[b, a]
            other = self.recv[2].at[1 - b, 1 - a]
        else:
            a = m - 8
            src = ext.at[pl.ds((d, nx)[a], d)]
            if self.land is None:
                got = ext.at[pl.ds((0, d + nx)[a], d)]
                other = ext.at[pl.ds((d + nx, 0)[a], d)]
            else:
                got = self.land.at[a]
                other = self.land.at[1 - a]
        return src, other, got

    def copy(self, m, incoming):
        src, other, got = self.message(m)
        k = m if incoming else MIRROR[m]
        return pltpu.make_async_remote_copy(
            src_ref=got if incoming else src,
            dst_ref=got if incoming else other,
            send_sem=self.send_sem.at[m],
            recv_sem=self.recv_sem.at[k],
            device_id=near(LINKS[m])[1],
            device_id_type=MESH,
        )

    def start(self, which):
        for m in which:
            @pl.when(near(LINKS[m])[0])
            def _():
                self.copy(m, False).start()

    def finish(self, which):
        for m in which:
            ok = near(LINKS[m])[0]

            @pl.when(ok)
            def _():
                self.copy(m, False).wait_send()
                self.copy(m, True).wait_recv()

            @pl.when(jnp.logical_not(ok))
            def _():
                got = self.message(m)[2]
                got[...] = jnp.zeros(got.shape, jnp.float32)

    def pack(self):
        d, nx, ny, nz, h = self.depth, self.nx, self.ny, self.nz, self.wide
        ext = self.ext
        if h != 8:
            for x in range(nx):
                at = slice(d * (x % 8), d * (x % 8) + d)
                self.send[0][0, x // 8, at] = ext[d + x, :d, :nz]
                self.send[0][1, x // 8, at] = ext[d + x, ny - d : ny, :nz]
        group = lax.broadcasted_iota(jnp.int32, (ny, 128), 1) // (2 * h)

        def slab(x, carry):
            low, high = carry
            mine = group == x
            shift = 2 * h * x + h
            low = jnp.where(mine, pltpu.roll(ext[d + x, :ny, :128], shift, 1), low)
            high = jnp.where(mine, pltpu.roll(ext[d + x, :ny, nz - 128 : nz], shift, 1), high)
            return low, high

        zero = jnp.zeros((ny, 128), jnp.float32)
        low, high = lax.fori_loop(0, nx, slab, (zero, zero), unroll=8)
        self.send[1][0] = low
        self.send[1][1] = high

    def unpack(self):
        d, nx, ny, nz, h = self.depth, self.nx, self.ny, self.nz, self.wide
        ext = self.ext
        if h != 8:
            for x in range(nx):
                at = slice(d * (x % 8), d * (x % 8) + d)
                ext[d + x, ny : ny + d, :nz] = self.recv[0][1, x // 8, at]
                ext[d + x, ny + 8 - d : ny + 8, :nz] = self.recv[0][0, x // 8, at]
        ends = []
        for b in range(2):
            corner = (self.recv[2][b, 1], self.recv[2][b, 0])
            if h == 8:
                ends.append(jnp.concatenate([self.recv[1][b], *corner], axis=0))
            else:
                sub = lax.broadcasted_iota(jnp.int32, (8, 128), 0)
                ends.append(
                    jnp.concatenate([self.recv[1][b], jnp.where(sub < h, *corner)], axis=0)
                )
        lane = lax.broadcasted_iota(jnp.int32, ends[0].shape, 1)
        both = jnp.where(lane % (2 * h) < h, ends[0], ends[1])
        edge = (lane < h) | (lane >= 128 - h)

        def slab(x, carry):
            moved = pltpu.roll(both, 128 - h - 2 * h * x, 1)
            ext[d + x, :, nz : nz + 128] = jnp.where(edge, moved, 0.0)
            return carry

        lax.fori_loop(0, nx, slab, 0, unroll=8)


def pair_up(src, pairs):
    def add(j, carry):
        pairs[j] = src[2 * j] + src[2 * j + 1]
        return carry

    lax.fori_loop(0, pairs.shape[0], add, 0)


def pooled(pairs, into, after):
    cx, ny, nz = pairs.shape
    depth = COARSE
    flat = pairs[...].reshape(cx * ny, nz)

    def halves(rows, cols, dim):
        r = lax.broadcasted_iota(jnp.int32, (rows, cols), dim)
        c = lax.broadcasted_iota(jnp.int32, (rows, cols), 1 - dim)
        return (r == jnp.right_shift(c, 1)).astype(jnp.float32).astype(jnp.bfloat16)

    along_z = halves(nz, nz // 2, 1)
    along_y = halves(cx * ny // 2, cx * ny, 0)
    flat = sum(jnp.dot(p, along_z, preferred_element_type=jnp.float32) for p in split3(flat)[:2])
    flat = sum(jnp.dot(along_y, p, preferred_element_type=jnp.float32) for p in split3(flat)[:2])
    out = after(0.5 * flat).reshape(cx, ny // 2, nz // 2)
    into[depth : depth + cx, : ny // 2, : nz // 2] = out


def fine_field(ext, bufs, sems, landing=None):
    ysend, yrecv, zsend, zrecv, yzrecv = bufs
    return Field(ext, FINE, 4, (ysend, zsend), (yrecv, zrecv, yzrecv), *sems, landing)


def coarse_field(ext, bufs, sems):
    zsend, zrecv, yzrecv = bufs
    return Field(ext, COARSE, 8, (None, zsend), (None, zrecv, yzrecv), *sems)


def buf(*shape):
    return pltpu.VMEM(shape, jnp.float32)


def wide_shapes(nx, ny, nz):
    cx, cy, cz = nx // 2, ny // 2, nz // 2
    return (
        (nx + 2 * FINE, ny + 8, nz + 128),
        (cx + 2 * COARSE, cy + 16, cz + 128),
    )


def fine_scratch(nx, ny, nz):
    rows = (2, nx // 8, 8 * FINE, nz)
    return [buf(*rows)] * 2 + [buf(2, ny, 128)] * 2 + [buf(2, 2, 8, 128)]


def coarse_scratch(nx, ny, nz):
    return [buf(2, ny // 2, 128)] * 2 + [buf(2, 2, 8, 128)]


FIRST, LAST = range(8), (8, 9)


def cycle_kernel(forcing, shift_hbm, inverse, cinverse, pressure, *scratch):
    shift, load_sem, scratch = scratch[0], scratch[-1], scratch[1:-1]
    fetch = pltpu.make_async_copy(shift_hbm, shift, load_sem)
    fetch.start()
    (rhs, one, two, update, land, crhs, cone, ctwo, cupdate, pairs), scratch = (
        scratch[:10], scratch[10:],
    )
    bufs_a, bufs_b, bufs_c = scratch[:5], scratch[5:10], scratch[10:13]
    send_sem, recv_sem = scratch[13:]
    nx, ny, nz = forcing.shape
    sems = [(send_sem.at[k], recv_sem.at[k]) for k in range(3)]

    def load(x, carry):
        rhs[FINE + x, :ny, :nz] = forcing[x]
        return carry

    lax.fori_loop(0, nx, load, 0, unroll=2)
    field = fine_field(rhs, bufs_a, sems[0])
    field.pack()
    greet(LINKS)
    field.start(FIRST)
    field.finish(FIRST)
    field.unpack()
    field.start(LAST)
    field.finish(LAST)

    slabs = nx + 2 * FINE
    pairs_of = factors(SMOOTH)
    bufs = (one, two)
    begin(rhs, inverse, one, update, slabs)
    for k in range(1, SMOOTH):
        sweep(rhs, inverse, bufs[(k - 1) % 2], bufs[k % 2], update, k, slabs - k, pairs_of[k])
    smooth = bufs[(SMOOTH - 1) % 2]
    other = bufs[SMOOTH % 2]

    fetch.wait()

    def residual(j, carry):
        for r in range(0, ny, 8):
            here = slice(r, r + 8)
            both = 0.0
            for half in range(2):
                x = 2 * j + half
                cells, total = around(smooth, FINE + x, r)
                total = total[:, :nz] + rhs[FINE + x, here, :nz]
                both = both + (total - (6.0 + shift[x, here]) * cells[:, :nz])
            pairs[j, here] = both
        return carry

    lax.fori_loop(0, nx // 2, residual, 0, unroll=2)
    pooled(pairs, crhs, lambda total: total)
    coarse = coarse_field(crhs, bufs_c, sems[2])
    coarse.pack()
    coarse.start(FIRST)
    field = fine_field(smooth, bufs_b, sems[1], land)
    field.pack()
    field.start(FIRST)
    cslabs = crhs.shape[0]
    low = COARSE - (FINE + 1) // 2
    count = cslabs - 2 * low
    cny, cnz = crhs.shape[1:]
    fny, fnz = smooth.shape[1:]

    def fan(shape, fine_dim, per_f, per_c, core, jump):
        f = lax.broadcasted_iota(jnp.int32, shape, fine_dim)
        c = lax.broadcasted_iota(jnp.int32, shape, 1 - fine_dim)
        block = 0
        for g in range(1, shape[fine_dim] // per_f):
            block = block + (f >= g * per_f).astype(jnp.int32)
        inner = f - block * per_f
        target = jnp.right_shift(inner, 1) + jnp.where(inner >= core, jump, 0) + block * per_c
        return (c == target).astype(jnp.float32).astype(jnp.bfloat16)

    fan_y = fan((count * fny, count * cny), 0, fny, cny, ny + 4, cny - fny // 2)
    fan_z = fan((cnz, fnz), 1, fnz, cnz, nz + 64, cnz - fnz // 2)
    coarse.finish(FIRST)
    coarse.unpack()
    coarse.start(LAST)
    coarse.finish(LAST)

    pairs_of = factors(COARSE_SMOOTH)
    cbufs = (cone, ctwo)
    begin(crhs, cinverse, cone, cupdate, cslabs)
    for k in range(1, COARSE_SMOOTH):
        sweep(
            crhs, cinverse, cbufs[(k - 1) % 2], cbufs[k % 2], cupdate, k, cslabs - k, pairs_of[k]
        )
    field.finish(FIRST)
    field.unpack()
    field.start(LAST)
    fix = cbufs[(COARSE_SMOOTH - 1) % 2]

    flat = fix[low : low + count].reshape(count * cny, cnz)

    tall = sum(jnp.dot(fan_y, p, preferred_element_type=jnp.float32) for p in split3(flat)[:2])
    full = sum(jnp.dot(p, fan_z, preferred_element_type=jnp.float32) for p in split3(tall)[:2])
    field.finish(LAST)
    for j in range(count):
        part = full[j * fny : (j + 1) * fny]
        for half in range(2):
            x = FINE + 2 * (low + j - COARSE) + half
            if 0 <= x < FINE:
                smooth[x] = land[0, x] + part
            elif FINE <= x < FINE + nx:
                smooth[x] = smooth[x] + part
            elif FINE + nx <= x < slabs:
                smooth[x] = land[1, x - FINE - nx] + part

    pairs_of = factors(SMOOTH)
    bufs = (smooth, other)

    for k in range(SMOOTH):
        sweep(
            rhs, inverse, bufs[k % 2], bufs[(k + 1) % 2], update,
            k + 1, slabs - k - 1, pairs_of[k], pressure if k == SMOOTH - 1 else None,
        )


def cycle(forcing, shift, inverse, cinverse):
    nx, ny, nz = forcing.shape
    wide, cwide = (buf(*shape) for shape in wide_shapes(nx, ny, nz))
    vmem = pl.BlockSpec(memory_space=pltpu.VMEM)
    return pl.pallas_call(
        cycle_kernel,
        in_specs=[vmem, pl.BlockSpec(memory_space=pltpu.HBM), vmem, vmem],
        out_specs=vmem,
        out_shape=jax.ShapeDtypeStruct(forcing.shape, jnp.float32),
        scratch_shapes=[buf(nx, ny, nz)]
        + [wide] * 4
        + [buf(2, FINE, ny + 8, nz + 128)]
        + [cwide] * 4
        + [buf(nx // 2, ny, nz)]
        + fine_scratch(nx, ny, nz) * 2
        + coarse_scratch(nx, ny, nz)
        + [pltpu.SemaphoreType.DMA((3, 10))] * 2
        + [pltpu.SemaphoreType.DMA],
        compiler_params=pltpu.CompilerParams(
            collective_id=1, has_side_effects=True, vmem_limit_bytes=VMEM_LIMIT
        ),
    )(forcing, in_hbm(shift), inverse, cinverse)


BIN = 256
BIN_SHIFT = 15
BIN_CELLS = 1 << BIN_SHIFT
AXES = ("gx", "gy", "gz")


def in_hbm(x):
    return pltpu.with_memory_space_constraint(x, pltpu.HBM)


def levels(rows):
    level = lax.broadcasted_iota(jnp.int32, (rows, LANES), 0)
    if rows > BIN:
        return level
    return level.astype(jnp.float32).astype(jnp.bfloat16)


def hot_rows(level, index, values=None):
    if level.dtype != jnp.int32:
        index = index.astype(jnp.float32).astype(jnp.bfloat16)
    columns = []
    for at in range(0, index.shape[1], LANES):
        here = slice(at, at + LANES)
        value = jnp.ones((), jnp.bfloat16) if values is None else values[:, here]
        same = level == index[:, here]
        columns.append(jnp.where(same, value, jnp.zeros((), jnp.bfloat16)))
    return jnp.concatenate(columns, axis=1)


def place_of(index):
    where = {}
    for axis in reversed(AXES):
        count = lax.axis_size(axis)
        where[axis] = lax.rem(index, count)
        index = lax.div(index, count)
    return where


def front_kernel(
    ndevice, nbin, *refs
):
    sources, refs = refs[:8], refs[8:]
    (force_ref, got_ref, inverse, cinverse), refs = refs[:4], refs[4:]
    (pos_ref, nrm_ref, ten_ref, wgt_ref, con_ref, own_ref, cel_ref, shift), scratch = (
        refs[:8], refs[8:],
    )
    load_sem, scratch = scratch[-1], scratch[:-1]

    def fetch(k):
        return pltpu.make_async_copy(sources[k], refs[k], load_sem.at[k])

    for k in (7, 0, 5, 6, 4, 3, 2, 1):
        fetch(k).start()
    (packed_ref, total_ref, carry_ref, rank_ref, jump_ref, pad_ref, psend, precv, pairs), scratch = (
        scratch[:9], scratch[9:],
    )
    fine_bufs, coarse_bufs = scratch[:5], scratch[5:8]
    send_sem, recv_sem, all_send, all_recv, pos_send, pos_recv = scratch[8:]
    chunk = 4 * LANES
    split = 4
    per = 2 * split
    npoint = ten_ref.shape[1]
    nx, ny, nz = shift.shape
    class_level, slot_level = levels(nbin * ndevice), levels(BIN)
    row_level = levels(total_ref.shape[0])
    me = lax.axis_index(AXES)
    barrier = pltpu.get_barrier_semaphore()

    def other(p):
        return lax.rem(me + p, ndevice)

    def hello(p, carry):
        pl.semaphore_signal(barrier, inc=1, device_id=place_of(other(p)), device_id_type=MESH)
        return carry

    lax.fori_loop(1, ndevice, hello, 0)

    fetch(0).wait()
    psend[0, :3] = pos_ref[:, npoint - LANES :]
    psend[1, :3] = pos_ref[:, :LANES]

    def spread_out(j, carry):
        lower = pos_ref[:, pl.ds(pl.multiple_of(j * LANES - LANES, LANES), LANES)]
        upper = pos_ref[:, pl.ds(pl.multiple_of(j * LANES, LANES), LANES)]
        both = jnp.concatenate([lower[:, HALO:], upper[:, :HALO]], axis=1)
        pad_ref[:3, pl.ds(pl.multiple_of(j * LANES, LANES), LANES)] = both
        return carry

    lax.fori_loop(1, npoint // LANES, spread_out, 0, unroll=7)

    def edge(side, incoming):
        return pltpu.make_async_remote_copy(
            src_ref=psend.at[side],
            dst_ref=precv.at[side],
            send_sem=pos_send.at[side],
            recv_sem=pos_recv.at[side],
            device_id=place_of(other((1, ndevice - 1)[side])),
            device_id_type=MESH,
        )

    def classes(here):
        return own_ref[:, here] + ndevice * jnp.right_shift(cel_ref[:, here], BIN_SHIFT)

    def count(i, total):
        here = pl.ds(pl.multiple_of(i * chunk, chunk), chunk)
        hot = hot_rows(class_level, classes(here)).astype(jnp.float32)
        return total + (
            hot[:, :LANES] + hot[:, LANES : 2 * LANES]
            + (hot[:, 2 * LANES : 3 * LANES] + hot[:, 3 * LANES :])
        )

    for k in (5, 6):
        fetch(k).wait()
    counts = lax.fori_loop(
        0, npoint // chunk, count, jnp.zeros((nbin * ndevice, LANES), jnp.float32), unroll=2
    )
    counts = jnp.sum(counts, axis=1, keepdims=True)
    base = jnp.zeros((ndevice, 1), jnp.float32)
    for b in range(nbin):
        carry_ref[b * ndevice : (b + 1) * ndevice] = base
        base = base + counts[b * ndevice : (b + 1) * ndevice]
    before = (
        lax.broadcasted_iota(jnp.int32, (chunk, chunk), 0)
        < lax.broadcasted_iota(jnp.int32, (chunk, chunk), 1)
    ).astype(jnp.float32).astype(jnp.bfloat16)

    def order(i, carry):
        here = pl.ds(pl.multiple_of(i * chunk, chunk), chunk)
        ones = hot_rows(class_level, classes(here))
        earlier = jnp.dot(ones, before, preferred_element_type=jnp.float32)
        wide = ones.astype(jnp.float32)
        rank = jnp.sum(wide * (earlier + carry), axis=0, keepdims=True)
        rank_ref[:, here] = rank.astype(jnp.int32)
        return carry + (earlier[:, chunk - 1 :] + wide[:, chunk - 1 :])

    lax.fori_loop(0, npoint // chunk, order, carry_ref[...], unroll=4)

    fetch(7).wait()

    def load(x, carry):
        inverse[FINE + x, :ny, :nz] = 1.0 / (6.0 + shift[x])
        return carry

    lax.fori_loop(0, nx, load, 0, unroll=2)
    pair_up(shift, pairs)
    pooled(pairs, cinverse, lambda total: 1.0 / (6.0 + total))
    fine = fine_field(inverse, fine_bufs, (send_sem.at[0], recv_sem.at[0]))
    coarse = coarse_field(cinverse, coarse_bufs, (send_sem.at[1], recv_sem.at[1]))
    fine.pack()
    coarse.pack()
    pl.semaphore_wait(barrier, ndevice - 1)

    for side in range(2):
        edge(side, False).start()
    fine.start(FIRST)
    coarse.start(FIRST)

    def rows_of(device):
        return pl.ds(pl.multiple_of(device * per, per), per)

    def deal(part, p, incoming):
        return pltpu.make_async_remote_copy(
            src_ref=packed_ref.at[part, rows_of(other(p))],
            dst_ref=got_ref.at[part, rows_of(other(ndevice - p) if incoming else me)],
            send_sem=all_send.at[part, p],
            recv_sem=all_recv.at[part, p],
            device_id=place_of(other(p)),
            device_id_type=MESH,
        )

    def send(part):
        def one(p, carry):
            deal(part, p, False).start()
            return carry

        lax.fori_loop(1, ndevice, one, 0)

    def pack(part, pieces):
        total_ref[...] = jnp.zeros_like(total_ref)

        big = npoint // 2

        def some(i, carry):
            here = pl.ds(pl.multiple_of(i * big, big), big)
            rank = rank_ref[:, here]
            slots = hot_rows(slot_level, jnp.bitwise_and(rank, BIN - 1))
            row = own_ref[:, here] * split + jnp.right_shift(rank, 8)
            left = [hot_rows(row_level, row, piece) for piece in pieces(here)]
            both = lax.dot_general(
                jnp.concatenate(left, axis=0), slots, (((1,), (1,)), ((), ())),
                preferred_element_type=jnp.float32,
            )
            count = total_ref.shape[0]
            total_ref[...] += sum(both[k * count : k * count + count] for k in range(len(left)))
            return carry

        lax.fori_loop(0, npoint // big, some, 0)
        sub = lax.broadcasted_iota(jnp.int32, (per, LANES), 0)
        for t in range(ndevice // 2):
            one = total_ref[t * per : t * per + per, :LANES]
            two = total_ref[t * per : t * per + per, LANES:]
            at = 2 * t * per
            packed_ref[part, at : at + per] = jnp.where(sub < split, one, pltpu.roll(two, split, 0))
            packed_ref[part, at + per : at + 2 * per] = jnp.where(
                sub < split, pltpu.roll(one, split, 0), two
            )

    def digits(here):
        cell = cel_ref[:, here] + 1
        for bits in (0, 8, 16):
            digit = jnp.left_shift(jnp.bitwise_and(jnp.right_shift(cell, bits), 255), bits)
            yield digit.astype(jnp.float32).astype(jnp.bfloat16)

    pack(1, digits)
    send(1)
    for k in (4, 3, 2, 1):
        fetch(k).wait()
    for side in range(2):
        edge(side, True).wait_send()
        edge(side, True).wait_recv()
    pad_ref[:3, :LANES] = jnp.concatenate(
        [precv[0, :3, HALO:], pos_ref[:, :HALO]], axis=1
    )
    pad_ref[:3, npoint:] = jnp.concatenate(
        [pos_ref[:, npoint - HALO :], precv[1, :3, :HALO]], axis=1
    )
    begin_at = me * npoint
    everything = npoint * ndevice

    def pull(i, carry):
        for sub in range(2):
            base = pl.multiple_of(i * 2 * LANES + sub * LANES, LANES)
            here = pl.ds(base, LANES)
            lower = pad_ref[:, here]
            upper = pad_ref[:, pl.ds(base + LANES, LANES)]
            centre_pos = jnp.concatenate([lower[:, HALO:], upper[:, :HALO]], axis=1)
            index = con_ref[:, here] - begin_at + HALO
            index = jnp.where(index < 0, index + everything, index)
            index = jnp.where(index >= everything, index - everything, index) - base
            total = jnp.zeros_like(lower)
            for which in range(con_ref.shape[0]):
                wide = jnp.broadcast_to(index[which : which + 1], lower.shape)
                low = jnp.bitwise_and(wide, LANES - 1)
                near_by = jnp.take_along_axis(lower, low, axis=1, mode="promise_in_bounds")
                far = jnp.take_along_axis(upper, low, axis=1, mode="promise_in_bounds")
                picked = jnp.where(wide < LANES, near_by, far)
                total = total + wgt_ref[which : which + 1, here] * (picked - centre_pos)
            force = ten_ref[:, here] * total[:3]
            force_ref[:, here] = force
            jump_ref[:, here] = jnp.sum(force * nrm_ref[:, here], axis=0, keepdims=True)
        return carry

    lax.fori_loop(0, npoint // (2 * LANES), pull, 0, unroll=4)

    pack(0, lambda here: split3(jump_ref[:, here])[:2])
    send(0)
    for part in range(2):
        got_ref[part, rows_of(me)] = packed_ref[part, rows_of(me)]
    fine.finish(FIRST)
    fine.unpack()
    fine.start(LAST)
    coarse.finish(FIRST)
    coarse.unpack()
    coarse.start(LAST)
    fine.finish(LAST)
    coarse.finish(LAST)

    def receive(p, carry):
        for part in range(2):
            deal(part, p, False).wait_send()
            deal(part, p, True).wait_recv()
        return carry

    lax.fori_loop(1, ndevice, receive, 0)


def front(
    positions, normals, tension, edge_weight, connectivity, owner_ids, cell_map, shift,
    ndevice, nbin,
):
    npoint = tension.shape[0]
    nx, ny, nz = shift.shape
    vmem = pl.BlockSpec(memory_space=pltpu.VMEM)
    wide, cwide = wide_shapes(nx, ny, nz)
    return pl.pallas_call(
        functools.partial(front_kernel, ndevice, nbin),
        in_specs=[pl.BlockSpec(memory_space=pltpu.HBM)] * 8,
        out_specs=[vmem] * 4,
        out_shape=[
            jax.ShapeDtypeStruct(shape, jnp.float32)
            for shape in ((3, npoint), (2, 8 * ndevice, LANES), wide, cwide)
        ],
        scratch_shapes=[
            buf(3, npoint),
            buf(3, npoint),
            buf(1, npoint),
            buf(*edge_weight.shape),
            pltpu.VMEM(connectivity.shape, jnp.int32),
            pltpu.VMEM((1, npoint), jnp.int32),
            pltpu.VMEM((1, npoint), jnp.int32),
            buf(nx, ny, nz),
            buf(2, 8 * ndevice, LANES),
            buf(4 * ndevice, BIN),
            buf(nbin * ndevice, 1),
            pltpu.VMEM((1, npoint), jnp.int32),
            buf(1, npoint),
            buf(8, npoint + LANES),
            buf(2, 8, LANES),
            buf(2, 8, LANES),
            buf(nx // 2, ny, nz),
        ]
        + fine_scratch(nx, ny, nz)
        + coarse_scratch(nx, ny, nz)
        + [pltpu.SemaphoreType.DMA((2, 10))] * 2
        + [pltpu.SemaphoreType.DMA((2, ndevice))] * 2
        + [pltpu.SemaphoreType.DMA((2,))] * 2
        + [pltpu.SemaphoreType.DMA((8,))],
        compiler_params=pltpu.CompilerParams(
            collective_id=0, has_side_effects=True, vmem_limit_bytes=20 * 2**20
        ),
    )(
        *map(
            in_hbm,
            (
                positions, normals, tension[None], edge_weight, connectivity, owner_ids[None],
                cell_map[None], shift,
            ),
        )
    )


GROUP = 72


def scatter_kernel(
    nbin, rhs_hbm, got_ref, force_ref, out_ref, force_hbm,
    rhs_ref, acc_ref, list_ref, chunk_ref, sems,
):
    nrow, nz = rhs_ref.shape
    fetch = pltpu.make_async_copy(rhs_hbm, rhs_ref, sems.at[1])
    fetch.start()
    put = pltpu.make_async_copy(force_ref, force_hbm, sems.at[2])
    put.start()
    per = 8
    nsource = got_ref.shape[1] // per
    rows = nrow // nbin
    got = got_ref[1].reshape(nsource, per, LANES)
    used = got > 0.0
    lane = lax.broadcasted_iota(jnp.int32, (nsource, LANES), 1)
    ends = jnp.zeros((nsource, LANES), jnp.float32)
    for b in range(nbin):
        inside = jnp.where(used & (got <= float((b + 1) * BIN_CELLS)), 1.0, 0.0)
        total = jnp.sum(jnp.sum(inside, axis=1), axis=1, keepdims=True)
        ends = jnp.where(lane == b + 1, total, ends)
    ends = ends.astype(jnp.int32)
    stops = pltpu.roll(ends, LANES - 1, 1)
    firsts = jnp.right_shift(ends, 7)
    counts = jnp.where(stops > ends, jnp.right_shift(stops + LANES - 1, 7) - firsts, 0)
    counts = jnp.where(lane < nbin, counts, 0).astype(jnp.float32)
    square = (nsource, nsource)
    before = (
        lax.broadcasted_iota(jnp.int32, square, 0) > lax.broadcasted_iota(jnp.int32, square, 1)
    ).astype(jnp.float32).astype(jnp.bfloat16)
    starts = jnp.dot(before, counts.astype(jnp.bfloat16), preferred_element_type=jnp.float32)
    sums = jnp.sum(counts, axis=0, keepdims=True)
    width = list_ref.shape[1]
    source = lax.broadcasted_iota(jnp.int32, (nsource, width), 0)
    position = lax.broadcasted_iota(jnp.int32, (nsource, width), 1)
    for b in range(nbin):
        pick = slice(b, b + 1)
        step = position - starts[:, pick].astype(jnp.int32)
        chunk = firsts[:, pick] + step
        row = source * per + jnp.bitwise_and(chunk, 1) * (per // 2) + jnp.right_shift(chunk, 1)
        inside = (step >= 0) & (step < counts[:, pick].astype(jnp.int32))
        row = jnp.sum(jnp.where(inside, row.astype(jnp.float32), 0.0), axis=0, keepdims=True)
        list_ref[b : b + 1] = row.astype(jnp.int32)
        list_ref[nbin + b : nbin + b + 1] = jnp.broadcast_to(sums[:, pick], (1, width)).astype(
            jnp.int32
        )
    copy = pltpu.make_async_copy(list_ref, chunk_ref, sems.at[0])
    copy.start()
    copy.wait()
    fetch.wait()
    zero, unit = jnp.zeros((), jnp.bfloat16), jnp.ones((), jnp.bfloat16)
    row_level, col_level = levels(2 * rows), levels(BIN)

    def quarter(b, carry):
        total = chunk_ref[nbin + b, 0]
        acc_ref[...] = jnp.zeros_like(acc_ref)

        def work(step, carry):
            highs, lows, cols = [], [], []
            for k in range(GROUP):
                at = step * GROUP + k
                row = chunk_ref[b, jnp.minimum(at, width - 1)]
                value = got_ref[0, pl.ds(row, 1)]
                cell = got_ref[1, pl.ds(row, 1)].astype(jnp.int32) - 1
                fits = (jnp.right_shift(cell, BIN_SHIFT) == b) & (at < total)
                half = jnp.bitwise_and(jnp.right_shift(cell, 8), 1)
                place = half * rows + jnp.bitwise_and(jnp.right_shift(cell, 9), rows - 1)
                place = jnp.where(fits, place, 2 * rows).astype(jnp.float32).astype(jnp.bfloat16)
                col = jnp.bitwise_and(cell, BIN - 1).astype(jnp.float32).astype(jnp.bfloat16)
                first = value.astype(jnp.bfloat16)
                second = (value - first.astype(jnp.float32)).astype(jnp.bfloat16)
                same = row_level == place
                highs.append(jnp.where(same, first, zero))
                lows.append(jnp.where(same, second, zero))
                cols.append(jnp.where(col_level == col, unit, zero))
            left = jnp.concatenate(
                [jnp.concatenate(highs, axis=1), jnp.concatenate(lows, axis=1)], axis=0
            )
            both = lax.dot_general(
                left, jnp.concatenate(cols, axis=1), (((1,), (1,)), ((), ())),
                preferred_element_type=jnp.float32,
            )
            acc_ref[...] += both[: 2 * rows] + both[2 * rows :]
            return carry

        lax.fori_loop(0, lax.div(total + GROUP - 1, GROUP), work, 0)
        here = pl.ds(pl.multiple_of(b * rows, rows), rows)
        for half in range(2):
            cols = slice(half * BIN, (half + 1) * BIN)
            out_ref[here, cols] = rhs_ref[here, cols] + acc_ref[half * rows : (half + 1) * rows]
        return carry

    lax.fori_loop(0, nbin, quarter, 0)
    put.wait()


def scatter(rhs, got, force, nsource, nbin):
    nx, ny, nz = rhs.shape
    nrow = nx * ny
    vmem = pl.BlockSpec(memory_space=pltpu.VMEM)
    hbm = pl.BlockSpec(memory_space=pltpu.HBM)
    out, force = pl.pallas_call(
        functools.partial(scatter_kernel, nbin),
        in_specs=[hbm, vmem, vmem],
        out_specs=[vmem, hbm],
        out_shape=[
            jax.ShapeDtypeStruct((nrow, nz), jnp.float32),
            jax.ShapeDtypeStruct(force.shape, jnp.float32),
        ],
        scratch_shapes=[
            pltpu.VMEM((nrow, nz), jnp.float32),
            pltpu.VMEM((2 * nrow // nbin, BIN), jnp.float32),
            pltpu.VMEM((2 * nbin, 8 * nsource), jnp.int32),
            pltpu.SMEM((2 * nbin, 8 * nsource), jnp.int32),
            pltpu.SemaphoreType.DMA((3,)),
        ],
        compiler_params=pltpu.CompilerParams(vmem_limit_bytes=24 * 2**20),
        cost_estimate=pl.CostEstimate(
            flops=4 * nrow * nz * got.size // 2, bytes_accessed=4000000, transcendentals=0
        ),
    )(in_hbm(rhs.reshape(nrow, nz)), got, force)
    return out.reshape(nx, ny, nz), force


def body(
    pressure_rhs,
    shift_diag,
    positions,
    normals,
    tension,
    edge_weight,
    owner_map,
    cell_map,
    connectivity,
):
    ndevice = lax.axis_size(AXES)
    nbin = pressure_rhs.size // BIN_CELLS
    surface_force, got, inverse, cinverse = front(
        positions, normals, tension, edge_weight, connectivity, owner_map[:, 0], cell_map,
        shift_diag, ndevice, nbin,
    )
    forcing, surface_force = scatter(pressure_rhs, got, surface_force, ndevice, nbin)
    pressure = cycle(forcing, shift_diag, inverse, cinverse)
    return (pressure, surface_force)


def solution(mesh):
    return jax.shard_map(
        body,
        mesh=mesh,
        in_specs=(
            P("gx", "gy", "gz"),
            P("gx", "gy", "gz"),
            P(None, ("gx", "gy", "gz")),
            P(None, ("gx", "gy", "gz")),
            P(("gx", "gy", "gz")),
            P(None, ("gx", "gy", "gz")),
            P(("gx", "gy", "gz"), None),
            P(("gx", "gy", "gz")),
            P(None, ("gx", "gy", "gz")),
        ),
        out_specs=(P("gx", "gy", "gz"), P(None, ("gx", "gy", "gz"))),
        check_vma=False,
    )
```

```python
import functools

import jax
import jax.numpy as jnp
from jax import lax
from jax.experimental import pallas as pl
from jax.experimental.pallas import tpu as pltpu
from jax.sharding import PartitionSpec as P

HALO = 64
SMOOTH = 3
COARSE_SMOOTH = 4
LANES = 2 * HALO


centre = 1.125
spread = 0.875


def factors(sweeps):
    ratio = centre / spread
    fac = 1.0 / ratio
    pairs = [(0.0, 1.0 / centre)]
    for _ in range(1, sweeps):
        fac_new = 1.0 / (2.0 * ratio - fac)
        pairs.append((fac_new * fac, 2.0 * fac_new / spread))
        fac = fac_new
    return pairs


def split3(x):
    a = x.astype(jnp.bfloat16)
    rest = x - a.astype(jnp.float32)
    b = rest.astype(jnp.bfloat16)
    c = (rest - b.astype(jnp.float32)).astype(jnp.bfloat16)
    return a, b, c


MESH = pl.DeviceIdType.MESH
FINE = SMOOTH
COARSE = COARSE_SMOOTH - 1 + (SMOOTH + 1) // 2


UNROLL = 4
VMEM_LIMIT = 36 * 2**20


def around(src, x, r):
    ny, nz = src.shape[1:]
    sub = lax.broadcasted_iota(jnp.int32, (8, nz), 0)
    here = slice(r, r + 8)
    below, above = (r - 8) % ny, (r + 8) % ny
    cells = src[x, here]
    total = src[x - 1, here] + src[x + 1, here]
    total = total + (
        pltpu.roll(jnp.where(sub == 7, src[x, below : below + 8], cells), 1, 0)
        + pltpu.roll(jnp.where(sub == 0, src[x, above : above + 8], cells), 7, 0)
    )
    return cells, total + (pltpu.roll(cells, 1, 1) + pltpu.roll(cells, nz - 1, 1))


def sweep(rhs, inverse, src, dst, update, first, last, pair, keep=None):
    old, new = pair
    rows = src.shape[1] if keep is None else keep.shape[1]

    def slab(x, carry):
        for r in range(0, rows, 8):
            here = slice(r, r + 8)
            cells, total = around(src, x, r)
            change = new * (inverse[x, here] * (rhs[x, here] + total) - cells)
            if old:
                change = change + old * update[x, here]
            if keep is None:
                update[x, here] = change
                dst[x, here] = cells + change
            else:
                keep[x - first, here] = (cells + change)[:, : keep.shape[2]]
        return carry

    lax.fori_loop(first, last, slab, 0, unroll=UNROLL)


def begin(rhs, inverse, dst, update, first, last):
    def slab(x, carry):
        change = inverse[x] * rhs[x] * (1.0 / centre)
        update[x] = change
        dst[x] = change
        return carry

    lax.fori_loop(first, last, slab, 0, unroll=2)


def near(axes):
    ok = None
    where = {}
    for axis, step in axes:
        place = lax.axis_index(axis) + step
        fits = (place >= 0) & (place < lax.axis_size(axis))
        ok = fits if ok is None else ok & fits
        where[axis] = place
    return ok, where


SIDES = (-1, 1)
LINKS = (
    [(("gy", a),) for a in SIDES]
    + [(("gz", b),) for b in SIDES]
    + [(("gy", a), ("gz", b)) for b in SIDES for a in SIDES]
    + [(("gx", a),) for a in SIDES]
)
MIRROR = [1, 0, 3, 2, 7, 6, 5, 4, 9, 8]


def greet(links):
    barrier = pltpu.get_barrier_semaphore()
    peers = 0
    for link in links:
        ok, where = near(link)
        peers = peers + ok.astype(jnp.int32)

        @pl.when(ok)
        def _():
            pl.semaphore_signal(barrier, inc=1, device_id=where, device_id_type=MESH)

    return lambda: pl.semaphore_wait(barrier, peers)


class Field:
    def __init__(self, ext, depth, wide, send, recv, send_sem, recv_sem, land=None):
        self.ext, self.depth, self.wide = ext, depth, wide
        self.send, self.recv = send, recv
        self.send_sem, self.recv_sem = send_sem, recv_sem
        self.land = land
        self.nx = ext.shape[0] - 2 * depth
        self.ny = ext.shape[1] - 2 * wide
        self.nz = ext.shape[2] - 128

    def message(self, m):
        d, nx, ny, nz, h = self.depth, self.nx, self.ny, self.nz, self.wide
        ext = self.ext
        if m < 2:
            if h == 8:
                rows = (0, ny - h)[m]
                src = ext.at[pl.ds(d, nx), pl.ds(rows, h), pl.ds(0, nz)]
                place = (ny + h, ny)[m]
                got = ext.at[pl.ds(d, nx), pl.ds(place, h), pl.ds(0, nz)]
                other = ext.at[pl.ds(d, nx), pl.ds((ny, ny + h)[m], h), pl.ds(0, nz)]
            else:
                src = self.send[0].at[m]
                got = self.recv[0].at[m]
                other = self.recv[0].at[1 - m]
        elif m < 4:
            src = self.send[1].at[m - 2]
            got = self.recv[1].at[m - 2]
            other = self.recv[1].at[3 - m]
        elif m < 8:
            b, a = divmod(m - 4, 2)
            src = self.send[1].at[b, pl.ds((0, ny - 8)[a], 8)]
            got = self.recv[2].at[b, a]
            other = self.recv[2].at[1 - b, 1 - a]
        else:
            a = m - 8
            src = ext.at[pl.ds((d, nx)[a], d)]
            if self.land is None:
                got = ext.at[pl.ds((0, d + nx)[a], d)]
                other = ext.at[pl.ds((d + nx, 0)[a], d)]
            else:
                got = self.land.at[a]
                other = self.land.at[1 - a]
        return src, other, got

    def copy(self, m, incoming):
        src, other, got = self.message(m)
        k = m if incoming else MIRROR[m]
        return pltpu.make_async_remote_copy(
            src_ref=got if incoming else src,
            dst_ref=got if incoming else other,
            send_sem=self.send_sem.at[m],
            recv_sem=self.recv_sem.at[k],
            device_id=near(LINKS[m])[1],
            device_id_type=MESH,
        )

    def start(self, which):
        for m in which:
            @pl.when(near(LINKS[m])[0])
            def _():
                self.copy(m, False).start()

    def finish(self, which):
        for m in which:
            ok = near(LINKS[m])[0]

            @pl.when(ok)
            def _():
                self.copy(m, False).wait_send()
                self.copy(m, True).wait_recv()

            @pl.when(jnp.logical_not(ok))
            def _():
                got = self.message(m)[2]
                got[...] = jnp.zeros(got.shape, jnp.float32)

    def pack(self):
        d, nx, ny, nz, h = self.depth, self.nx, self.ny, self.nz, self.wide
        ext = self.ext
        if h != 8:
            for x in range(nx):
                at = slice(d * (x % 8), d * (x % 8) + d)
                self.send[0][0, x // 8, at] = ext[d + x, :d, :nz]
                self.send[0][1, x // 8, at] = ext[d + x, ny - d : ny, :nz]
        group = lax.broadcasted_iota(jnp.int32, (ny, 128), 1) // (2 * h)

        def slab(x, carry):
            low, high = carry
            mine = group == x
            shift = 2 * h * x + h
            low = jnp.where(mine, pltpu.roll(ext[d + x, :ny, :128], shift, 1), low)
            high = jnp.where(mine, pltpu.roll(ext[d + x, :ny, nz - 128 : nz], shift, 1), high)
            return low, high

        zero = jnp.zeros((ny, 128), jnp.float32)
        low, high = lax.fori_loop(0, nx, slab, (zero, zero), unroll=8)
        self.send[1][0] = low
        self.send[1][1] = high

    def unpack(self):
        d, nx, ny, nz, h = self.depth, self.nx, self.ny, self.nz, self.wide
        ext = self.ext
        if h != 8:
            for x in range(nx):
                at = slice(d * (x % 8), d * (x % 8) + d)
                ext[d + x, ny : ny + d, :nz] = self.recv[0][1, x // 8, at]
                ext[d + x, ny + 8 - d : ny + 8, :nz] = self.recv[0][0, x // 8, at]
        ends = []
        for b in range(2):
            corner = (self.recv[2][b, 1], self.recv[2][b, 0])
            if h == 8:
                ends.append(jnp.concatenate([self.recv[1][b], *corner], axis=0))
            else:
                sub = lax.broadcasted_iota(jnp.int32, (8, 128), 0)
                ends.append(
                    jnp.concatenate([self.recv[1][b], jnp.where(sub < h, *corner)], axis=0)
                )
        lane = lax.broadcasted_iota(jnp.int32, ends[0].shape, 1)
        both = jnp.where(lane % (2 * h) < h, ends[0], ends[1])
        edge = (lane < h) | (lane >= 128 - h)

        def slab(x, carry):
            moved = pltpu.roll(both, 128 - h - 2 * h * x, 1)
            ext[d + x, :, nz : nz + 128] = jnp.where(edge, moved, 0.0)
            return carry

        lax.fori_loop(0, nx, slab, 0, unroll=8)


def pair_up(src, pairs):
    def add(j, carry):
        pairs[j] = src[2 * j] + src[2 * j + 1]
        return carry

    lax.fori_loop(0, pairs.shape[0], add, 0)


def pooled(pairs, into, after):
    cx, ny, nz = pairs.shape
    depth = COARSE
    flat = pairs[...].reshape(cx * ny, nz)

    def halves(rows, cols, dim):
        r = lax.broadcasted_iota(jnp.int32, (rows, cols), dim)
        c = lax.broadcasted_iota(jnp.int32, (rows, cols), 1 - dim)
        return (r == jnp.right_shift(c, 1)).astype(jnp.float32).astype(jnp.bfloat16)

    along_z = halves(nz, nz // 2, 1)
    along_y = halves(cx * ny // 2, cx * ny, 0)
    flat = sum(jnp.dot(p, along_z, preferred_element_type=jnp.float32) for p in split3(flat)[:2])
    flat = sum(jnp.dot(along_y, p, preferred_element_type=jnp.float32) for p in split3(flat)[:2])
    out = after(0.5 * flat).reshape(cx, ny // 2, nz // 2)
    into[depth : depth + cx, : ny // 2, : nz // 2] = out


def fine_field(ext, bufs, sems, landing=None):
    ysend, yrecv, zsend, zrecv, yzrecv = bufs
    return Field(ext, FINE, 4, (ysend, zsend), (yrecv, zrecv, yzrecv), *sems, landing)


def coarse_field(ext, bufs, sems):
    zsend, zrecv, yzrecv = bufs
    return Field(ext, COARSE, 8, (None, zsend), (None, zrecv, yzrecv), *sems)


def buf(*shape):
    return pltpu.VMEM(shape, jnp.float32)


def wide_shapes(nx, ny, nz):
    cx, cy, cz = nx // 2, ny // 2, nz // 2
    return (
        (nx + 2 * FINE, ny + 8, nz + 128),
        (cx + 2 * COARSE, cy + 16, cz + 128),
    )


def fine_scratch(nx, ny, nz):
    rows = (2, nx // 8, 8 * FINE, nz)
    return [buf(*rows)] * 2 + [buf(2, ny, 128)] * 2 + [buf(2, 2, 8, 128)]


def coarse_scratch(nx, ny, nz):
    return [buf(2, ny // 2, 128)] * 2 + [buf(2, 2, 8, 128)]


FIRST, LAST = range(8), (8, 9)


def cycle_kernel(forcing, shift_hbm, inverse, cinverse, pressure, *scratch):
    shift, load_sem, scratch = scratch[0], scratch[-1], scratch[1:-1]
    fetch = pltpu.make_async_copy(shift_hbm, shift, load_sem)
    fetch.start()
    (rhs, one, two, update, land, crhs, cone, ctwo, cupdate, pairs), scratch = (
        scratch[:10], scratch[10:],
    )
    bufs_a, bufs_b, bufs_c = scratch[:5], scratch[5:10], scratch[10:13]
    send_sem, recv_sem = scratch[13:]
    arrived = greet(LINKS)
    nx, ny, nz = forcing.shape
    sems = [(send_sem.at[k], recv_sem.at[k]) for k in range(3)]

    def load(x, carry):
        rhs[FINE + x, :ny, :nz] = forcing[x]
        return carry

    lax.fori_loop(0, nx, load, 0, unroll=2)
    field = fine_field(rhs, bufs_a, sems[0])
    field.pack()
    arrived()
    field.start(FIRST)
    field.finish(FIRST)
    field.unpack()
    field.start(LAST)
    slabs = nx + 2 * FINE
    low, high = FINE, FINE + nx
    pairs_of = factors(SMOOTH)
    bufs = (one, two)
    begin(rhs, inverse, one, update, low, high)
    sweep(rhs, inverse, one, two, update, low + 1, high - 1, pairs_of[1])
    field.finish(LAST)
    begin(rhs, inverse, one, update, 0, low)
    begin(rhs, inverse, one, update, high, slabs)
    sweep(rhs, inverse, one, two, update, 1, low + 1, pairs_of[1])
    sweep(rhs, inverse, one, two, update, high - 1, slabs - 1, pairs_of[1])
    for k in range(2, SMOOTH):
        sweep(rhs, inverse, bufs[(k - 1) % 2], bufs[k % 2], update, k, slabs - k, pairs_of[k])
    smooth = bufs[(SMOOTH - 1) % 2]
    other = bufs[SMOOTH % 2]

    fetch.wait()

    def residual(j, carry):
        for r in range(0, ny, 8):
            here = slice(r, r + 8)
            both = 0.0
            for half in range(2):
                x = 2 * j + half
                cells, total = around(smooth, FINE + x, r)
                total = total[:, :nz] + rhs[FINE + x, here, :nz]
                both = both + (total - (6.0 + shift[x, here]) * cells[:, :nz])
            pairs[j, here] = both
        return carry

    lax.fori_loop(0, nx // 2, residual, 0, unroll=2)
    pooled(pairs, crhs, lambda total: total)
    coarse = coarse_field(crhs, bufs_c, sems[2])
    coarse.pack()
    coarse.start(FIRST)
    field = fine_field(smooth, bufs_b, sems[1], land)
    field.pack()
    field.start(FIRST)
    cslabs = crhs.shape[0]
    low = COARSE - (FINE + 1) // 2
    count = cslabs - 2 * low
    cny, cnz = crhs.shape[1:]
    fny, fnz = smooth.shape[1:]

    def fan(shape, fine_dim, per_f, per_c, core, jump):
        f = lax.broadcasted_iota(jnp.int32, shape, fine_dim)
        c = lax.broadcasted_iota(jnp.int32, shape, 1 - fine_dim)
        block = 0
        for g in range(1, shape[fine_dim] // per_f):
            block = block + (f >= g * per_f).astype(jnp.int32)
        inner = f - block * per_f
        target = jnp.right_shift(inner, 1) + jnp.where(inner >= core, jump, 0) + block * per_c
        return (c == target).astype(jnp.float32).astype(jnp.bfloat16)

    fan_y = fan((count * fny, count * cny), 0, fny, cny, ny + 4, cny - fny // 2)
    fan_z = fan((cnz, fnz), 1, fnz, cnz, nz + 64, cnz - fnz // 2)
    coarse.finish(FIRST)
    coarse.unpack()
    coarse.start(LAST)
    pairs_of = factors(COARSE_SMOOTH)
    cbufs = (cone, ctwo)
    inner, outer = COARSE, cslabs - COARSE
    begin(crhs, cinverse, cone, cupdate, inner, outer)
    sweep(crhs, cinverse, cone, ctwo, cupdate, inner + 1, outer - 1, pairs_of[1])
    coarse.finish(LAST)
    begin(crhs, cinverse, cone, cupdate, 0, inner)
    begin(crhs, cinverse, cone, cupdate, outer, cslabs)
    sweep(crhs, cinverse, cone, ctwo, cupdate, 1, inner + 1, pairs_of[1])
    sweep(crhs, cinverse, cone, ctwo, cupdate, outer - 1, cslabs - 1, pairs_of[1])
    for k in range(2, COARSE_SMOOTH):
        sweep(
            crhs, cinverse, cbufs[(k - 1) % 2], cbufs[k % 2], cupdate, k, cslabs - k, pairs_of[k]
        )
    field.finish(FIRST)
    field.unpack()
    field.start(LAST)
    fix = cbufs[(COARSE_SMOOTH - 1) % 2]

    flat = fix[low : low + count].reshape(count * cny, cnz)

    tall = sum(jnp.dot(fan_y, p, preferred_element_type=jnp.float32) for p in split3(flat)[:2])
    full = sum(jnp.dot(p, fan_z, preferred_element_type=jnp.float32) for p in split3(tall)[:2])
    field.finish(LAST)
    for j in range(count):
        part = full[j * fny : (j + 1) * fny]
        for half in range(2):
            x = FINE + 2 * (low + j - COARSE) + half
            if 0 <= x < FINE:
                smooth[x] = land[0, x] + part
            elif FINE <= x < FINE + nx:
                smooth[x] = smooth[x] + part
            elif FINE + nx <= x < slabs:
                smooth[x] = land[1, x - FINE - nx] + part

    pairs_of = factors(SMOOTH)
    bufs = (smooth, other)

    for k in range(SMOOTH):
        sweep(
            rhs, inverse, bufs[k % 2], bufs[(k + 1) % 2], update,
            k + 1, slabs - k - 1, pairs_of[k], pressure if k == SMOOTH - 1 else None,
        )


def cycle(forcing, shift, inverse, cinverse):
    nx, ny, nz = forcing.shape
    wide, cwide = (buf(*shape) for shape in wide_shapes(nx, ny, nz))
    vmem = pl.BlockSpec(memory_space=pltpu.VMEM)
    return pl.pallas_call(
        cycle_kernel,
        in_specs=[vmem, pl.BlockSpec(memory_space=pltpu.HBM), vmem, vmem],
        out_specs=vmem,
        out_shape=jax.ShapeDtypeStruct(forcing.shape, jnp.float32),
        scratch_shapes=[buf(nx, ny, nz)]
        + [wide] * 4
        + [buf(2, FINE, ny + 8, nz + 128)]
        + [cwide] * 4
        + [buf(nx // 2, ny, nz)]
        + fine_scratch(nx, ny, nz) * 2
        + coarse_scratch(nx, ny, nz)
        + [pltpu.SemaphoreType.DMA((3, 10))] * 2
        + [pltpu.SemaphoreType.DMA],
        compiler_params=pltpu.CompilerParams(
            collective_id=1, has_side_effects=True, vmem_limit_bytes=VMEM_LIMIT
        ),
    )(forcing, in_hbm(shift), inverse, cinverse)


BIN = 256
BIN_SHIFT = 15
BIN_CELLS = 1 << BIN_SHIFT
AXES = ("gx", "gy", "gz")


def in_hbm(x):
    return pltpu.with_memory_space_constraint(x, pltpu.HBM)


def levels(rows):
    level = lax.broadcasted_iota(jnp.int32, (rows, LANES), 0)
    if rows > BIN:
        return level
    return level.astype(jnp.float32).astype(jnp.bfloat16)


def hot_rows(level, index, values=None):
    if level.dtype != jnp.int32:
        index = index.astype(jnp.float32).astype(jnp.bfloat16)
    columns = []
    for at in range(0, index.shape[1], LANES):
        here = slice(at, at + LANES)
        value = jnp.ones((), jnp.bfloat16) if values is None else values[:, here]
        same = level == index[:, here]
        columns.append(jnp.where(same, value, jnp.zeros((), jnp.bfloat16)))
    return jnp.concatenate(columns, axis=1)


def place_of(index):
    where = {}
    for axis in reversed(AXES):
        count = lax.axis_size(axis)
        where[axis] = lax.rem(index, count)
        index = lax.div(index, count)
    return where


def front_kernel(
    ndevice, nbin, *refs
):
    sources, refs = refs[:8], refs[8:]
    (force_ref, got_ref, inverse, cinverse), refs = refs[:4], refs[4:]
    (pos_ref, nrm_ref, ten_ref, wgt_ref, con_ref, own_ref, cel_ref, shift), scratch = (
        refs[:8], refs[8:],
    )
    load_sem, scratch = scratch[-1], scratch[:-1]

    def fetch(k):
        return pltpu.make_async_copy(sources[k], refs[k], load_sem.at[k])

    for k in (7, 0, 5, 6, 4, 3, 2, 1):
        fetch(k).start()
    (packed_ref, total_ref, carry_ref, rank_ref, jump_ref, pad_ref, psend, precv, pairs), scratch = (
        scratch[:9], scratch[9:],
    )
    fine_bufs, coarse_bufs = scratch[:5], scratch[5:8]
    send_sem, recv_sem, all_send, all_recv, pos_send, pos_recv = scratch[8:]
    chunk = 4 * LANES
    split = 4
    per = 2 * split
    npoint = ten_ref.shape[1]
    nx, ny, nz = shift.shape
    class_level, slot_level = levels(nbin * ndevice), levels(BIN)
    row_level = levels(total_ref.shape[0])
    me = lax.axis_index(AXES)
    barrier = pltpu.get_barrier_semaphore()

    def other(p):
        return lax.rem(me + p, ndevice)

    def hello(p, carry):
        pl.semaphore_signal(barrier, inc=1, device_id=place_of(other(p)), device_id_type=MESH)
        return carry

    lax.fori_loop(1, ndevice, hello, 0)

    fetch(0).wait()
    psend[0, :3] = pos_ref[:, npoint - LANES :]
    psend[1, :3] = pos_ref[:, :LANES]

    def spread_out(j, carry):
        lower = pos_ref[:, pl.ds(pl.multiple_of(j * LANES - LANES, LANES), LANES)]
        upper = pos_ref[:, pl.ds(pl.multiple_of(j * LANES, LANES), LANES)]
        both = jnp.concatenate([lower[:, HALO:], upper[:, :HALO]], axis=1)
        pad_ref[:3, pl.ds(pl.multiple_of(j * LANES, LANES), LANES)] = both
        return carry

    lax.fori_loop(1, npoint // LANES, spread_out, 0, unroll=7)

    def edge(side, incoming):
        return pltpu.make_async_remote_copy(
            src_ref=psend.at[side],
            dst_ref=precv.at[side],
            send_sem=pos_send.at[side],
            recv_sem=pos_recv.at[side],
            device_id=place_of(other((1, ndevice - 1)[side])),
            device_id_type=MESH,
        )

    def classes(here):
        return own_ref[:, here] + ndevice * jnp.right_shift(cel_ref[:, here], BIN_SHIFT)

    def count(i, total):
        here = pl.ds(pl.multiple_of(i * chunk, chunk), chunk)
        hot = hot_rows(class_level, classes(here)).astype(jnp.float32)
        return total + (
            hot[:, :LANES] + hot[:, LANES : 2 * LANES]
            + (hot[:, 2 * LANES : 3 * LANES] + hot[:, 3 * LANES :])
        )

    for k in (5, 6):
        fetch(k).wait()
    counts = lax.fori_loop(
        0, npoint // chunk, count, jnp.zeros((nbin * ndevice, LANES), jnp.float32), unroll=2
    )
    counts = jnp.sum(counts, axis=1, keepdims=True)
    base = jnp.zeros((ndevice, 1), jnp.float32)
    for b in range(nbin):
        carry_ref[b * ndevice : (b + 1) * ndevice] = base
        base = base + counts[b * ndevice : (b + 1) * ndevice]
    before = (
        lax.broadcasted_iota(jnp.int32, (chunk, chunk), 0)
        < lax.broadcasted_iota(jnp.int32, (chunk, chunk), 1)
    ).astype(jnp.float32).astype(jnp.bfloat16)

    def order(i, carry):
        here = pl.ds(pl.multiple_of(i * chunk, chunk), chunk)
        ones = hot_rows(class_level, classes(here))
        earlier = jnp.dot(ones, before, preferred_element_type=jnp.float32)
        wide = ones.astype(jnp.float32)
        rank = jnp.sum(wide * (earlier + carry), axis=0, keepdims=True)
        rank_ref[:, here] = rank.astype(jnp.int32)
        return carry + (earlier[:, chunk - 1 :] + wide[:, chunk - 1 :])

    lax.fori_loop(0, npoint // chunk, order, carry_ref[...], unroll=4)

    pl.semaphore_wait(barrier, ndevice - 1)

    for side in range(2):
        edge(side, False).start()
    fetch(7).wait()

    def load(x, carry):
        inverse[FINE + x, :ny, :nz] = 1.0 / (6.0 + shift[x])
        return carry

    lax.fori_loop(0, nx, load, 0, unroll=2)
    pair_up(shift, pairs)
    pooled(pairs, cinverse, lambda total: 1.0 / (6.0 + total))
    fine = fine_field(inverse, fine_bufs, (send_sem.at[0], recv_sem.at[0]))
    coarse = coarse_field(cinverse, coarse_bufs, (send_sem.at[1], recv_sem.at[1]))
    fine.pack()
    coarse.pack()
    fine.start(FIRST)
    coarse.start(FIRST)

    def rows_of(device):
        return pl.ds(pl.multiple_of(device * per, per), per)

    def deal(part, p, incoming):
        return pltpu.make_async_remote_copy(
            src_ref=packed_ref.at[part, rows_of(other(p))],
            dst_ref=got_ref.at[part, rows_of(other(ndevice - p) if incoming else me)],
            send_sem=all_send.at[part, p],
            recv_sem=all_recv.at[part, p],
            device_id=place_of(other(p)),
            device_id_type=MESH,
        )

    def send(part):
        def one(p, carry):
            deal(part, p, False).start()
            return carry

        lax.fori_loop(1, ndevice, one, 0)

    def pack(part, pieces):
        total_ref[...] = jnp.zeros_like(total_ref)

        big = npoint // 2

        def some(i, carry):
            here = pl.ds(pl.multiple_of(i * big, big), big)
            rank = rank_ref[:, here]
            slots = hot_rows(slot_level, jnp.bitwise_and(rank, BIN - 1))
            row = own_ref[:, here] * split + jnp.right_shift(rank, 8)
            left = [hot_rows(row_level, row, piece) for piece in pieces(here)]
            both = lax.dot_general(
                jnp.concatenate(left, axis=0), slots, (((1,), (1,)), ((), ())),
                preferred_element_type=jnp.float32,
            )
            count = total_ref.shape[0]
            total_ref[...] += sum(both[k * count : k * count + count] for k in range(len(left)))
            return carry

        lax.fori_loop(0, npoint // big, some, 0)
        sub = lax.broadcasted_iota(jnp.int32, (per, LANES), 0)
        for t in range(ndevice // 2):
            one = total_ref[t * per : t * per + per, :LANES]
            two = total_ref[t * per : t * per + per, LANES:]
            at = 2 * t * per
            packed_ref[part, at : at + per] = jnp.where(sub < split, one, pltpu.roll(two, split, 0))
            packed_ref[part, at + per : at + 2 * per] = jnp.where(
                sub < split, pltpu.roll(one, split, 0), two
            )

    def digits(here):
        cell = cel_ref[:, here] + 1
        for bits in (0, 8, 16):
            digit = jnp.left_shift(jnp.bitwise_and(jnp.right_shift(cell, bits), 255), bits)
            yield digit.astype(jnp.float32).astype(jnp.bfloat16)

    pack(1, digits)
    send(1)
    for k in (4, 3, 2, 1):
        fetch(k).wait()
    for side in range(2):
        edge(side, True).wait_send()
        edge(side, True).wait_recv()
    pad_ref[:3, :LANES] = jnp.concatenate(
        [precv[0, :3, HALO:], pos_ref[:, :HALO]], axis=1
    )
    pad_ref[:3, npoint:] = jnp.concatenate(
        [pos_ref[:, npoint - HALO :], precv[1, :3, :HALO]], axis=1
    )
    begin_at = me * npoint
    everything = npoint * ndevice

    def pull(i, carry):
        for sub in range(2):
            base = pl.multiple_of(i * 2 * LANES + sub * LANES, LANES)
            here = pl.ds(base, LANES)
            lower = pad_ref[:, here]
            upper = pad_ref[:, pl.ds(base + LANES, LANES)]
            centre_pos = jnp.concatenate([lower[:, HALO:], upper[:, :HALO]], axis=1)
            index = con_ref[:, here] - begin_at + HALO
            index = jnp.where(index < 0, index + everything, index)
            index = jnp.where(index >= everything, index - everything, index) - base
            total = jnp.zeros_like(lower)
            for which in range(con_ref.shape[0]):
                wide = jnp.broadcast_to(index[which : which + 1], lower.shape)
                low = jnp.bitwise_and(wide, LANES - 1)
                near_by = jnp.take_along_axis(lower, low, axis=1, mode="promise_in_bounds")
                far = jnp.take_along_axis(upper, low, axis=1, mode="promise_in_bounds")
                picked = jnp.where(wide < LANES, near_by, far)
                total = total + wgt_ref[which : which + 1, here] * (picked - centre_pos)
            force = ten_ref[:, here] * total[:3]
            force_ref[:, here] = force
            jump_ref[:, here] = jnp.sum(force * nrm_ref[:, here], axis=0, keepdims=True)
        return carry

    lax.fori_loop(0, npoint // (2 * LANES), pull, 0, unroll=4)

    pack(0, lambda here: split3(jump_ref[:, here])[:2])
    send(0)
    for part in range(2):
        got_ref[part, rows_of(me)] = packed_ref[part, rows_of(me)]
    fine.finish(FIRST)
    fine.unpack()
    fine.start(LAST)
    coarse.finish(FIRST)
    coarse.unpack()
    coarse.start(LAST)
    fine.finish(LAST)
    coarse.finish(LAST)

    def receive(p, carry):
        for part in range(2):
            deal(part, p, False).wait_send()
            deal(part, p, True).wait_recv()
        return carry

    lax.fori_loop(1, ndevice, receive, 0)


def front(
    positions, normals, tension, edge_weight, connectivity, owner_ids, cell_map, shift,
    ndevice, nbin,
):
    npoint = tension.shape[0]
    nx, ny, nz = shift.shape
    vmem = pl.BlockSpec(memory_space=pltpu.VMEM)
    wide, cwide = wide_shapes(nx, ny, nz)
    return pl.pallas_call(
        functools.partial(front_kernel, ndevice, nbin),
        in_specs=[pl.BlockSpec(memory_space=pltpu.HBM)] * 8,
        out_specs=[vmem] * 4,
        out_shape=[
            jax.ShapeDtypeStruct(shape, jnp.float32)
            for shape in ((3, npoint), (2, 8 * ndevice, LANES), wide, cwide)
        ],
        scratch_shapes=[
            buf(3, npoint),
            buf(3, npoint),
            buf(1, npoint),
            buf(*edge_weight.shape),
            pltpu.VMEM(connectivity.shape, jnp.int32),
            pltpu.VMEM((1, npoint), jnp.int32),
            pltpu.VMEM((1, npoint), jnp.int32),
            buf(nx, ny, nz),
            buf(2, 8 * ndevice, LANES),
            buf(4 * ndevice, BIN),
            buf(nbin * ndevice, 1),
            pltpu.VMEM((1, npoint), jnp.int32),
            buf(1, npoint),
            buf(8, npoint + LANES),
            buf(2, 8, LANES),
            buf(2, 8, LANES),
            buf(nx // 2, ny, nz),
        ]
        + fine_scratch(nx, ny, nz)
        + coarse_scratch(nx, ny, nz)
        + [pltpu.SemaphoreType.DMA((2, 10))] * 2
        + [pltpu.SemaphoreType.DMA((2, ndevice))] * 2
        + [pltpu.SemaphoreType.DMA((2,))] * 2
        + [pltpu.SemaphoreType.DMA((8,))],
        compiler_params=pltpu.CompilerParams(
            collective_id=0, has_side_effects=True, vmem_limit_bytes=20 * 2**20
        ),
    )(
        *map(
            in_hbm,
            (
                positions, normals, tension[None], edge_weight, connectivity, owner_ids[None],
                cell_map[None], shift,
            ),
        )
    )


GROUP = 72


def scatter_kernel(
    nbin, rhs_hbm, got_ref, force_ref, out_ref, force_hbm,
    rhs_ref, acc_ref, list_ref, chunk_ref, sems,
):
    nrow, nz = rhs_ref.shape
    fetch = pltpu.make_async_copy(rhs_hbm, rhs_ref, sems.at[1])
    fetch.start()
    put = pltpu.make_async_copy(force_ref, force_hbm, sems.at[2])
    put.start()
    per = 8
    nsource = got_ref.shape[1] // per
    rows = nrow // nbin
    got = got_ref[1].reshape(nsource, per, LANES)
    used = got > 0.0
    lane = lax.broadcasted_iota(jnp.int32, (nsource, LANES), 1)
    ends = jnp.zeros((nsource, LANES), jnp.float32)
    for b in range(nbin):
        inside = jnp.where(used & (got <= float((b + 1) * BIN_CELLS)), 1.0, 0.0)
        total = jnp.sum(jnp.sum(inside, axis=1), axis=1, keepdims=True)
        ends = jnp.where(lane == b + 1, total, ends)
    ends = ends.astype(jnp.int32)
    stops = pltpu.roll(ends, LANES - 1, 1)
    firsts = jnp.right_shift(ends, 7)
    counts = jnp.where(stops > ends, jnp.right_shift(stops + LANES - 1, 7) - firsts, 0)
    counts = jnp.where(lane < nbin, counts, 0).astype(jnp.float32)
    square = (nsource, nsource)
    before = (
        lax.broadcasted_iota(jnp.int32, square, 0) > lax.broadcasted_iota(jnp.int32, square, 1)
    ).astype(jnp.float32).astype(jnp.bfloat16)
    starts = jnp.dot(before, counts.astype(jnp.bfloat16), preferred_element_type=jnp.float32)
    sums = jnp.sum(counts, axis=0, keepdims=True)
    width = list_ref.shape[1]
    source = lax.broadcasted_iota(jnp.int32, (nsource, width), 0)
    position = lax.broadcasted_iota(jnp.int32, (nsource, width), 1)
    for b in range(nbin):
        pick = slice(b, b + 1)
        step = position - starts[:, pick].astype(jnp.int32)
        chunk = firsts[:, pick] + step
        row = source * per + jnp.bitwise_and(chunk, 1) * (per // 2) + jnp.right_shift(chunk, 1)
        inside = (step >= 0) & (step < counts[:, pick].astype(jnp.int32))
        row = jnp.sum(jnp.where(inside, row.astype(jnp.float32), 0.0), axis=0, keepdims=True)
        list_ref[b : b + 1] = row.astype(jnp.int32)
        list_ref[nbin + b : nbin + b + 1] = jnp.broadcast_to(sums[:, pick], (1, width)).astype(
            jnp.int32
        )
    copy = pltpu.make_async_copy(list_ref, chunk_ref, sems.at[0])
    copy.start()
    copy.wait()
    fetch.wait()
    zero, unit = jnp.zeros((), jnp.bfloat16), jnp.ones((), jnp.bfloat16)
    row_level, col_level = levels(2 * rows), levels(BIN)

    def quarter(b, carry):
        total = chunk_ref[nbin + b, 0]
        acc_ref[...] = jnp.zeros_like(acc_ref)

        def work(step, carry):
            highs, lows, cols = [], [], []
            for k in range(GROUP):
                at = step * GROUP + k
                row = chunk_ref[b, jnp.minimum(at, width - 1)]
                value = got_ref[0, pl.ds(row, 1)]
                cell = got_ref[1, pl.ds(row, 1)].astype(jnp.int32) - 1
                fits = (jnp.right_shift(cell, BIN_SHIFT) == b) & (at < total)
                half = jnp.bitwise_and(jnp.right_shift(cell, 8), 1)
                place = half * rows + jnp.bitwise_and(jnp.right_shift(cell, 9), rows - 1)
                place = jnp.where(fits, place, 2 * rows).astype(jnp.float32).astype(jnp.bfloat16)
                col = jnp.bitwise_and(cell, BIN - 1).astype(jnp.float32).astype(jnp.bfloat16)
                first = value.astype(jnp.bfloat16)
                second = (value - first.astype(jnp.float32)).astype(jnp.bfloat16)
                same = row_level == place
                highs.append(jnp.where(same, first, zero))
                lows.append(jnp.where(same, second, zero))
                cols.append(jnp.where(col_level == col, unit, zero))
            left = jnp.concatenate(
                [jnp.concatenate(highs, axis=1), jnp.concatenate(lows, axis=1)], axis=0
            )
            both = lax.dot_general(
                left, jnp.concatenate(cols, axis=1), (((1,), (1,)), ((), ())),
                preferred_element_type=jnp.float32,
            )
            acc_ref[...] += both[: 2 * rows] + both[2 * rows :]
            return carry

        lax.fori_loop(0, lax.div(total + GROUP - 1, GROUP), work, 0)
        here = pl.ds(pl.multiple_of(b * rows, rows), rows)
        for half in range(2):
            cols = slice(half * BIN, (half + 1) * BIN)
            out_ref[here, cols] = rhs_ref[here, cols] + acc_ref[half * rows : (half + 1) * rows]
        return carry

    lax.fori_loop(0, nbin, quarter, 0)
    put.wait()


def scatter(rhs, got, force, nsource, nbin):
    nx, ny, nz = rhs.shape
    nrow = nx * ny
    vmem = pl.BlockSpec(memory_space=pltpu.VMEM)
    hbm = pl.BlockSpec(memory_space=pltpu.HBM)
    out, force = pl.pallas_call(
        functools.partial(scatter_kernel, nbin),
        in_specs=[hbm, vmem, vmem],
        out_specs=[vmem, hbm],
        out_shape=[
            jax.ShapeDtypeStruct((nrow, nz), jnp.float32),
            jax.ShapeDtypeStruct(force.shape, jnp.float32),
        ],
        scratch_shapes=[
            pltpu.VMEM((nrow, nz), jnp.float32),
            pltpu.VMEM((2 * nrow // nbin, BIN), jnp.float32),
            pltpu.VMEM((2 * nbin, 8 * nsource), jnp.int32),
            pltpu.SMEM((2 * nbin, 8 * nsource), jnp.int32),
            pltpu.SemaphoreType.DMA((3,)),
        ],
        compiler_params=pltpu.CompilerParams(vmem_limit_bytes=24 * 2**20),
        cost_estimate=pl.CostEstimate(
            flops=4 * nrow * nz * got.size // 2, bytes_accessed=4000000, transcendentals=0
        ),
    )(in_hbm(rhs.reshape(nrow, nz)), got, force)
    return out.reshape(nx, ny, nz), force


def body(
    pressure_rhs,
    shift_diag,
    positions,
    normals,
    tension,
    edge_weight,
    owner_map,
    cell_map,
    connectivity,
):
    ndevice = lax.axis_size(AXES)
    nbin = pressure_rhs.size // BIN_CELLS
    surface_force, got, inverse, cinverse = front(
        positions, normals, tension, edge_weight, connectivity, owner_map[:, 0], cell_map,
        shift_diag, ndevice, nbin,
    )
    forcing, surface_force = scatter(pressure_rhs, got, surface_force, ndevice, nbin)
    pressure = cycle(forcing, shift_diag, inverse, cinverse)
    return (pressure, surface_force)


def solution(mesh):
    return jax.shard_map(
        body,
        mesh=mesh,
        in_specs=(
            P("gx", "gy", "gz"),
            P("gx", "gy", "gz"),
            P(None, ("gx", "gy", "gz")),
            P(None, ("gx", "gy", "gz")),
            P(("gx", "gy", "gz")),
            P(None, ("gx", "gy", "gz")),
            P(("gx", "gy", "gz"), None),
            P(("gx", "gy", "gz")),
            P(None, ("gx", "gy", "gz")),
        ),
        out_specs=(P("gx", "gy", "gz"), P(None, ("gx", "gy", "gz"))),
        check_vma=False,
    )
```

```python
import functools

import jax
import jax.numpy as jnp
from jax import lax
from jax.experimental import pallas as pl
from jax.experimental.pallas import tpu as pltpu
from jax.sharding import PartitionSpec as P

HALO = 64
SMOOTH = 3
COARSE_SMOOTH = 4
LANES = 2 * HALO


centre = 1.125
spread = 0.875


def factors(sweeps):
    ratio = centre / spread
    fac = 1.0 / ratio
    pairs = [(0.0, 1.0 / centre)]
    for _ in range(1, sweeps):
        fac_new = 1.0 / (2.0 * ratio - fac)
        pairs.append((fac_new * fac, 2.0 * fac_new / spread))
        fac = fac_new
    return pairs


def split3(x):
    a = x.astype(jnp.bfloat16)
    rest = x - a.astype(jnp.float32)
    b = rest.astype(jnp.bfloat16)
    c = (rest - b.astype(jnp.float32)).astype(jnp.bfloat16)
    return a, b, c


MESH = pl.DeviceIdType.MESH
FINE = SMOOTH
COARSE = COARSE_SMOOTH - 1 + (SMOOTH + 1) // 2


UNROLL = 4
VMEM_LIMIT = 36 * 2**20


def around(src, x, r):
    ny, nz = src.shape[1:]
    sub = lax.broadcasted_iota(jnp.int32, (8, nz), 0)
    here = slice(r, r + 8)
    below, above = (r - 8) % ny, (r + 8) % ny
    cells = src[x, here]
    total = src[x - 1, here] + src[x + 1, here]
    total = total + (
        pltpu.roll(jnp.where(sub == 7, src[x, below : below + 8], cells), 1, 0)
        + pltpu.roll(jnp.where(sub == 0, src[x, above : above + 8], cells), 7, 0)
    )
    return cells, total + (pltpu.roll(cells, 1, 1) + pltpu.roll(cells, nz - 1, 1))


def sweep(rhs, inverse, src, dst, update, first, last, pair, keep=None):
    old, new = pair
    rows = src.shape[1] if keep is None else keep.shape[1]

    def slab(x, carry):
        for r in range(0, rows, 8):
            here = slice(r, r + 8)
            cells, total = around(src, x, r)
            change = new * (inverse[x, here] * (rhs[x, here] + total) - cells)
            if old:
                change = change + old * update[x, here]
            if keep is None:
                update[x, here] = change
                dst[x, here] = cells + change
            else:
                keep[x - first, here] = (cells + change)[:, : keep.shape[2]]
        return carry

    lax.fori_loop(first, last, slab, 0, unroll=UNROLL)


def begin(rhs, inverse, dst, update, first, last):
    def slab(x, carry):
        change = inverse[x] * rhs[x] * (1.0 / centre)
        update[x] = change
        dst[x] = change
        return carry

    lax.fori_loop(first, last, slab, 0, unroll=2)


def near(axes):
    ok = None
    where = {}
    for axis, step in axes:
        place = lax.axis_index(axis) + step
        fits = (place >= 0) & (place < lax.axis_size(axis))
        ok = fits if ok is None else ok & fits
        where[axis] = place
    return ok, where


SIDES = (-1, 1)
LINKS = (
    [(("gy", a),) for a in SIDES]
    + [(("gz", b),) for b in SIDES]
    + [(("gy", a), ("gz", b)) for b in SIDES for a in SIDES]
    + [(("gx", a),) for a in SIDES]
)
MIRROR = [1, 0, 3, 2, 7, 6, 5, 4, 9, 8]


def greet(links):
    barrier = pltpu.get_barrier_semaphore()
    peers = 0
    for link in links:
        ok, where = near(link)
        peers = peers + ok.astype(jnp.int32)

        @pl.when(ok)
        def _():
            pl.semaphore_signal(barrier, inc=1, device_id=where, device_id_type=MESH)

    return lambda: pl.semaphore_wait(barrier, peers)


class Field:
    def __init__(self, ext, depth, wide, send, recv, send_sem, recv_sem, land=None):
        self.ext, self.depth, self.wide = ext, depth, wide
        self.send, self.recv = send, recv
        self.send_sem, self.recv_sem = send_sem, recv_sem
        self.land = land
        self.nx = ext.shape[0] - 2 * depth
        self.ny = ext.shape[1] - 2 * wide
        self.nz = ext.shape[2] - 128

    def message(self, m):
        d, nx, ny, nz, h = self.depth, self.nx, self.ny, self.nz, self.wide
        ext = self.ext
        if m < 2:
            if h == 8:
                rows = (0, ny - h)[m]
                src = ext.at[pl.ds(d, nx), pl.ds(rows, h), pl.ds(0, nz)]
                place = (ny + h, ny)[m]
                got = ext.at[pl.ds(d, nx), pl.ds(place, h), pl.ds(0, nz)]
                other = ext.at[pl.ds(d, nx), pl.ds((ny, ny + h)[m], h), pl.ds(0, nz)]
            else:
                src = self.send[0].at[m]
                got = self.recv[0].at[m]
                other = self.recv[0].at[1 - m]
        elif m < 4:
            src = self.send[1].at[m - 2]
            got = self.recv[1].at[m - 2]
            other = self.recv[1].at[3 - m]
        elif m < 8:
            b, a = divmod(m - 4, 2)
            src = self.send[1].at[b, pl.ds((0, ny - 8)[a], 8)]
            got = self.recv[2].at[b, a]
            other = self.recv[2].at[1 - b, 1 - a]
        else:
            a = m - 8
            src = ext.at[pl.ds((d, nx)[a], d)]
            if self.land is None:
                got = ext.at[pl.ds((0, d + nx)[a], d)]
                other = ext.at[pl.ds((d + nx, 0)[a], d)]
            else:
                got = self.land.at[a]
                other = self.land.at[1 - a]
        return src, other, got

    def copy(self, m, incoming):
        src, other, got = self.message(m)
        k = m if incoming else MIRROR[m]
        return pltpu.make_async_remote_copy(
            src_ref=got if incoming else src,
            dst_ref=got if incoming else other,
            send_sem=self.send_sem.at[m],
            recv_sem=self.recv_sem.at[k],
            device_id=near(LINKS[m])[1],
            device_id_type=MESH,
        )

    def start(self, which):
        for m in which:
            @pl.when(near(LINKS[m])[0])
            def _():
                self.copy(m, False).start()

    def finish(self, which):
        for m in which:
            ok = near(LINKS[m])[0]

            @pl.when(ok)
            def _():
                self.copy(m, False).wait_send()
                self.copy(m, True).wait_recv()

            @pl.when(jnp.logical_not(ok))
            def _():
                got = self.message(m)[2]
                got[...] = jnp.zeros(got.shape, jnp.float32)

    def pack(self):
        d, nx, ny, nz, h = self.depth, self.nx, self.ny, self.nz, self.wide
        ext = self.ext
        if h != 8:
            for x in range(nx):
                at = slice(d * (x % 8), d * (x % 8) + d)
                self.send[0][0, x // 8, at] = ext[d + x, :d, :nz]
                self.send[0][1, x // 8, at] = ext[d + x, ny - d : ny, :nz]
        group = lax.broadcasted_iota(jnp.int32, (ny, 128), 1) // (2 * h)

        def slab(x, carry):
            low, high = carry
            mine = group == x
            shift = 2 * h * x + h
            low = jnp.where(mine, pltpu.roll(ext[d + x, :ny, :128], shift, 1), low)
            high = jnp.where(mine, pltpu.roll(ext[d + x, :ny, nz - 128 : nz], shift, 1), high)
            return low, high

        zero = jnp.zeros((ny, 128), jnp.float32)
        low, high = lax.fori_loop(0, nx, slab, (zero, zero), unroll=8)
        self.send[1][0] = low
        self.send[1][1] = high

    def unpack(self):
        d, nx, ny, nz, h = self.depth, self.nx, self.ny, self.nz, self.wide
        ext = self.ext
        if h != 8:
            for x in range(nx):
                at = slice(d * (x % 8), d * (x % 8) + d)
                ext[d + x, ny : ny + d, :nz] = self.recv[0][1, x // 8, at]
                ext[d + x, ny + 8 - d : ny + 8, :nz] = self.recv[0][0, x // 8, at]
        ends = []
        for b in range(2):
            corner = (self.recv[2][b, 1], self.recv[2][b, 0])
            if h == 8:
                ends.append(jnp.concatenate([self.recv[1][b], *corner], axis=0))
            else:
                sub = lax.broadcasted_iota(jnp.int32, (8, 128), 0)
                ends.append(
                    jnp.concatenate([self.recv[1][b], jnp.where(sub < h, *corner)], axis=0)
                )
        lane = lax.broadcasted_iota(jnp.int32, ends[0].shape, 1)
        both = jnp.where(lane % (2 * h) < h, ends[0], ends[1])
        edge = (lane < h) | (lane >= 128 - h)

        def slab(x, carry):
            moved = pltpu.roll(both, 128 - h - 2 * h * x, 1)
            ext[d + x, :, nz : nz + 128] = jnp.where(edge, moved, 0.0)
            return carry

        lax.fori_loop(0, nx, slab, 0, unroll=8)


def pair_up(src, pairs):
    def add(j, carry):
        pairs[j] = src[2 * j] + src[2 * j + 1]
        return carry

    lax.fori_loop(0, pairs.shape[0], add, 0)


def pooled(pairs, into, after):
    cx, ny, nz = pairs.shape
    depth = COARSE
    flat = pairs[...].reshape(cx * ny, nz)

    def halves(rows, cols, dim):
        r = lax.broadcasted_iota(jnp.int32, (rows, cols), dim)
        c = lax.broadcasted_iota(jnp.int32, (rows, cols), 1 - dim)
        return (r == jnp.right_shift(c, 1)).astype(jnp.float32).astype(jnp.bfloat16)

    along_z = halves(nz, nz // 2, 1)
    along_y = halves(cx * ny // 2, cx * ny, 0)
    flat = sum(jnp.dot(p, along_z, preferred_element_type=jnp.float32) for p in split3(flat)[:2])
    flat = sum(jnp.dot(along_y, p, preferred_element_type=jnp.float32) for p in split3(flat)[:2])
    out = after(0.5 * flat).reshape(cx, ny // 2, nz // 2)
    into[depth : depth + cx, : ny // 2, : nz // 2] = out


def fine_field(ext, bufs, sems, landing=None):
    ysend, yrecv, zsend, zrecv, yzrecv = bufs
    return Field(ext, FINE, 4, (ysend, zsend), (yrecv, zrecv, yzrecv), *sems, landing)


def coarse_field(ext, bufs, sems):
    zsend, zrecv, yzrecv = bufs
    return Field(ext, COARSE, 8, (None, zsend), (None, zrecv, yzrecv), *sems)


def buf(*shape):
    return pltpu.VMEM(shape, jnp.float32)


def wide_shapes(nx, ny, nz):
    cx, cy, cz = nx // 2, ny // 2, nz // 2
    return (
        (nx + 2 * FINE, ny + 8, nz + 128),
        (cx + 2 * COARSE, cy + 16, cz + 128),
    )


def fine_scratch(nx, ny, nz):
    rows = (2, nx // 8, 8 * FINE, nz)
    return [buf(*rows)] * 2 + [buf(2, ny, 128)] * 2 + [buf(2, 2, 8, 128)]


def coarse_scratch(nx, ny, nz):
    return [buf(2, ny // 2, 128)] * 2 + [buf(2, 2, 8, 128)]


FIRST, LAST = range(8), (8, 9)


def cycle_kernel(forcing, shift_hbm, inverse, cinverse, pressure, *scratch):
    shift, load_sem, scratch = scratch[0], scratch[-1], scratch[1:-1]
    fetch = pltpu.make_async_copy(shift_hbm, shift, load_sem)
    fetch.start()
    (rhs, one, two, update, land, crhs, cone, ctwo, cupdate, pairs), scratch = (
        scratch[:10], scratch[10:],
    )
    bufs_a, bufs_b, bufs_c = scratch[:5], scratch[5:10], scratch[10:13]
    send_sem, recv_sem = scratch[13:]
    arrived = greet(LINKS)
    nx, ny, nz = forcing.shape
    sems = [(send_sem.at[k], recv_sem.at[k]) for k in range(3)]

    def load(x, carry):
        rhs[FINE + x, :ny, :nz] = forcing[x]
        return carry

    lax.fori_loop(0, nx, load, 0, unroll=2)
    field = fine_field(rhs, bufs_a, sems[0])
    field.pack()
    arrived()
    field.start(FIRST)
    field.finish(FIRST)
    field.unpack()
    field.start(LAST)
    slabs = nx + 2 * FINE
    low, high = FINE, FINE + nx
    pairs_of = factors(SMOOTH)
    bufs = (one, two)
    begin(rhs, inverse, one, update, low, high)
    sweep(rhs, inverse, one, two, update, low + 1, high - 1, pairs_of[1])
    field.finish(LAST)
    begin(rhs, inverse, one, update, 0, low)
    begin(rhs, inverse, one, update, high, slabs)
    sweep(rhs, inverse, one, two, update, 1, low + 1, pairs_of[1])
    sweep(rhs, inverse, one, two, update, high - 1, slabs - 1, pairs_of[1])
    for k in range(2, SMOOTH):
        sweep(rhs, inverse, bufs[(k - 1) % 2], bufs[k % 2], update, k, slabs - k, pairs_of[k])
    smooth = bufs[(SMOOTH - 1) % 2]
    other = bufs[SMOOTH % 2]

    fetch.wait()

    def residual(j, carry):
        for r in range(0, ny, 8):
            here = slice(r, r + 8)
            both = 0.0
            for half in range(2):
                x = 2 * j + half
                cells, total = around(smooth, FINE + x, r)
                total = total[:, :nz] + rhs[FINE + x, here, :nz]
                both = both + (total - (6.0 + shift[x, here]) * cells[:, :nz])
            pairs[j, here] = both
        return carry

    lax.fori_loop(0, nx // 2, residual, 0, unroll=2)
    pooled(pairs, crhs, lambda total: total)
    coarse = coarse_field(crhs, bufs_c, sems[2])
    coarse.pack()
    coarse.start(FIRST)
    field = fine_field(smooth, bufs_b, sems[1], land)
    field.pack()
    field.start(FIRST)
    cslabs = crhs.shape[0]
    low = COARSE - (FINE + 1) // 2
    count = cslabs - 2 * low
    cny, cnz = crhs.shape[1:]
    fny, fnz = smooth.shape[1:]

    def fan(shape, fine_dim, per_f, per_c, core, jump):
        f = lax.broadcasted_iota(jnp.int32, shape, fine_dim)
        c = lax.broadcasted_iota(jnp.int32, shape, 1 - fine_dim)
        block = 0
        for g in range(1, shape[fine_dim] // per_f):
            block = block + (f >= g * per_f).astype(jnp.int32)
        inner = f - block * per_f
        target = jnp.right_shift(inner, 1) + jnp.where(inner >= core, jump, 0) + block * per_c
        return (c == target).astype(jnp.float32).astype(jnp.bfloat16)

    fan_y = fan((count * fny, count * cny), 0, fny, cny, ny + 4, cny - fny // 2)
    fan_z = fan((cnz, fnz), 1, fnz, cnz, nz + 64, cnz - fnz // 2)
    coarse.finish(FIRST)
    coarse.unpack()
    coarse.start(LAST)
    pairs_of = factors(COARSE_SMOOTH)
    cbufs = (cone, ctwo)
    inner, outer = COARSE, cslabs - COARSE
    begin(crhs, cinverse, cone, cupdate, inner, outer)
    sweep(crhs, cinverse, cone, ctwo, cupdate, inner + 1, outer - 1, pairs_of[1])
    coarse.finish(LAST)
    begin(crhs, cinverse, cone, cupdate, 0, inner)
    begin(crhs, cinverse, cone, cupdate, outer, cslabs)
    sweep(crhs, cinverse, cone, ctwo, cupdate, 1, inner + 1, pairs_of[1])
    sweep(crhs, cinverse, cone, ctwo, cupdate, outer - 1, cslabs - 1, pairs_of[1])
    for k in range(2, COARSE_SMOOTH):
        sweep(
            crhs, cinverse, cbufs[(k - 1) % 2], cbufs[k % 2], cupdate, k, cslabs - k, pairs_of[k]
        )
    field.finish(FIRST)
    field.unpack()
    field.start(LAST)
    fix = cbufs[(COARSE_SMOOTH - 1) % 2]

    flat = fix[low : low + count].reshape(count * cny, cnz)

    tall = sum(jnp.dot(fan_y, p, preferred_element_type=jnp.float32) for p in split3(flat)[:2])
    full = sum(jnp.dot(p, fan_z, preferred_element_type=jnp.float32) for p in split3(tall)[:2])
    field.finish(LAST)
    for j in range(count):
        part = full[j * fny : (j + 1) * fny]
        for half in range(2):
            x = FINE + 2 * (low + j - COARSE) + half
            if 0 <= x < FINE:
                smooth[x] = land[0, x] + part
            elif FINE <= x < FINE + nx:
                smooth[x] = smooth[x] + part
            elif FINE + nx <= x < slabs:
                smooth[x] = land[1, x - FINE - nx] + part

    pairs_of = factors(SMOOTH)
    bufs = (smooth, other)

    for k in range(SMOOTH):
        sweep(
            rhs, inverse, bufs[k % 2], bufs[(k + 1) % 2], update,
            k + 1, slabs - k - 1, pairs_of[k], pressure if k == SMOOTH - 1 else None,
        )


def cycle(forcing, shift, inverse, cinverse):
    nx, ny, nz = forcing.shape
    wide, cwide = (buf(*shape) for shape in wide_shapes(nx, ny, nz))
    vmem = pl.BlockSpec(memory_space=pltpu.VMEM)
    return pl.pallas_call(
        cycle_kernel,
        in_specs=[vmem, pl.BlockSpec(memory_space=pltpu.HBM), vmem, vmem],
        out_specs=vmem,
        out_shape=jax.ShapeDtypeStruct(forcing.shape, jnp.float32),
        scratch_shapes=[buf(nx, ny, nz)]
        + [wide] * 4
        + [buf(2, FINE, ny + 8, nz + 128)]
        + [cwide] * 4
        + [buf(nx // 2, ny, nz)]
        + fine_scratch(nx, ny, nz) * 2
        + coarse_scratch(nx, ny, nz)
        + [pltpu.SemaphoreType.DMA((3, 10))] * 2
        + [pltpu.SemaphoreType.DMA],
        compiler_params=pltpu.CompilerParams(
            collective_id=1, has_side_effects=True, vmem_limit_bytes=VMEM_LIMIT
        ),
    )(forcing, in_hbm(shift), inverse, cinverse)


BIN = 256
BIN_SHIFT = 15
BIN_CELLS = 1 << BIN_SHIFT
AXES = ("gx", "gy", "gz")


def in_hbm(x):
    return pltpu.with_memory_space_constraint(x, pltpu.HBM)


def levels(rows):
    level = lax.broadcasted_iota(jnp.int32, (rows, LANES), 0)
    if rows > BIN:
        return level
    return level.astype(jnp.float32).astype(jnp.bfloat16)


def hot_rows(level, index, values=None):
    if level.dtype != jnp.int32:
        index = index.astype(jnp.float32).astype(jnp.bfloat16)
    columns = []
    for at in range(0, index.shape[1], LANES):
        here = slice(at, at + LANES)
        value = jnp.ones((), jnp.bfloat16) if values is None else values[:, here]
        same = level == index[:, here]
        columns.append(jnp.where(same, value, jnp.zeros((), jnp.bfloat16)))
    return jnp.concatenate(columns, axis=1)


def place_of(index):
    where = {}
    for axis in reversed(AXES):
        count = lax.axis_size(axis)
        where[axis] = lax.rem(index, count)
        index = lax.div(index, count)
    return where


def front_kernel(
    ndevice, nbin, *refs
):
    sources, refs = refs[:8], refs[8:]
    (force_ref, got_ref, inverse, cinverse), refs = refs[:4], refs[4:]
    (pos_ref, nrm_ref, ten_ref, wgt_ref, con_ref, own_ref, cel_ref, shift), scratch = (
        refs[:8], refs[8:],
    )
    load_sem, scratch = scratch[-1], scratch[:-1]

    def fetch(k):
        return pltpu.make_async_copy(sources[k], refs[k], load_sem.at[k])

    for k in (7, 0, 5, 6, 4, 3, 2, 1):
        fetch(k).start()
    (packed_ref, total_ref, carry_ref, rank_ref, jump_ref, pad_ref, psend, precv, pairs), scratch = (
        scratch[:9], scratch[9:],
    )
    fine_bufs, coarse_bufs = scratch[:5], scratch[5:8]
    send_sem, recv_sem, all_send, all_recv, pos_send, pos_recv = scratch[8:]
    chunk = 4 * LANES
    split = 4
    per = 2 * split
    npoint = ten_ref.shape[1]
    nx, ny, nz = shift.shape
    class_level, slot_level = levels(nbin * ndevice), levels(BIN)
    row_level = levels(total_ref.shape[0])
    me = lax.axis_index(AXES)
    barrier = pltpu.get_barrier_semaphore()

    def other(p):
        return lax.rem(me + p, ndevice)

    def hello(p, carry):
        pl.semaphore_signal(barrier, inc=1, device_id=place_of(other(p)), device_id_type=MESH)
        return carry

    lax.fori_loop(1, ndevice, hello, 0)

    fetch(0).wait()
    psend[0, :3] = pos_ref[:, npoint - LANES :]
    psend[1, :3] = pos_ref[:, :LANES]

    def spread_out(j, carry):
        lower = pos_ref[:, pl.ds(pl.multiple_of(j * LANES - LANES, LANES), LANES)]
        upper = pos_ref[:, pl.ds(pl.multiple_of(j * LANES, LANES), LANES)]
        both = jnp.concatenate([lower[:, HALO:], upper[:, :HALO]], axis=1)
        pad_ref[:3, pl.ds(pl.multiple_of(j * LANES, LANES), LANES)] = both
        return carry

    lax.fori_loop(1, npoint // LANES, spread_out, 0, unroll=7)

    def edge(side, incoming):
        return pltpu.make_async_remote_copy(
            src_ref=psend.at[side],
            dst_ref=precv.at[side],
            send_sem=pos_send.at[side],
            recv_sem=pos_recv.at[side],
            device_id=place_of(other((1, ndevice - 1)[side])),
            device_id_type=MESH,
        )

    def classes(here):
        return own_ref[:, here] + ndevice * jnp.right_shift(cel_ref[:, here], BIN_SHIFT)

    def count(i, total):
        here = pl.ds(pl.multiple_of(i * chunk, chunk), chunk)
        hot = hot_rows(class_level, classes(here)).astype(jnp.float32)
        return total + (
            hot[:, :LANES] + hot[:, LANES : 2 * LANES]
            + (hot[:, 2 * LANES : 3 * LANES] + hot[:, 3 * LANES :])
        )

    for k in (5, 6):
        fetch(k).wait()
    counts = lax.fori_loop(
        0, npoint // chunk, count, jnp.zeros((nbin * ndevice, LANES), jnp.float32), unroll=2
    )
    counts = jnp.sum(counts, axis=1, keepdims=True)
    base = jnp.zeros((ndevice, 1), jnp.float32)
    for b in range(nbin):
        carry_ref[b * ndevice : (b + 1) * ndevice] = base
        base = base + counts[b * ndevice : (b + 1) * ndevice]
    before = (
        lax.broadcasted_iota(jnp.int32, (chunk, chunk), 0)
        < lax.broadcasted_iota(jnp.int32, (chunk, chunk), 1)
    ).astype(jnp.float32).astype(jnp.bfloat16)

    def order(i, carry):
        here = pl.ds(pl.multiple_of(i * chunk, chunk), chunk)
        ones = hot_rows(class_level, classes(here))
        earlier = jnp.dot(ones, before, preferred_element_type=jnp.float32)
        wide = ones.astype(jnp.float32)
        rank = jnp.sum(wide * (earlier + carry), axis=0, keepdims=True)
        rank_ref[:, here] = rank.astype(jnp.int32)
        return carry + (earlier[:, chunk - 1 :] + wide[:, chunk - 1 :])

    lax.fori_loop(0, npoint // chunk, order, carry_ref[...], unroll=8)

    pl.semaphore_wait(barrier, ndevice - 1)

    for side in range(2):
        edge(side, False).start()
    fetch(7).wait()

    def load(x, carry):
        inverse[FINE + x, :ny, :nz] = 1.0 / (6.0 + shift[x])
        return carry

    lax.fori_loop(0, nx, load, 0, unroll=2)
    pair_up(shift, pairs)
    pooled(pairs, cinverse, lambda total: 1.0 / (6.0 + total))
    fine = fine_field(inverse, fine_bufs, (send_sem.at[0], recv_sem.at[0]))
    coarse = coarse_field(cinverse, coarse_bufs, (send_sem.at[1], recv_sem.at[1]))
    fine.pack()
    coarse.pack()
    fine.start(FIRST)
    coarse.start(FIRST)

    def rows_of(device):
        return pl.ds(pl.multiple_of(device * per, per), per)

    def deal(part, p, incoming):
        return pltpu.make_async_remote_copy(
            src_ref=packed_ref.at[part, rows_of(other(p))],
            dst_ref=got_ref.at[part, rows_of(other(ndevice - p) if incoming else me)],
            send_sem=all_send.at[part, p],
            recv_sem=all_recv.at[part, p],
            device_id=place_of(other(p)),
            device_id_type=MESH,
        )

    def send(part):
        def one(p, carry):
            deal(part, p, False).start()
            return carry

        lax.fori_loop(1, ndevice, one, 0)

    def pack(part, pieces):
        total_ref[...] = jnp.zeros_like(total_ref)

        big = npoint // 2

        def some(i, carry):
            here = pl.ds(pl.multiple_of(i * big, big), big)
            rank = rank_ref[:, here]
            slots = hot_rows(slot_level, jnp.bitwise_and(rank, BIN - 1))
            row = own_ref[:, here] * split + jnp.right_shift(rank, 8)
            left = [hot_rows(row_level, row, piece) for piece in pieces(here)]
            both = lax.dot_general(
                jnp.concatenate(left, axis=0), slots, (((1,), (1,)), ((), ())),
                preferred_element_type=jnp.float32,
            )
            count = total_ref.shape[0]
            total_ref[...] += sum(both[k * count : k * count + count] for k in range(len(left)))
            return carry

        lax.fori_loop(0, npoint // big, some, 0)
        sub = lax.broadcasted_iota(jnp.int32, (per, LANES), 0)
        for t in range(ndevice // 2):
            one = total_ref[t * per : t * per + per, :LANES]
            two = total_ref[t * per : t * per + per, LANES:]
            at = 2 * t * per
            packed_ref[part, at : at + per] = jnp.where(sub < split, one, pltpu.roll(two, split, 0))
            packed_ref[part, at + per : at + 2 * per] = jnp.where(
                sub < split, pltpu.roll(one, split, 0), two
            )

    def digits(here):
        cell = cel_ref[:, here] + 1
        for bits in (0, 8, 16):
            digit = jnp.left_shift(jnp.bitwise_and(jnp.right_shift(cell, bits), 255), bits)
            yield digit.astype(jnp.float32).astype(jnp.bfloat16)

    pack(1, digits)
    send(1)
    for k in (4, 3, 2, 1):
        fetch(k).wait()
    for side in range(2):
        edge(side, True).wait_send()
        edge(side, True).wait_recv()
    pad_ref[:3, :LANES] = jnp.concatenate(
        [precv[0, :3, HALO:], pos_ref[:, :HALO]], axis=1
    )
    pad_ref[:3, npoint:] = jnp.concatenate(
        [pos_ref[:, npoint - HALO :], precv[1, :3, :HALO]], axis=1
    )
    begin_at = me * npoint
    everything = npoint * ndevice

    def pull(i, carry):
        for sub in range(2):
            base = pl.multiple_of(i * 2 * LANES + sub * LANES, LANES)
            here = pl.ds(base, LANES)
            lower = pad_ref[:, here]
            upper = pad_ref[:, pl.ds(base + LANES, LANES)]
            centre_pos = jnp.concatenate([lower[:, HALO:], upper[:, :HALO]], axis=1)
            index = con_ref[:, here] - begin_at + HALO
            index = jnp.where(index < 0, index + everything, index)
            index = jnp.where(index >= everything, index - everything, index) - base
            total = jnp.zeros_like(lower)
            for which in range(con_ref.shape[0]):
                wide = jnp.broadcast_to(index[which : which + 1], lower.shape)
                low = jnp.bitwise_and(wide, LANES - 1)
                near_by = jnp.take_along_axis(lower, low, axis=1, mode="promise_in_bounds")
                far = jnp.take_along_axis(upper, low, axis=1, mode="promise_in_bounds")
                picked = jnp.where(wide < LANES, near_by, far)
                total = total + wgt_ref[which : which + 1, here] * (picked - centre_pos)
            force = ten_ref[:, here] * total[:3]
            force_ref[:, here] = force
            jump_ref[:, here] = jnp.sum(force * nrm_ref[:, here], axis=0, keepdims=True)
        return carry

    lax.fori_loop(0, npoint // (2 * LANES), pull, 0, unroll=8)

    pack(0, lambda here: split3(jump_ref[:, here])[:2])
    send(0)
    for part in range(2):
        got_ref[part, rows_of(me)] = packed_ref[part, rows_of(me)]
    fine.finish(FIRST)
    fine.unpack()
    fine.start(LAST)
    coarse.finish(FIRST)
    coarse.unpack()
    coarse.start(LAST)
    fine.finish(LAST)
    coarse.finish(LAST)

    def receive(p, carry):
        for part in range(2):
            deal(part, p, False).wait_send()
            deal(part, p, True).wait_recv()
        return carry

    lax.fori_loop(1, ndevice, receive, 0)


def front(
    positions, normals, tension, edge_weight, connectivity, owner_ids, cell_map, shift,
    ndevice, nbin,
):
    npoint = tension.shape[0]
    nx, ny, nz = shift.shape
    vmem = pl.BlockSpec(memory_space=pltpu.VMEM)
    wide, cwide = wide_shapes(nx, ny, nz)
    return pl.pallas_call(
        functools.partial(front_kernel, ndevice, nbin),
        in_specs=[pl.BlockSpec(memory_space=pltpu.HBM)] * 8,
        out_specs=[vmem] * 4,
        out_shape=[
            jax.ShapeDtypeStruct(shape, jnp.float32)
            for shape in ((3, npoint), (2, 8 * ndevice, LANES), wide, cwide)
        ],
        scratch_shapes=[
            buf(3, npoint),
            buf(3, npoint),
            buf(1, npoint),
            buf(*edge_weight.shape),
            pltpu.VMEM(connectivity.shape, jnp.int32),
            pltpu.VMEM((1, npoint), jnp.int32),
            pltpu.VMEM((1, npoint), jnp.int32),
            buf(nx, ny, nz),
            buf(2, 8 * ndevice, LANES),
            buf(4 * ndevice, BIN),
            buf(nbin * ndevice, 1),
            pltpu.VMEM((1, npoint), jnp.int32),
            buf(1, npoint),
            buf(8, npoint + LANES),
            buf(2, 8, LANES),
            buf(2, 8, LANES),
            buf(nx // 2, ny, nz),
        ]
        + fine_scratch(nx, ny, nz)
        + coarse_scratch(nx, ny, nz)
        + [pltpu.SemaphoreType.DMA((2, 10))] * 2
        + [pltpu.SemaphoreType.DMA((2, ndevice))] * 2
        + [pltpu.SemaphoreType.DMA((2,))] * 2
        + [pltpu.SemaphoreType.DMA((8,))],
        compiler_params=pltpu.CompilerParams(
            collective_id=0, has_side_effects=True, vmem_limit_bytes=20 * 2**20
        ),
    )(
        *map(
            in_hbm,
            (
                positions, normals, tension[None], edge_weight, connectivity, owner_ids[None],
                cell_map[None], shift,
            ),
        )
    )


GROUP = 72


def scatter_kernel(
    nbin, rhs_hbm, got_ref, force_ref, out_ref, force_hbm,
    rhs_ref, acc_ref, list_ref, chunk_ref, sems,
):
    nrow, nz = rhs_ref.shape
    fetch = pltpu.make_async_copy(rhs_hbm, rhs_ref, sems.at[1])
    fetch.start()
    put = pltpu.make_async_copy(force_ref, force_hbm, sems.at[2])
    put.start()
    per = 8
    nsource = got_ref.shape[1] // per
    rows = nrow // nbin
    got = got_ref[1].reshape(nsource, per, LANES)
    used = got > 0.0
    lane = lax.broadcasted_iota(jnp.int32, (nsource, LANES), 1)
    ends = jnp.zeros((nsource, LANES), jnp.float32)
    for b in range(nbin):
        inside = jnp.where(used & (got <= float((b + 1) * BIN_CELLS)), 1.0, 0.0)
        total = jnp.sum(jnp.sum(inside, axis=1), axis=1, keepdims=True)
        ends = jnp.where(lane == b + 1, total, ends)
    ends = ends.astype(jnp.int32)
    stops = pltpu.roll(ends, LANES - 1, 1)
    firsts = jnp.right_shift(ends, 7)
    counts = jnp.where(stops > ends, jnp.right_shift(stops + LANES - 1, 7) - firsts, 0)
    counts = jnp.where(lane < nbin, counts, 0).astype(jnp.float32)
    square = (nsource, nsource)
    before = (
        lax.broadcasted_iota(jnp.int32, square, 0) > lax.broadcasted_iota(jnp.int32, square, 1)
    ).astype(jnp.float32).astype(jnp.bfloat16)
    starts = jnp.dot(before, counts.astype(jnp.bfloat16), preferred_element_type=jnp.float32)
    sums = jnp.sum(counts, axis=0, keepdims=True)
    width = list_ref.shape[1]
    source = lax.broadcasted_iota(jnp.int32, (nsource, width), 0)
    position = lax.broadcasted_iota(jnp.int32, (nsource, width), 1)
    for b in range(nbin):
        pick = slice(b, b + 1)
        step = position - starts[:, pick].astype(jnp.int32)
        chunk = firsts[:, pick] + step
        row = source * per + jnp.bitwise_and(chunk, 1) * (per // 2) + jnp.right_shift(chunk, 1)
        inside = (step >= 0) & (step < counts[:, pick].astype(jnp.int32))
        row = jnp.sum(jnp.where(inside, row.astype(jnp.float32), 0.0), axis=0, keepdims=True)
        list_ref[b : b + 1] = row.astype(jnp.int32)
        list_ref[nbin + b : nbin + b + 1] = jnp.broadcast_to(sums[:, pick], (1, width)).astype(
            jnp.int32
        )
    copy = pltpu.make_async_copy(list_ref, chunk_ref, sems.at[0])
    copy.start()
    copy.wait()
    fetch.wait()
    zero, unit = jnp.zeros((), jnp.bfloat16), jnp.ones((), jnp.bfloat16)
    row_level, col_level = levels(2 * rows), levels(BIN)

    def quarter(b, carry):
        total = chunk_ref[nbin + b, 0]
        acc_ref[...] = jnp.zeros_like(acc_ref)

        def work(step, carry):
            highs, lows, cols = [], [], []
            for k in range(GROUP):
                at = step * GROUP + k
                row = chunk_ref[b, jnp.minimum(at, width - 1)]
                value = got_ref[0, pl.ds(row, 1)]
                cell = got_ref[1, pl.ds(row, 1)].astype(jnp.int32) - 1
                fits = (jnp.right_shift(cell, BIN_SHIFT) == b) & (at < total)
                half = jnp.bitwise_and(jnp.right_shift(cell, 8), 1)
                place = half * rows + jnp.bitwise_and(jnp.right_shift(cell, 9), rows - 1)
                place = jnp.where(fits, place, 2 * rows).astype(jnp.float32).astype(jnp.bfloat16)
                col = jnp.bitwise_and(cell, BIN - 1).astype(jnp.float32).astype(jnp.bfloat16)
                first = value.astype(jnp.bfloat16)
                second = (value - first.astype(jnp.float32)).astype(jnp.bfloat16)
                same = row_level == place
                highs.append(jnp.where(same, first, zero))
                lows.append(jnp.where(same, second, zero))
                cols.append(jnp.where(col_level == col, unit, zero))
            left = jnp.concatenate(
                [jnp.concatenate(highs, axis=1), jnp.concatenate(lows, axis=1)], axis=0
            )
            both = lax.dot_general(
                left, jnp.concatenate(cols, axis=1), (((1,), (1,)), ((), ())),
                preferred_element_type=jnp.float32,
            )
            acc_ref[...] += both[: 2 * rows] + both[2 * rows :]
            return carry

        lax.fori_loop(0, lax.div(total + GROUP - 1, GROUP), work, 0)
        here = pl.ds(pl.multiple_of(b * rows, rows), rows)
        for half in range(2):
            cols = slice(half * BIN, (half + 1) * BIN)
            out_ref[here, cols] = rhs_ref[here, cols] + acc_ref[half * rows : (half + 1) * rows]
        return carry

    lax.fori_loop(0, nbin, quarter, 0)
    put.wait()


def scatter(rhs, got, force, nsource, nbin):
    nx, ny, nz = rhs.shape
    nrow = nx * ny
    vmem = pl.BlockSpec(memory_space=pltpu.VMEM)
    hbm = pl.BlockSpec(memory_space=pltpu.HBM)
    out, force = pl.pallas_call(
        functools.partial(scatter_kernel, nbin),
        in_specs=[hbm, vmem, vmem],
        out_specs=[vmem, hbm],
        out_shape=[
            jax.ShapeDtypeStruct((nrow, nz), jnp.float32),
            jax.ShapeDtypeStruct(force.shape, jnp.float32),
        ],
        scratch_shapes=[
            pltpu.VMEM((nrow, nz), jnp.float32),
            pltpu.VMEM((2 * nrow // nbin, BIN), jnp.float32),
            pltpu.VMEM((2 * nbin, 8 * nsource), jnp.int32),
            pltpu.SMEM((2 * nbin, 8 * nsource), jnp.int32),
            pltpu.SemaphoreType.DMA((3,)),
        ],
        compiler_params=pltpu.CompilerParams(vmem_limit_bytes=24 * 2**20),
        cost_estimate=pl.CostEstimate(
            flops=4 * nrow * nz * got.size // 2, bytes_accessed=4000000, transcendentals=0
        ),
    )(in_hbm(rhs.reshape(nrow, nz)), got, force)
    return out.reshape(nx, ny, nz), force


def body(
    pressure_rhs,
    shift_diag,
    positions,
    normals,
    tension,
    edge_weight,
    owner_map,
    cell_map,
    connectivity,
):
    ndevice = lax.axis_size(AXES)
    nbin = pressure_rhs.size // BIN_CELLS
    surface_force, got, inverse, cinverse = front(
        positions, normals, tension, edge_weight, connectivity, owner_map[:, 0], cell_map,
        shift_diag, ndevice, nbin,
    )
    forcing, surface_force = scatter(pressure_rhs, got, surface_force, ndevice, nbin)
    pressure = cycle(forcing, shift_diag, inverse, cinverse)
    return (pressure, surface_force)


def solution(mesh):
    return jax.shard_map(
        body,
        mesh=mesh,
        in_specs=(
            P("gx", "gy", "gz"),
            P("gx", "gy", "gz"),
            P(None, ("gx", "gy", "gz")),
            P(None, ("gx", "gy", "gz")),
            P(("gx", "gy", "gz")),
            P(None, ("gx", "gy", "gz")),
            P(("gx", "gy", "gz"), None),
            P(("gx", "gy", "gz")),
            P(None, ("gx", "gy", "gz")),
        ),
        out_specs=(P("gx", "gy", "gz"), P(None, ("gx", "gy", "gz"))),
        check_vma=False,
    )
```
